32 devices in a mesh: tables: 8 (over z, y), cells: 4 (over x, core).
Axes of the slice: x: 2, y: 2, z: 4, core: 2. Of those that a mesh axis runs over, the one named last changes fastest.
Arguments:
- cells_in: bfloat16 [8, 128, 112, 192], P('tables', 'cells'), may hold values from -6 to 6
- train_count: int32 [8], P('tables'), may hold values from 32 to 96
- feat_count: int32 [8], P('tables'), may hold values from 28 to 112
- feat_qkv: bfloat16 [192, 576], replicated, may hold values from -2 to 2
- feat_proj: bfloat16 [192, 192], replicated, may hold values from -2 to 2
- row_qkv: bfloat16 [192, 576], replicated, may hold values from -2 to 2
- row_proj: bfloat16 [192, 192], replicated, may hold values from -0.4375 to 0.4375
- w_in: bfloat16 [192, 768], replicated, may hold values from -0.4375 to 0.4375
- w_out: bfloat16 [768, 192], replicated, may hold values from -0.21875 to 0.21875
- cotangent: bfloat16 [8, 128, 112, 192], P('tables', 'cells'), may hold values from -6 to 6
Outputs:
- cells_out: bfloat16 [8, 128, 112, 192], P('tables', 'cells')
- grad_in: float32 [192, 768], P(None, ('tables', 'cells'))
- grad_out: float32 [768, 192], P(('tables', 'cells'))
The draws below stay inside these ranges and needn't reach their ends.
All inputs are finite; a program needn't handle non-finite values.
Results may differ from the reference program's by a relative error of at most 0.018.
Values may be sent and summed in bfloat16 or wider, within the bound.
No kernel may reach another device: no remote copies, remote signals or barrier semaphores. Data moves between devices by JAX's collectives and lax.ppermute only.
A program may use at most 128 MiB of HBM per device.

```python
import math
import jax
import jax.numpy as jnp
from jax import lax

E = 192
HEADS = 6
HEAD_DIM = 32
HID = 768
FEATS = 112
ROWS = 128
TABLES = 8


def base_weight(key, salt, rows, cols):
    values = jax.random.truncated_normal(jax.random.fold_in(key, salt), -6.0, 6.0, (rows, cols), jnp.float32)
    return values / jnp.float32(math.sqrt(rows))


def draw_feat_qkv(key, part):
    weight = base_weight(key, 31, E, 3 * E)
    return jnp.clip(weight, -2.0, 2.0).astype(jnp.bfloat16)


def draw_row_qkv(key, part):
    weight = base_weight(key, 41, E, 3 * E)
    return jnp.clip(weight, -2.0, 2.0).astype(jnp.bfloat16)


def draw_feat_proj(key, part):
    weight = base_weight(key, 51, E, E)
    return jnp.clip(weight, -2.0, 2.0).astype(jnp.bfloat16)


def draw_cells_in(key, part):
    cells = jax.random.truncated_normal(jax.random.fold_in(key, 21), -6.0, 6.0, (TABLES, ROWS, FEATS, E), jnp.float32)
    return jnp.clip(cells, -6.0, 6.0).astype(jnp.bfloat16)


def touch_ends(result, own_key, smallest, top_value):
    longest = result.shape.index(max(result.shape))
    spots = []
    for shift in (0, 1):
        where = [jax.random.randint(jax.random.fold_in(own_key, axis), (), 0, length) for axis, length in enumerate(result.shape)]
        where[longest] = (where[longest] + shift) % result.shape[longest]
        spots.append(tuple(where))
    return result.at[spots[0]].set(smallest).at[spots[1]].set(top_value)


def steps_of(own_key, shape, cuts, least, largest):
    loudness = 1.0
    for axis_at, shards_of in cuts:
        draws = jax.random.uniform(jax.random.fold_in(jax.random.fold_in(own_key, 6), axis_at), (shards_of,), jnp.float32, least / len(cuts), largest / len(cuts))
        loudness = loudness * jnp.repeat(jnp.exp(draws), shape[axis_at] // shards_of).reshape((-1,) + (1,) * (len(shape) - 1 - axis_at))
    return loudness


def bell_draw(rng, shape, scale, most, shards=(), kind=jnp.bfloat16):
    level = steps_of(rng, shape, shards, -0.22, 0.18) if shards else 1.0
    array = jax.random.normal(rng, shape, jnp.float32) * scale * level
    return jnp.minimum(jnp.maximum(array, -most), most).astype(kind)


def setup_inputs(seed: int = 0) -> dict:
    streams_of = jax.random.split(jax.random.key(seed), 11)
    cells_in = draw_cells_in(jax.random.fold_in(streams_of[10], 71), 0)
    train_count = touch_ends(jax.random.randint(streams_of[1], (TABLES,), ROWS // 4, ROWS - ROWS // 4 + 1), jax.random.fold_in(streams_of[1], 1), ROWS // 4, (ROWS - ROWS // 4 + 1) - 1).astype(jnp.int32)
    feat_count = touch_ends(jax.random.randint(streams_of[2], (TABLES,), FEATS // 4, FEATS + 1), jax.random.fold_in(streams_of[2], 1), FEATS // 4, FEATS).astype(jnp.int32)
    feat_qkv = draw_feat_qkv(jax.random.fold_in(streams_of[10], 71), 0)
    feat_proj = draw_feat_proj(jax.random.fold_in(streams_of[10], 71), 0)
    row_qkv = draw_row_qkv(jax.random.fold_in(streams_of[10], 71), 0)
    row_proj = bell_draw(streams_of[6], (E, E), E ** -0.5, 0.4375)
    w_in = bell_draw(streams_of[7], (E, HID), E ** -0.5, 0.4375)
    w_out = bell_draw(streams_of[8], (HID, E), HID ** -0.5, 0.21875)
    cotangent = bell_draw(streams_of[9], (TABLES, ROWS, FEATS, E), 1.0, 6.0, ((0, 8), (1, 4)))
    return dict(cells_in=cells_in, train_count=train_count, feat_count=feat_count, feat_qkv=feat_qkv, feat_proj=feat_proj, row_qkv=row_qkv, row_proj=row_proj, w_in=w_in, w_out=w_out, cotangent=cotangent)


def layer_norm(values):
    mean = lax.optimization_barrier(jnp.mean(values, axis=-1, keepdims=True))
    centred = values - mean
    var = lax.optimization_barrier(jnp.mean(centred * centred, axis=-1, keepdims=True))
    return centred / jnp.sqrt(var + 1e-05)

def feature_layer(block, feat_limit, weight_qkv, weight_proj):
    rows, feats, width = block.shape
    packed = jnp.dot(block.reshape(rows * feats, width), weight_qkv, preferred_element_type=jnp.float32)
    packed = packed.astype(jnp.bfloat16).reshape(rows, feats, 3, HEADS, HEAD_DIM).astype(jnp.float32)
    query, keys, values = (packed[:, :, 0], packed[:, :, 1], packed[:, :, 2])
    score = jnp.einsum('rfhd,rghd->rhfg', query, keys) / jnp.sqrt(jnp.float32(HEAD_DIM))
    keep = jnp.arange(feats, dtype=jnp.int32) < feat_limit
    score = jnp.where(keep[None, None, None, :], score, jnp.float32(-1e+30))
    probs = jax.nn.softmax(score, axis=-1).astype(jnp.bfloat16).astype(jnp.float32)
    attended = jnp.einsum('rhfg,rghd->rfhd', probs, values).astype(jnp.bfloat16)
    mixed = jnp.dot(attended.reshape(rows * feats, width), weight_proj, preferred_element_type=jnp.float32)
    total = block.reshape(rows * feats, width).astype(jnp.float32) + mixed
    return layer_norm(total).astype(jnp.bfloat16).reshape(rows, feats, width)

def row_single(column, train_limit, weight_qkv, weight_proj):
    rows, width = column.shape
    packed = jnp.dot(column, weight_qkv, preferred_element_type=jnp.float32)
    packed = packed.astype(jnp.bfloat16).reshape(rows, 3, HEADS, HEAD_DIM).astype(jnp.float32)
    query, keys, values = (packed[:, 0], packed[:, 1], packed[:, 2])
    score = jnp.einsum('ihd,jhd->hij', query, keys) / jnp.sqrt(jnp.float32(HEAD_DIM))
    keep = jnp.arange(rows, dtype=jnp.int32) < train_limit
    score = jnp.where(keep[None, None, :], score, jnp.float32(-1e+30))
    probs = jax.nn.softmax(score, axis=-1).astype(jnp.bfloat16).astype(jnp.float32)
    attended = jnp.einsum('hij,jhd->ihd', probs, values).astype(jnp.bfloat16).reshape(rows, width)
    mixed = jnp.dot(attended, weight_proj, preferred_element_type=jnp.float32)
    return layer_norm(column.astype(jnp.float32) + mixed).astype(jnp.bfloat16)

def exact_gelu(values):
    return jax.nn.gelu(values, approximate=False)

def reference(cells_in, train_count, feat_count, feat_qkv, feat_proj, row_qkv, row_proj, w_in, w_out, cotangent):

    def one_table(operands):
        block, cot_block, train_limit, feat_limit = operands
        mid = feature_layer(block, feat_limit, feat_qkv, feat_proj)
        columns = jnp.moveaxis(mid, 1, 0)
        normed_cols = lax.map(lambda column: row_single(column, train_limit, row_qkv, row_proj), columns)
        normed = jnp.moveaxis(normed_cols, 0, 1).reshape(-1, E)
        pre = jnp.dot(normed, w_in, preferred_element_type=jnp.float32)
        act_f, backward = jax.vjp(exact_gelu, pre)
        act = act_f.astype(jnp.bfloat16)
        output = (normed.astype(jnp.float32) + jnp.dot(act, w_out, preferred_element_type=jnp.float32)).astype(jnp.bfloat16)
        cot_flat = cot_block.reshape(-1, E)
        dact = jnp.dot(cot_flat, w_out.T, preferred_element_type=jnp.float32)
        dpre = backward(dact)[0].astype(jnp.bfloat16)
        part_in = jnp.dot(normed.T, dpre, preferred_element_type=jnp.float32)
        part_out = jnp.dot(act.T, cot_flat, preferred_element_type=jnp.float32)
        return (output.reshape(block.shape), part_in, part_out)
    outputs, parts_in, parts_out = lax.map(one_table, (cells_in, cotangent, train_count, feat_count))
    factor = 1.0 / jnp.sqrt(jnp.float32(TABLES * ROWS * FEATS))
    return (outputs, lax.optimization_barrier(jnp.sum(parts_in, axis=0)) * factor, lax.optimization_barrier(jnp.sum(parts_out, axis=0)) * factor)
```

```python
import functools
import math

import jax
import jax.numpy as jnp
from jax import lax
from jax.experimental import pallas as pl
from jax.experimental.pallas import tpu as pltpu
from jax.sharding import PartitionSpec as P

HEADS = 6
HEAD_DIM = 32
BF = jnp.bfloat16
F32 = jnp.float32
ERFC_P = 0.305
ERFC_C = (
    0.12163883478264824,
    0.12248037803568095,
    0.10333774640881799,
    0.1212905556291413,
    -0.03847457227018546,
    0.18624646374757975,
    -0.15328938951627163,
    0.03677003168237961,
)
NT = (((1,), (1,)), ((), ()))
TN = (((0,), (0,)), ((), ()))


def dot(a, b, dims=(((1,), (0,)), ((), ()))):
    return lax.dot_general(a, b, dims, preferred_element_type=F32)


def layer_norm(values):
    mean = jnp.mean(values, axis=-1, keepdims=True)
    centred = values - mean
    var = jnp.mean(centred * centred, axis=-1, keepdims=True)
    return centred * lax.rsqrt(var + 1e-05)


def swap_matrix(side):
    out = lax.broadcasted_iota(jnp.int32, (side * side, side * side), 0)
    src = lax.broadcasted_iota(jnp.int32, (side * side, side * side), 1)
    return (src == (out % side) * side + out // side).astype(F32).astype(BF)


def pack(parts):
    if len(parts) == 1:
        return parts[0]
    a, b = parts
    cut = a.shape[-1] // 128 * 128
    return jnp.concatenate([a[..., :cut], b[..., :cut], a[..., cut:], b[..., cut:]], axis=-1)


def unpack(block, per, width):
    if per == 1:
        return [block]
    cut = width // 128 * 128
    rest = width - cut
    return [
        jnp.concatenate(
            [block[..., q * cut : (q + 1) * cut], block[..., 2 * cut + q * rest : 2 * cut + (q + 1) * rest]],
            axis=-1,
        )
        for q in range(2)
    ]


def attend(items, keys, count, w_t, w_proj):
    n, width = items[0].shape
    lanes = -(-n // 128) * 128
    fill = [jnp.zeros((lanes - n, width), BF)] if lanes > n else []
    padded = jnp.concatenate([piece for item in items for piece in [item] + fill], axis=0)
    q_t = dot(w_t[:width], padded, NT) * F32(math.log2(math.e) / math.sqrt(HEAD_DIM))
    q_t = q_t.astype(BF)
    v_t = dot(w_t[2 * width :], padded, NT)
    k_all = dot(padded, w_t[width : 2 * width], NT)
    key_row = lax.broadcasted_iota(jnp.int32, (keys, 1), 0) < count
    key_lane = lax.broadcasted_iota(jnp.int32, (1, keys), 1) < count
    ones = jnp.broadcast_to(jnp.where(key_lane, F32(1), F32(0)), (16, keys)).astype(BF)
    hd = HEAD_DIM
    blank = jnp.zeros((hd, lanes), BF)
    results = []
    for a, item in enumerate(items):
        start = a * lanes
        k_own = k_all[start : start + keys]
        k_own = jnp.where(key_row, k_own, k_own[0:1]).astype(BF)
        v_own = jnp.where(key_lane, v_t[:, start : start + keys], F32(0)).astype(BF)
        q_own = q_t[:, start : start + lanes]
        heads = []
        for i in range(HEADS // 2):
            lo = 2 * i * hd
            top = jnp.concatenate([q_own[lo : lo + hd], blank], axis=1)
            bottom = jnp.concatenate([blank, q_own[lo + hd : lo + 2 * hd]], axis=1)
            tile = lo // 128 * 128
            tile_end = min(tile + 128, width)
            pieces = [top, bottom]
            if lo > tile:
                pieces = [jnp.zeros((lo - tile, 2 * lanes), BF)] + pieces
            if lo + 2 * hd < tile_end:
                pieces = pieces + [jnp.zeros((tile_end - lo - 2 * hd, 2 * lanes), BF)]
            score = dot(k_own[:, tile:tile_end], jnp.concatenate(pieces, axis=0))
            weight = jnp.exp2(score - jnp.max(score, axis=0, keepdims=True)).astype(BF)
            lhs = jnp.concatenate([v_own[lo : lo + 2 * hd], ones], axis=0)
            mixed = dot(lhs, weight)
            scale = 1.0 / mixed[2 * hd : 2 * hd + 1]
            heads.append((mixed[:hd, :lanes] * scale[:, :lanes]).astype(BF))
            heads.append((mixed[hd : 2 * hd, lanes:] * scale[:, lanes:]).astype(BF))
        attended_t = jnp.concatenate(heads, axis=0)
        mixed = dot(attended_t, w_proj, TN)
        results.append(layer_norm(item.astype(F32) + mixed[:n]))
    return results


def feature_kernel(groups, per, count_ref, cells_ref, wqkv_ref, wproj_ref, *refs):
    outs, (mid_ref, swap_ref) = refs[:groups], refs[groups:]
    rows, feats, width = cells_ref.shape
    fg = feats // groups
    half = fg // per
    count = count_ref[0]
    w_t = wqkv_ref[...].astype(F32).T.astype(BF)
    w_proj = wproj_ref[...]

    def step(r, carry):
        done = attend([cells_ref[2 * r], cells_ref[2 * r + 1]], feats, count, w_t, w_proj)
        for a in range(2):
            mid_ref[2 * r + a] = done[a].astype(BF)
        return carry

    lax.fori_loop(0, rows // 2, step, 0)
    swap = swap_matrix(rows)
    for f in range(feats // rows):
        block = mid_ref[:, f * rows : (f + 1) * rows, :].reshape(rows * rows, width)
        swapped = dot(swap, block).astype(BF).reshape(rows, rows, width)
        swap_ref[f * rows : (f + 1) * rows] = swapped
    here = lax.axis_index("cells")
    for m in range(groups):
        base = (here ^ m) * fg
        outs[m][...] = pack([swap_ref[pl.ds(base + q * half, half)] for q in range(per)])


def feature_chunk(block, count, wqkv, wproj, groups, per, chunk, rows):
    _, feats, width = block.shape
    half = feats // groups // per
    whole = lambda shape: pl.BlockSpec(shape, lambda i: (0,) * len(shape))
    return pl.pallas_call(
        functools.partial(feature_kernel, groups, per),
        grid=(1,),
        in_specs=[
            pl.BlockSpec(memory_space=pltpu.SMEM),
            pl.BlockSpec((rows, feats, width), lambda i: (chunk, 0, 0)),
            whole(wqkv.shape),
            whole(wproj.shape),
        ],
        out_specs=[whole((half, rows, per * width))] * groups,
        out_shape=[jax.ShapeDtypeStruct((half, rows, per * width), BF)] * groups,
        scratch_shapes=[pltpu.VMEM((rows, feats, width), BF), pltpu.VMEM((feats, rows, width), BF)],
        cost_estimate=pl.CostEstimate(flops=4 * 10**9, transcendentals=0, bytes_accessed=10**6),
        name=f"feature_{chunk}",
    )(count, block, wqkv, wproj)


def row_kernel(groups, per, chunks, keys, count_ref, wqkv_ref, wproj_ref, *refs):
    ins = refs[: groups * chunks]
    outs = refs[groups * chunks : groups * chunks + groups]
    x_ref, y_ref = refs[groups * chunks + groups :]
    pairs, sub_rows, _ = ins[0].shape
    local = sub_rows * chunks
    width = wproj_ref.shape[0]
    rows = local * groups
    count = count_ref[0]
    w_t = wqkv_ref[...].astype(F32).T.astype(BF)
    w_proj = wproj_ref[...]
    here = lax.axis_index("cells")

    def step(p, carry):
        for m in range(groups):
            for k in range(chunks):
                at = pl.multiple_of((here ^ m) * local + k * sub_rows, sub_rows)
                for q, part in enumerate(unpack(ins[k * groups + m][p], per, width)):
                    x_ref[p * per + q, pl.ds(at, sub_rows), :] = part
        done = attend([x_ref[p * per + q] for q in range(per)], keys, count, w_t, w_proj)
        y_ref[p] = pack([d.astype(BF) for d in done])
        return carry

    lax.fori_loop(0, pairs, step, 0)
    for m in range(groups):
        at = pl.multiple_of((here ^ m) * local, local)
        outs[m][...] = y_ref[:, pl.ds(at, local), :]


def row_chunk(pieces, count, wqkv, wproj, groups, per, chunks, chunk, pairs):
    sub_rows, packed = pieces[0].shape[1:]
    width = wproj.shape[0]
    local = sub_rows * chunks
    rows = local * groups
    keys = rows - rows // 4
    whole = lambda shape: pl.BlockSpec(shape, lambda i: (0,) * len(shape))
    return pl.pallas_call(
        functools.partial(row_kernel, groups, per, chunks, keys),
        grid=(1,),
        in_specs=[pl.BlockSpec(memory_space=pltpu.SMEM), whole(wqkv.shape), whole(wproj.shape)]
        + [pl.BlockSpec((pairs, sub_rows, packed), lambda i: (chunk, 0, 0))] * len(pieces),
        out_specs=[whole((pairs, local, packed))] * groups,
        out_shape=[jax.ShapeDtypeStruct((pairs, local, packed), BF)] * groups,
        scratch_shapes=[pltpu.VMEM((pairs * per, rows, width), BF), pltpu.VMEM((pairs, rows, packed), BF)],
        cost_estimate=pl.CostEstimate(flops=4 * 10**9, transcendentals=0, bytes_accessed=10**6),
        name=f"row_{chunk}",
    )(count, wqkv, wproj, *pieces)


def swap_kernel(in_ref, out_ref):
    first, second, width = in_ref.shape
    side = 16
    swap = swap_matrix(side)
    for a in range(first // side):
        for b in range(second // side):
            block = in_ref[a * side : (a + 1) * side, b * side : (b + 1) * side, :]
            swapped = dot(swap, block.reshape(side * side, width)).astype(BF)
            out_ref[b * side : (b + 1) * side, a * side : (a + 1) * side, :] = swapped.reshape(side, side, width)


def swap_cotangent(array):
    first, second, width = array.shape
    return pl.pallas_call(
        swap_kernel,
        out_shape=jax.ShapeDtypeStruct((second, first, width), BF),
        cost_estimate=pl.CostEstimate(flops=10**9, transcendentals=0, bytes_accessed=10**6),
        name="swap_cotangent",
    )(array)


def output_kernel(groups, per, *refs):
    ins, out_ref = refs[:-1], refs[-1]
    local, feats, width = out_ref.shape
    pairs = ins[0].shape[1]
    half = feats // groups // per
    side = 16
    swap = swap_matrix(side)

    def rows_of(feature, start):
        at, rest = divmod(feature, half)
        return ins[rest // pairs][at, rest % pairs, start : start + side, :]

    for f in range(0, feats, side):
        for r in range(0, local, side):
            block = jnp.concatenate([rows_of(f + i, r) for i in range(side)], axis=0)
            out_ref[r : r + side, f : f + side, :] = dot(swap, block).astype(BF).reshape(side, side, width)


def swap_output(chunks, groups, per, feats):
    _, _, local, width = chunks[0].shape
    return pl.pallas_call(
        functools.partial(output_kernel, groups, per),
        out_shape=jax.ShapeDtypeStruct((local, feats, width), BF),
        cost_estimate=pl.CostEstimate(flops=10**9, transcendentals=0, bytes_accessed=10**6),
        name="swap_output",
    )(*chunks)


def gelu_and_slope(pre):
    size = jnp.abs(pre)
    bell = jnp.exp2(pre * pre * F32(-0.5 * math.log2(math.e)))
    t = 1.0 / (1.0 + F32(ERFC_P) * size)
    poly = F32(ERFC_C[-1])
    for coefficient in ERFC_C[-2::-1]:
        poly = poly * t + F32(coefficient)
    tail = poly * t * bell
    cdf = jnp.where(pre >= 0, 1.0 - tail, tail)
    return pre * cdf, cdf + pre * (bell * F32(1.0 / math.sqrt(2.0 * math.pi)))


def dense_kernel(groups, per, chunk, factor, *refs):
    last = factor is not None
    ins = refs[:groups]
    win_ref, wout_ref, cot_ref = refs[groups : groups + 3]
    rest = refs[groups + 3 :]
    if chunk > 0:
        prev_in, prev_out = rest[:2]
        rest = rest[2:]
    if last:
        out_ref, grad_ref, n_ref, gin_ref, gout_ref = rest
    else:
        out_ref, gin_ref, gout_ref, n_ref = rest
    pairs, local, _ = ins[0].shape
    width, hid = win_ref.shape
    size = pairs * local
    fg = cot_ref.shape[0] // groups
    half = fg // per
    here = lax.axis_index("cells")
    for m in range(groups):
        for q, part in enumerate(unpack(ins[m][...], per, width)):
            n_ref[m * per + q] = part.reshape(size, width)
    if chunk > 0:
        gin_ref[...] = prev_in[...]
        gout_ref[...] = prev_out[...]
    else:
        gin_ref[...] = jnp.zeros_like(gin_ref)
        gout_ref[...] = jnp.zeros_like(gout_ref)
    w_in = win_ref[...]
    w_out = wout_ref[...]

    def step(b, carry):
        group = here ^ (b // per)
        feature = group * fg + (b % per) * half + chunk * pairs
        normed = n_ref[b]
        cot = cot_ref[pl.ds(feature, pairs)].reshape(size, width)
        act, slope = gelu_and_slope(dot(normed, w_in))
        act = act.astype(BF)
        dpre = (dot(cot, w_out, NT) * slope).astype(BF)
        result = (normed.astype(F32) + dot(act, w_out)).astype(BF)
        out_ref[group * per + b % per] = result.reshape(pairs, local, width)
        gin_ref[...] += dot(normed, dpre, TN)
        gout_ref[...] += dot(cot, act, TN)
        return carry

    lax.fori_loop(0, groups * per, step, 0)
    if last:
        grad_ref[...] = pack(
            [(gin_ref[...].T * F32(factor)).astype(BF), (gout_ref[...].T * F32(factor)).astype(BF)]
        )


def dense_chunk(pieces, cot_t, w_in, w_out, prev, groups, per, chunk, factor):
    pairs, local, packed = pieces[0].shape
    width, hid = w_in.shape
    cells = jax.ShapeDtypeStruct((groups * per, pairs, local, width), BF)
    partial = jax.ShapeDtypeStruct((width, hid), F32)
    operands = list(pieces) + [w_in, w_out, cot_t]
    if prev is not None:
        operands += list(prev)
    scratch = [pltpu.VMEM((groups * per, pairs * local, width), BF)]
    if factor is None:
        outs = [cells, partial, partial]
    else:
        outs = [cells, jax.ShapeDtypeStruct((hid, 2 * width), BF)]
        scratch += [pltpu.VMEM((width, hid), F32)] * 2
    return pl.pallas_call(
        functools.partial(dense_kernel, groups, per, chunk, factor),
        out_shape=outs,
        scratch_shapes=scratch,
        cost_estimate=pl.CostEstimate(flops=10**10, transcendentals=0, bytes_accessed=10**6),
        name=f"dense_{chunk}",
    )(*operands)


def exchange(pieces, groups):
    return [pieces[0]] + [
        lax.ppermute(pieces[m], "cells", [(s, s ^ m) for s in range(groups)]) for m in range(1, groups)
    ]


def per_device(
    cells_in, train_count, feat_count, feat_qkv, feat_proj, row_qkv, row_proj, w_in, w_out, cotangent
):
    block = cells_in[0]
    local, feats, width = block.shape
    groups = lax.axis_size("cells")
    tables = lax.axis_size("tables")
    fg = feats // groups
    per = 2 if fg % 2 == 0 else 1
    half = fg // per
    sub_rows = 16
    row_chunks = local // sub_rows
    feat_chunks = 2 if half % 2 == 0 else 1
    factor = 1.0 / math.sqrt(tables * local * groups * feats)
    pieces = []
    for k in range(row_chunks):
        sent = feature_chunk(block, feat_count, feat_qkv, feat_proj, groups, per, k, sub_rows)
        pieces += exchange(sent, groups)
    cot_t = swap_cotangent(cotangent[0])
    back = []
    for j in range(feat_chunks):
        done = row_chunk(
            pieces, train_count, row_qkv, row_proj, groups, per, row_chunks, j, half // feat_chunks
        )
        back.append(exchange(done, groups))
    outs = []
    grads = None
    for j in range(feat_chunks):
        out_j, *grads = dense_chunk(
            back[j], cot_t, w_in, w_out, grads, groups, per, j, factor if j == feat_chunks - 1 else None
        )
        outs.append(out_j)
    output = swap_output(outs, groups, per, feats)
    pieces = grads[0].reshape(tables * groups, -1, 2 * width)
    total = lax.all_to_all(pieces, ("tables", "cells"), split_axis=0, concat_axis=0, tiled=True)
    total = jnp.sum(total.astype(F32), axis=0)
    grad_in, grad_out = unpack(total, 2, width)
    return (output[None], grad_in.T, grad_out)


def solution(mesh):
    spread = P("tables", "cells", None, None)
    return jax.shard_map(
        per_device,
        mesh=mesh,
        in_specs=(spread, P("tables"), P("tables"), P(), P(), P(), P(), P(), P(), spread),
        out_specs=(spread, P(None, ("tables", "cells")), P(("tables", "cells"), None)),
        check_vma=False,
    )
```

```python
import functools
import math

import jax
import jax.numpy as jnp
from jax import lax
from jax.experimental import pallas as pl
from jax.experimental.pallas import tpu as pltpu
from jax.sharding import PartitionSpec as P

HEADS = 6
HEAD_DIM = 32
BF = jnp.bfloat16
F32 = jnp.float32
ERFC_K = 3.5
ERFC_C = (
    0.4096238545958983,
    1.030471715475736,
    9.637057789606283,
    -24.75291485624482,
    177.3359613786631,
    -181.2859739558248,
)
NT = (((1,), (1,)), ((), ()))
TN = (((0,), (0,)), ((), ()))


def dot(a, b, dims=(((1,), (0,)), ((), ()))):
    return lax.dot_general(a, b, dims, preferred_element_type=F32)


def layer_norm(values):
    mean = jnp.mean(values, axis=-1, keepdims=True)
    centred = values - mean
    var = jnp.mean(centred * centred, axis=-1, keepdims=True)
    return centred * lax.rsqrt(var + 1e-05)


def swap_matrix(side):
    out = lax.broadcasted_iota(jnp.int32, (side * side, side * side), 0)
    src = lax.broadcasted_iota(jnp.int32, (side * side, side * side), 1)
    return (src == (out % side) * side + out // side).astype(F32).astype(BF)


def pack(parts):
    if len(parts) == 1:
        return parts[0]
    a, b = parts
    cut = a.shape[-1] // 128 * 128
    return jnp.concatenate([a[..., :cut], b[..., :cut], a[..., cut:], b[..., cut:]], axis=-1)


def unpack(block, per, width):
    if per == 1:
        return [block]
    cut = width // 128 * 128
    rest = width - cut
    return [
        jnp.concatenate(
            [block[..., q * cut : (q + 1) * cut], block[..., 2 * cut + q * rest : 2 * cut + (q + 1) * rest]],
            axis=-1,
        )
        for q in range(2)
    ]


def mask_of(keys, count):
    rows = lax.broadcasted_iota(jnp.int32, (keys, 1), 0) < count
    lanes = lax.broadcasted_iota(jnp.int32, (1, keys), 1) < count
    return rows, lanes


def keep_projected(refs, at, q_v, k_rows, n, lanes, masks):
    q_ref, k_ref, v_ref = refs
    width, keys = q_ref.shape[1], k_ref.shape[1]
    key_row, key_lane = masks
    scale = F32(math.log2(math.e) / math.sqrt(HEAD_DIM))
    q_ref[at] = (q_v[:width] * scale).astype(BF)
    v_ref[at] = jnp.where(key_lane, q_v[width:, :keys], F32(0)).astype(BF)
    k_ref[at] = jnp.where(key_row, k_rows[:keys], k_rows[0:1]).astype(BF)


def score_blocks(q_own, lanes):
    hd = HEAD_DIM
    width = q_own.shape[0]
    blank = jnp.zeros((hd, lanes), BF)
    blocks = []
    for i in range(HEADS // 2):
        lo = 2 * i * hd
        tile = lo // 128 * 128
        end = min(tile + 128, width)
        pieces = [
            jnp.concatenate([q_own[lo : lo + hd], blank], axis=1),
            jnp.concatenate([blank, q_own[lo + hd : lo + 2 * hd]], axis=1),
        ]
        if lo > tile:
            pieces = [jnp.zeros((lo - tile, 2 * lanes), BF)] + pieces
        if lo + 2 * hd < end:
            pieces = pieces + [jnp.zeros((end - lo - 2 * hd, 2 * lanes), BF)]
        blocks.append((tile, end, jnp.concatenate(pieces, axis=0)))
    return blocks


def attend(refs, att_ref, ats, ones):
    q_ref, k_ref, v_ref = refs
    lanes = q_ref.shape[2]
    hd = HEAD_DIM
    scores = []
    for at in ats:
        k_own = k_ref[at]
        for tile, end, block in score_blocks(q_ref[at], lanes):
            scores.append(dot(k_own[:, tile:end], block))
    weights = [jnp.exp2(s - jnp.max(s, axis=0, keepdims=True)).astype(BF) for s in scores]
    for n, at in enumerate(ats):
        v_own = v_ref[at]
        for i in range(HEADS // 2):
            lo = 2 * i * hd
            lhs = jnp.concatenate([v_own[lo : lo + 2 * hd], ones], axis=0)
            mixed = dot(lhs, weights[n * (HEADS // 2) + i])
            scale = 1.0 / mixed[2 * hd : 2 * hd + 1]
            att_ref[at, lo : lo + hd] = (mixed[:hd, :lanes] * scale[:, :lanes]).astype(BF)
            att_ref[at, lo + hd : lo + 2 * hd] = (mixed[hd : 2 * hd, lanes:] * scale[:, lanes:]).astype(BF)


def loop(count, most, body):
    group = max(d for d in range(1, most + 1) if count % d == 0)

    def step(i, carry):
        body([i * group + a for a in range(group)])
        return carry

    lax.fori_loop(0, count // group, step, 0)


def pad_lanes(value, lanes):
    rows, n = value.shape
    return value if n == lanes else jnp.concatenate([value, jnp.zeros((rows, lanes - n), value.dtype)], axis=1)


def feature_kernel(groups, per, first, rows, count_ref, cells_ref, wqkv_ref, wproj_ref, *refs):
    outs = refs[:groups]
    q_ref, k_ref, v_ref, att_ref, x_ref, mid_ref, swap_ref = refs[groups:]
    _, width, feats = cells_ref.shape
    lanes = q_ref.shape[2]
    fg = feats // groups
    half = fg // per
    count = count_ref[0]
    w_t = wqkv_ref[...].astype(F32).T.astype(BF)
    w_qv = jnp.concatenate([w_t[:width], w_t[2 * width :]], axis=0)
    w_k = w_t[width : 2 * width]
    w_proj = wproj_ref[...]
    masks = mask_of(feats, count)
    ones = jnp.broadcast_to(jnp.where(masks[1], F32(1), F32(0)), (16, feats)).astype(BF)
    kept = (q_ref, k_ref, v_ref)

    def project(ats):
        x_t = [pad_lanes(cells_ref[first + at], lanes) for at in ats]
        q_v = dot(w_qv, jnp.concatenate(x_t, axis=1))
        x = [t.T[:feats] for t in x_t]
        k = dot(jnp.concatenate(x, axis=0), w_k, NT)
        for a, at in enumerate(ats):
            x_ref[at] = x[a]
            keep_projected(
                kept, at, q_v[:, a * lanes : (a + 1) * lanes], k[a * feats : (a + 1) * feats], feats, lanes, masks
            )

    def finish(ats):
        for at in ats:
            mixed = dot(att_ref[at], w_proj, TN)[:feats]
            mid_ref[at] = layer_norm(x_ref[at].astype(F32) + mixed).astype(BF)

    loop(rows, 4, project)
    loop(rows, UNROLL, lambda ats: attend(kept, att_ref, ats, ones))
    loop(rows, 4, finish)
    swap = swap_matrix(rows)
    for f in range(feats // rows):
        block = mid_ref[:, f * rows : (f + 1) * rows, :].reshape(rows * rows, width)
        swap_ref[f * rows : (f + 1) * rows] = dot(swap, block).astype(BF).reshape(rows, rows, width)
    here = lax.axis_index("cells")
    for m in range(groups):
        base = (here ^ m) * fg
        outs[m][...] = pack([swap_ref[pl.ds(base + q * half, half)] for q in range(per)])


UNROLL = 4
IN_VMEM = pl.BlockSpec(memory_space=pltpu.VMEM)
IN_SMEM = pl.BlockSpec(memory_space=pltpu.SMEM)


def attention_scratch(items, width, lanes, keys):
    return [
        pltpu.VMEM((items, width, lanes), BF),
        pltpu.VMEM((items, keys, width), BF),
        pltpu.VMEM((items, width, keys), BF),
        pltpu.VMEM((items, width, lanes), BF),
    ]


def cost(flops):
    return pl.CostEstimate(flops=flops, transcendentals=0, bytes_accessed=10**6)


def feature_chunk(block_t, count, wqkv, wproj, groups, per, chunk, rows):
    _, width, feats = block_t.shape
    half = feats // groups // per
    lanes = -(-feats // 128) * 128
    return pl.pallas_call(
        functools.partial(feature_kernel, groups, per, chunk * rows, rows),
        in_specs=[IN_SMEM] + [IN_VMEM] * 3,
        out_specs=[IN_VMEM] * groups,
        out_shape=[jax.ShapeDtypeStruct((half, rows, per * width), BF)] * groups,
        scratch_shapes=attention_scratch(rows, width, lanes, feats)
        + [
            pltpu.VMEM((rows, feats, width), BF),
            pltpu.VMEM((rows, feats, width), BF),
            pltpu.VMEM((feats, rows, width), BF),
        ],
        cost_estimate=cost(4 * 10**9),
        name=f"feature_{chunk}",
    )(count, block_t, wqkv, wproj)


def row_kernel(groups, per, chunks, first, count_ref, wqkv_ref, wproj_ref, *refs):
    ins = refs[: groups * chunks]
    outs = refs[groups * chunks : groups * chunks + groups]
    q_ref, k_ref, v_ref, att_ref, x_ref, y_ref = refs[groups * chunks + groups :]
    pairs, local, _ = outs[0].shape
    sub_rows = local // chunks
    items, rows, width = x_ref.shape
    keys = k_ref.shape[1]
    count = count_ref[0]
    w_t = wqkv_ref[...].astype(F32).T.astype(BF)
    w_qv = jnp.concatenate([w_t[:width], w_t[2 * width :]], axis=0)
    w_k = w_t[width : 2 * width]
    w_proj = wproj_ref[...]
    masks = mask_of(keys, count)
    ones = jnp.broadcast_to(jnp.where(masks[1], F32(1), F32(0)), (16, keys)).astype(BF)
    kept = (q_ref, k_ref, v_ref)
    here = lax.axis_index("cells")
    for m in range(groups):
        for k in range(chunks):
            at = pl.multiple_of((here ^ m) * local + k * sub_rows, sub_rows)
            for q, part in enumerate(unpack(ins[k * groups + m][first : first + pairs], per, width)):
                x_ref[q * pairs : (q + 1) * pairs, pl.ds(at, sub_rows), :] = part

    def project(ats):
        x = jnp.concatenate([x_ref[at] for at in ats], axis=0)
        q_v = dot(w_qv, x, NT)
        for a, at in enumerate(ats):
            k = dot(x[a * rows : a * rows + keys], w_k, NT)
            keep_projected(kept, at, q_v[:, a * rows : (a + 1) * rows], k, rows, rows, masks)

    def finish(ps):
        for p in ps:
            done = []
            for q in range(per):
                at = q * pairs + p
                done.append(layer_norm(x_ref[at].astype(F32) + dot(att_ref[at], w_proj, TN)).astype(BF))
            y_ref[p] = pack(done)

    loop(items, 4, project)
    loop(items, UNROLL, lambda ats: attend(kept, att_ref, ats, ones))
    loop(pairs, 2, finish)
    for m in range(groups):
        at = pl.multiple_of((here ^ m) * local, local)
        outs[m][...] = y_ref[:, pl.ds(at, local), :]


def row_chunk(pieces, count, wqkv, wproj, groups, per, chunks, chunk, pairs):
    sub_rows, packed = pieces[0].shape[1:]
    width = wproj.shape[0]
    local = sub_rows * chunks
    rows = local * groups
    keys = rows - rows // 4
    return pl.pallas_call(
        functools.partial(row_kernel, groups, per, chunks, chunk * pairs),
        in_specs=[IN_SMEM] + [IN_VMEM] * (2 + len(pieces)),
        out_specs=[IN_VMEM] * groups,
        out_shape=[jax.ShapeDtypeStruct((pairs, local, packed), BF)] * groups,
        scratch_shapes=attention_scratch(pairs * per, width, rows, keys)
        + [pltpu.VMEM((pairs * per, rows, width), BF), pltpu.VMEM((pairs, rows, packed), BF)],
        cost_estimate=cost(4 * 10**9),
        name=f"row_{chunk}",
    )(count, wqkv, wproj, *pieces)


def swap_kernel(in_ref, out_ref, x_ref):
    first, width, second = in_ref.shape
    lanes = -(-second // 128) * 128
    side = 16
    swap = swap_matrix(side)
    for a in range(first):
        x_ref[a] = pad_lanes(in_ref[a], lanes).T[:second]
    for a in range(first // side):
        for b in range(second // side):
            block = x_ref[a * side : (a + 1) * side, b * side : (b + 1) * side, :]
            swapped = dot(swap, block.reshape(side * side, width)).astype(BF)
            out_ref[b * side : (b + 1) * side, a * side : (a + 1) * side, :] = swapped.reshape(side, side, width)


def swap_cotangent(array_t):
    first, width, second = array_t.shape
    return pl.pallas_call(
        swap_kernel,
        in_specs=[IN_VMEM],
        out_specs=IN_VMEM,
        out_shape=jax.ShapeDtypeStruct((second, first, width), BF),
        scratch_shapes=[pltpu.VMEM((first, second, width), BF)],
        cost_estimate=cost(10**9),
        name="swap_cotangent",
    )(array_t)


def output_kernel(groups, per, *refs):
    ins, (out_ref, y_ref) = refs[:-2], refs[-2:]
    local, width, feats = out_ref.shape
    pairs = ins[0].shape[1]
    half = feats // groups // per
    lanes = -(-feats // 128) * 128
    side = 16
    swap = swap_matrix(side)

    def rows_of(feature, start):
        at, rest = divmod(feature, half)
        return ins[rest // pairs][at, rest % pairs, start : start + side, :]

    for f in range(0, feats, side):
        for r in range(0, local, side):
            block = jnp.concatenate([rows_of(f + i, r) for i in range(side)], axis=0)
            y_ref[r : r + side, f : f + side, :] = dot(swap, block).astype(BF).reshape(side, side, width)
    for r in range(local):
        y = y_ref[r]
        if lanes > feats:
            y = jnp.concatenate([y, jnp.zeros((lanes - feats, width), BF)], axis=0)
        out_ref[r] = y.T[:, :feats]


def swap_output(chunks, groups, per, feats):
    _, _, local, width = chunks[0].shape
    return pl.pallas_call(
        functools.partial(output_kernel, groups, per),
        in_specs=[IN_VMEM] * len(chunks),
        out_specs=IN_VMEM,
        out_shape=jax.ShapeDtypeStruct((local, width, feats), BF),
        scratch_shapes=[pltpu.VMEM((local, feats, width), BF)],
        cost_estimate=cost(10**9),
        name="swap_output",
    )(*chunks)


def gelu_and_slope(pre):
    size = jnp.abs(pre)
    bell = jnp.exp2(pre * pre * F32(-0.5 * math.log2(math.e)))
    t = 1.0 / (size + F32(ERFC_K))
    poly = F32(ERFC_C[-1])
    for coefficient in ERFC_C[-2::-1]:
        poly = poly * t + F32(coefficient)
    tail = poly * t * bell
    cdf = jnp.where(pre >= 0, 1.0 - tail, tail)
    return pre * cdf, cdf + pre * (bell * F32(1.0 / math.sqrt(2.0 * math.pi)))


def dense_kernel(groups, per, chunk, factor, *refs):
    last = factor is not None
    ins = refs[:groups]
    win_ref, woutt_ref, cot_ref = refs[groups : groups + 3]
    rest = refs[groups + 3 :]
    if chunk > 0:
        prev_in, prev_out = rest[:2]
        rest = rest[2:]
    if last:
        out_ref, grad_ref, n_ref, gin_ref, gout_ref = rest
    else:
        out_ref, gin_ref, gout_ref, n_ref = rest
    pairs, local, _ = ins[0].shape
    width, hid = win_ref.shape
    size = pairs * local
    fg = cot_ref.shape[0] // groups
    half = fg // per
    here = lax.axis_index("cells")
    for m in range(groups):
        for q, part in enumerate(unpack(ins[m][...], per, width)):
            n_ref[m * per + q] = part.reshape(size, width)
    if chunk > 0:
        gin_ref[...] = prev_in[...]
        gout_ref[...] = prev_out[...]
    else:
        gin_ref[...] = jnp.zeros_like(gin_ref)
        gout_ref[...] = jnp.zeros_like(gout_ref)
    w_in = win_ref[...]
    w_out_t = woutt_ref[...]

    def step(b, carry):
        group = here ^ (b // per)
        feature = group * fg + (b % per) * half + chunk * pairs
        normed = n_ref[b]
        cot = cot_ref[pl.ds(feature, pairs)].reshape(size, width)
        act, slope = gelu_and_slope(dot(normed, w_in))
        act = act.astype(BF)
        dpre = (dot(cot, w_out_t) * slope).astype(BF)
        result = (normed.astype(F32) + dot(act, w_out_t, NT)).astype(BF)
        out_ref[group * per + b % per] = result.reshape(pairs, local, width)
        gin_ref[...] += dot(normed, dpre, TN)
        gout_ref[...] += dot(cot, act, TN)
        return carry

    lax.fori_loop(0, groups * per, step, 0)
    if last:
        grad_ref[...] = pack(
            [(gin_ref[...].T * F32(factor)).astype(BF), (gout_ref[...].T * F32(factor)).astype(BF)]
        )


def dense_chunk(pieces, cot_t, w_in, w_out_t, prev, groups, per, chunk, factor):
    pairs, local, packed = pieces[0].shape
    width, hid = w_in.shape
    cells = jax.ShapeDtypeStruct((groups * per, pairs, local, width), BF)
    partial = jax.ShapeDtypeStruct((width, hid), F32)
    operands = list(pieces) + [w_in, w_out_t, cot_t]
    if prev is not None:
        operands += list(prev)
    scratch = [pltpu.VMEM((groups * per, pairs * local, width), BF)]
    if factor is None:
        outs = [cells, partial, partial]
    else:
        outs = [cells, jax.ShapeDtypeStruct((hid, 2 * width), BF)]
        scratch += [pltpu.VMEM((width, hid), F32)] * 2
    return pl.pallas_call(
        functools.partial(dense_kernel, groups, per, chunk, factor),
        in_specs=[IN_VMEM] * len(operands),
        out_specs=[IN_VMEM] * len(outs),
        out_shape=outs,
        scratch_shapes=scratch,
        cost_estimate=cost(10**10),
        name=f"dense_{chunk}",
    )(*operands)


def exchange(pieces, groups):
    return [pieces[0]] + [
        lax.ppermute(pieces[m], "cells", [(s, s ^ m) for s in range(groups)]) for m in range(1, groups)
    ]


def per_device(
    cells_in, train_count, feat_count, feat_qkv, feat_proj, row_qkv, row_proj, w_in, w_out, cotangent
):
    block_t = jnp.swapaxes(cells_in[0], 1, 2)
    local, width, feats = block_t.shape
    groups = lax.axis_size("cells")
    tables = lax.axis_size("tables")
    fg = feats // groups
    per = 2 if fg % 2 == 0 else 1
    half = fg // per
    sub_rows = 16
    row_chunks = local // sub_rows
    feat_chunks = 2 if half % 2 == 0 else 1
    factor = 1.0 / math.sqrt(tables * local * groups * feats)
    pieces = []
    for k in range(row_chunks):
        sent = feature_chunk(block_t, feat_count, feat_qkv, feat_proj, groups, per, k, sub_rows)
        pieces += exchange(sent, groups)
    cot_t = swap_cotangent(jnp.swapaxes(cotangent[0], 1, 2))
    back = []
    for j in range(feat_chunks):
        done = row_chunk(
            pieces, train_count, row_qkv, row_proj, groups, per, row_chunks, j, half // feat_chunks
        )
        back.append(exchange(done, groups))
    outs = []
    grads = None
    for j in range(feat_chunks):
        out_j, *grads = dense_chunk(
            back[j], cot_t, w_in, w_out.T, grads, groups, per, j, factor if j == feat_chunks - 1 else None
        )
        outs.append(out_j)
    output = jnp.swapaxes(swap_output(outs, groups, per, feats), 1, 2)
    pieces = grads[0].reshape(tables * groups, -1, 2 * width)
    total = lax.all_to_all(pieces, ("tables", "cells"), split_axis=0, concat_axis=0, tiled=True)
    total = jnp.sum(total.astype(F32), axis=0)
    grad_in, grad_out = unpack(total, 2, width)
    return (output[None], grad_in.T, grad_out)


def solution(mesh):
    spread = P("tables", "cells", None, None)
    return jax.shard_map(
        per_device,
        mesh=mesh,
        in_specs=(spread, P("tables"), P("tables"), P(), P(), P(), P(), P(), P(), spread),
        out_specs=(spread, P(None, ("tables", "cells")), P(("tables", "cells"), None)),
        check_vma=False,
    )
```

```python
import functools
import math

import jax
import jax.numpy as jnp
from jax import lax
from jax.experimental import pallas as pl
from jax.experimental.pallas import tpu as pltpu
from jax.sharding import PartitionSpec as P

HEADS = 6
HEAD_DIM = 32
BF = jnp.bfloat16
F32 = jnp.float32
ERFC_K = 3.5
ERFC_C = (
    0.4096238545958983,
    1.030471715475736,
    9.637057789606283,
    -24.75291485624482,
    177.3359613786631,
    -181.2859739558248,
)
NT = (((1,), (1,)), ((), ()))
TN = (((0,), (0,)), ((), ()))


def dot(a, b, dims=(((1,), (0,)), ((), ()))):
    return lax.dot_general(a, b, dims, preferred_element_type=F32)


def layer_norm(values):
    mean = jnp.mean(values, axis=-1, keepdims=True)
    centred = values - mean
    var = jnp.mean(centred * centred, axis=-1, keepdims=True)
    return centred * lax.rsqrt(var + 1e-05)


def swap_matrix(side):
    out = lax.broadcasted_iota(jnp.int32, (side * side, side * side), 0)
    src = lax.broadcasted_iota(jnp.int32, (side * side, side * side), 1)
    return (src == (out % side) * side + out // side).astype(F32).astype(BF)


def pack(parts):
    if len(parts) == 1:
        return parts[0]
    a, b = parts
    cut = a.shape[-1] // 128 * 128
    return jnp.concatenate([a[..., :cut], b[..., :cut], a[..., cut:], b[..., cut:]], axis=-1)


def unpack(block, per, width):
    if per == 1:
        return [block]
    cut = width // 128 * 128
    rest = width - cut
    return [
        jnp.concatenate(
            [block[..., q * cut : (q + 1) * cut], block[..., 2 * cut + q * rest : 2 * cut + (q + 1) * rest]],
            axis=-1,
        )
        for q in range(2)
    ]


def mask_of(keys, count):
    rows = lax.broadcasted_iota(jnp.int32, (keys, 1), 0) < count
    lanes = lax.broadcasted_iota(jnp.int32, (1, keys), 1) < count
    return rows, lanes


def keep_projected(refs, at, q_v, k_rows, n, lanes, masks):
    q_ref, k_ref, v_ref = refs
    width, keys = q_ref.shape[1], k_ref.shape[1]
    key_row, key_lane = masks
    scale = F32(math.log2(math.e) / math.sqrt(HEAD_DIM))
    q_ref[at] = (q_v[:width] * scale).astype(BF)
    v_ref[at] = jnp.where(key_lane, q_v[width:, :keys], F32(0)).astype(BF)
    k_ref[at] = jnp.where(key_row, k_rows[:keys], k_rows[0:1]).astype(BF)


def score_blocks(q_own, lanes):
    hd = HEAD_DIM
    width = q_own.shape[0]
    blank = jnp.zeros((hd, lanes), BF)
    blocks = []
    for i in range(HEADS // 2):
        lo = 2 * i * hd
        tile = lo // 128 * 128
        end = min(tile + 128, width)
        pieces = [
            jnp.concatenate([q_own[lo : lo + hd], blank], axis=1),
            jnp.concatenate([blank, q_own[lo + hd : lo + 2 * hd]], axis=1),
        ]
        if lo > tile:
            pieces = [jnp.zeros((lo - tile, 2 * lanes), BF)] + pieces
        if lo + 2 * hd < end:
            pieces = pieces + [jnp.zeros((end - lo - 2 * hd, 2 * lanes), BF)]
        blocks.append((tile, end, jnp.concatenate(pieces, axis=0)))
    return blocks


def attend(refs, att_ref, ats, ones):
    q_ref, k_ref, v_ref = refs
    lanes = q_ref.shape[2]
    hd = HEAD_DIM
    scores = []
    for at in ats:
        k_own = k_ref[at]
        for tile, end, block in score_blocks(q_ref[at], lanes):
            scores.append(dot(k_own[:, tile:end], block))
    weights = [jnp.exp2(s - jnp.max(s, axis=0, keepdims=True)).astype(BF) for s in scores]
    for n, at in enumerate(ats):
        v_own = v_ref[at]
        for i in range(HEADS // 2):
            lo = 2 * i * hd
            lhs = jnp.concatenate([v_own[lo : lo + 2 * hd], ones], axis=0)
            mixed = dot(lhs, weights[n * (HEADS // 2) + i])
            scale = 1.0 / mixed[2 * hd : 2 * hd + 1]
            att_ref[at, lo : lo + hd] = (mixed[:hd, :lanes] * scale[:, :lanes]).astype(BF)
            att_ref[at, lo + hd : lo + 2 * hd] = (mixed[hd : 2 * hd, lanes:] * scale[:, lanes:]).astype(BF)


def loop(count, most, body):
    group = max(d for d in range(1, most + 1) if count % d == 0)

    def step(i, carry):
        body([i * group + a for a in range(group)])
        return carry

    lax.fori_loop(0, count // group, step, 0)


def pad_lanes(value, lanes):
    rows, n = value.shape
    return value if n == lanes else jnp.concatenate([value, jnp.zeros((rows, lanes - n), value.dtype)], axis=1)


def feature_kernel(groups, per, first, rows, count_ref, cells_ref, wqkv_ref, wproj_ref, *refs):
    outs = refs[:groups]
    q_ref, k_ref, v_ref, att_ref, x_ref, mid_ref, swap_ref = refs[groups:]
    _, width, feats = cells_ref.shape
    lanes = q_ref.shape[2]
    fg = feats // groups
    half = fg // per
    count = count_ref[0]
    w_t = wqkv_ref[...].T
    w_qv = jnp.concatenate([w_t[:width], w_t[2 * width :]], axis=0)
    w_k = w_t[width : 2 * width]
    w_proj = wproj_ref[...]
    masks = mask_of(feats, count)
    ones = jnp.broadcast_to(jnp.where(masks[1], F32(1), F32(0)), (16, feats)).astype(BF)
    kept = (q_ref, k_ref, v_ref)

    def project(ats):
        x_t = [pad_lanes(cells_ref[first + at], lanes) for at in ats]
        q_v = dot(w_qv, jnp.concatenate(x_t, axis=1))
        x = [t.T[:feats] for t in x_t]
        k = dot(jnp.concatenate(x, axis=0), w_k, NT)
        for a, at in enumerate(ats):
            x_ref[at] = x[a]
            keep_projected(
                kept, at, q_v[:, a * lanes : (a + 1) * lanes], k[a * feats : (a + 1) * feats], feats, lanes, masks
            )

    def finish(ats):
        for at in ats:
            mixed = dot(att_ref[at].T[:feats], w_proj)
            mid_ref[at] = layer_norm(x_ref[at].astype(F32) + mixed).astype(BF)

    loop(rows, 8, project)
    loop(rows, 8, lambda ats: attend(kept, att_ref, ats, ones))
    loop(rows, 8, finish)
    swap = swap_matrix(rows)
    for f in range(feats // rows):
        block = mid_ref[:, f * rows : (f + 1) * rows, :].reshape(rows * rows, width)
        swap_ref[f * rows : (f + 1) * rows] = dot(swap, block).astype(BF).reshape(rows, rows, width)
    here = lax.axis_index("cells")
    for m in range(groups):
        base = (here ^ m) * fg
        outs[m][...] = pack([swap_ref[pl.ds(base + q * half, half)] for q in range(per)])


IN_VMEM = pl.BlockSpec(memory_space=pltpu.VMEM)
IN_SMEM = pl.BlockSpec(memory_space=pltpu.SMEM)


def attention_scratch(items, width, lanes, keys):
    return [
        pltpu.VMEM((items, width, lanes), BF),
        pltpu.VMEM((items, keys, width), BF),
        pltpu.VMEM((items, width, keys), BF),
        pltpu.VMEM((items, width, lanes), BF),
    ]


def near(shape, dtype=BF):
    return pltpu.VMEM(shape, dtype)


def bring(*arrays):
    return [pltpu.with_memory_space_constraint(x, pltpu.VMEM) for x in arrays]


PARAMS = pltpu.CompilerParams(vmem_limit_bytes=32 * 2**20)


def cost(flops):
    return pl.CostEstimate(flops=flops, transcendentals=0, bytes_accessed=10**6)


def feature_chunk(block_t, count, wqkv, wproj, groups, per, chunk, rows):
    _, width, feats = block_t.shape
    half = feats // groups // per
    lanes = -(-feats // 128) * 128
    return pl.pallas_call(
        functools.partial(feature_kernel, groups, per, chunk * rows, rows),
        in_specs=[IN_SMEM] + [IN_VMEM] * 3,
        out_specs=[IN_VMEM] * groups,
        out_shape=[near((half, rows, per * width))] * groups,
        scratch_shapes=attention_scratch(rows, width, lanes, feats)
        + [
            pltpu.VMEM((rows, feats, width), BF),
            pltpu.VMEM((rows, feats, width), BF),
            pltpu.VMEM((feats, rows, width), BF),
        ],
        compiler_params=PARAMS,
        cost_estimate=cost(4 * 10**9),
        name=f"feature_{chunk}",
    )(count, *bring(block_t, wqkv, wproj))


def row_kernel(groups, per, chunks, first, count_ref, wqkv_ref, wproj_ref, *refs):
    ins = refs[: groups * chunks]
    outs = refs[groups * chunks : groups * chunks + groups]
    q_ref, k_ref, v_ref, att_ref, x_ref, y_ref = refs[groups * chunks + groups :]
    pairs, local, _ = outs[0].shape
    sub_rows = local // chunks
    items, rows, width = x_ref.shape
    keys = k_ref.shape[1]
    count = count_ref[0]
    w_t = wqkv_ref[...].T
    w_qv = jnp.concatenate([w_t[:width], w_t[2 * width :]], axis=0)
    w_k = w_t[width : 2 * width]
    w_proj = wproj_ref[...]
    masks = mask_of(keys, count)
    ones = jnp.broadcast_to(jnp.where(masks[1], F32(1), F32(0)), (16, keys)).astype(BF)
    kept = (q_ref, k_ref, v_ref)
    here = lax.axis_index("cells")
    for m in range(groups):
        for k in range(chunks):
            at = pl.multiple_of((here ^ m) * local + k * sub_rows, sub_rows)
            for q, part in enumerate(unpack(ins[k * groups + m][first : first + pairs], per, width)):
                x_ref[q * pairs : (q + 1) * pairs, pl.ds(at, sub_rows), :] = part

    def project(ats):
        x = jnp.concatenate([x_ref[at] for at in ats], axis=0)
        q_v = dot(w_qv, x, NT)
        for a, at in enumerate(ats):
            k = dot(x[a * rows : a * rows + keys], w_k, NT)
            keep_projected(kept, at, q_v[:, a * rows : (a + 1) * rows], k, rows, rows, masks)

    def finish(ps):
        for p in ps:
            done = []
            for q in range(per):
                at = q * pairs + p
                done.append(layer_norm(x_ref[at].astype(F32) + dot(att_ref[at].T, w_proj)).astype(BF))
            y_ref[p] = pack(done)

    most = max(1, 1024 // rows)
    loop(items, min(most, 7), project)
    loop(items, min(most, 7), lambda ats: attend(kept, att_ref, ats, ones))
    loop(pairs, min(most, 7), finish)
    for m in range(groups):
        at = pl.multiple_of((here ^ m) * local, local)
        outs[m][...] = y_ref[:, pl.ds(at, local), :]


def row_chunk(pieces, count, wqkv, wproj, groups, per, chunks, chunk, pairs):
    sub_rows, packed = pieces[0].shape[1:]
    width = wproj.shape[0]
    local = sub_rows * chunks
    rows = local * groups
    keys = rows - rows // 4
    return pl.pallas_call(
        functools.partial(row_kernel, groups, per, chunks, chunk * pairs),
        in_specs=[IN_SMEM] + [IN_VMEM] * (2 + len(pieces)),
        out_specs=[IN_VMEM] * groups,
        out_shape=[near((pairs, local, packed))] * groups,
        scratch_shapes=attention_scratch(pairs * per, width, rows, keys)
        + [pltpu.VMEM((pairs * per, rows, width), BF), pltpu.VMEM((pairs, rows, packed), BF)],
        compiler_params=PARAMS,
        cost_estimate=cost(4 * 10**9),
        name=f"row_{chunk}",
    )(count, *bring(wqkv, wproj, *pieces))


def swap_kernel(in_ref, out_ref, x_ref):
    first, width, second = in_ref.shape
    lanes = -(-second // 128) * 128
    side = 16
    swap = swap_matrix(side)
    for a in range(first):
        x_ref[a] = pad_lanes(in_ref[a], lanes).T[:second]
    for a in range(first // side):
        for b in range(second // side):
            block = x_ref[a * side : (a + 1) * side, b * side : (b + 1) * side, :]
            swapped = dot(swap, block.reshape(side * side, width)).astype(BF)
            out_ref[b * side : (b + 1) * side, a * side : (a + 1) * side, :] = swapped.reshape(side, side, width)


def swap_cotangent(array_t):
    first, width, second = array_t.shape
    return pl.pallas_call(
        swap_kernel,
        in_specs=[IN_VMEM],
        out_specs=IN_VMEM,
        out_shape=near((second, first, width)),
        scratch_shapes=[pltpu.VMEM((first, second, width), BF)],
        compiler_params=PARAMS,
        cost_estimate=cost(10**9),
        name="swap_cotangent",
    )(*bring(array_t))


def output_kernel(groups, per, *refs):
    ins, (out_ref, y_ref) = refs[:-2], refs[-2:]
    local, width, feats = out_ref.shape
    pairs = ins[0].shape[1]
    half = feats // groups // per
    lanes = -(-feats // 128) * 128
    side = 16
    swap = swap_matrix(side)

    def rows_of(feature, start):
        at, rest = divmod(feature, half)
        return ins[rest // pairs][at, rest % pairs, start : start + side, :]

    for f in range(0, feats, side):
        for r in range(0, local, side):
            block = jnp.concatenate([rows_of(f + i, r) for i in range(side)], axis=0)
            y_ref[r : r + side, f : f + side, :] = dot(swap, block).astype(BF).reshape(side, side, width)
    for r in range(local):
        y = y_ref[r]
        if lanes > feats:
            y = jnp.concatenate([y, jnp.zeros((lanes - feats, width), BF)], axis=0)
        out_ref[r] = y.T[:, :feats]


def swap_output(chunks, groups, per, feats):
    _, _, local, width = chunks[0].shape
    return pl.pallas_call(
        functools.partial(output_kernel, groups, per),
        in_specs=[IN_VMEM] * len(chunks),
        out_specs=IN_VMEM,
        out_shape=jax.ShapeDtypeStruct((local, width, feats), BF),
        scratch_shapes=[pltpu.VMEM((local, feats, width), BF)],
        compiler_params=PARAMS,
        cost_estimate=cost(10**9),
        name="swap_output",
    )(*bring(*chunks))


def gelu_and_slope(pre):
    size = jnp.abs(pre)
    bell = jnp.exp2(pre * pre * F32(-0.5 * math.log2(math.e)))
    t = 1.0 / (size + F32(ERFC_K))
    poly = F32(ERFC_C[-1])
    for coefficient in ERFC_C[-2::-1]:
        poly = poly * t + F32(coefficient)
    tail = poly * t * bell
    cdf = jnp.where(pre >= 0, 1.0 - tail, tail)
    return pre * cdf, cdf + pre * (bell * F32(1.0 / math.sqrt(2.0 * math.pi)))


def dense_kernel(groups, per, chunk, factor, *refs):
    last = factor is not None
    ins = refs[:groups]
    win_ref, woutt_ref, cot_ref = refs[groups : groups + 3]
    rest = refs[groups + 3 :]
    if chunk > 0:
        prev_in, prev_out = rest[:2]
        rest = rest[2:]
    if last:
        out_ref, grad_ref, n_ref, gin_ref, gout_ref = rest
    else:
        out_ref, gin_ref, gout_ref, n_ref = rest
    pairs, local, _ = ins[0].shape
    width, hid = win_ref.shape
    size = pairs * local
    fg = cot_ref.shape[0] // groups
    half = fg // per
    here = lax.axis_index("cells")
    for m in range(groups):
        for q, part in enumerate(unpack(ins[m][...], per, width)):
            n_ref[m * per + q] = part.reshape(size, width)
    if chunk > 0:
        gin_ref[...] = prev_in[...]
        gout_ref[...] = prev_out[...]
    else:
        gin_ref[...] = jnp.zeros_like(gin_ref)
        gout_ref[...] = jnp.zeros_like(gout_ref)
    w_in = win_ref[...]
    w_out_t = woutt_ref[...]

    def step(b, carry):
        group = here ^ (b // per)
        feature = group * fg + (b % per) * half + chunk * pairs
        normed = n_ref[b]
        cot = cot_ref[pl.ds(feature, pairs)].reshape(size, width)
        act, slope = gelu_and_slope(dot(normed, w_in))
        act = act.astype(BF)
        dpre = (dot(cot, w_out_t) * slope).astype(BF)
        result = (normed.astype(F32) + dot(act, w_out_t, NT)).astype(BF)
        out_ref[group * per + b % per] = result.reshape(pairs, local, width)
        gin_ref[...] += dot(normed, dpre, TN)
        gout_ref[...] += dot(cot, act, TN)
        return carry

    lax.fori_loop(0, groups * per, step, 0)
    if last:
        grad_ref[...] = pack(
            [(gin_ref[...].T * F32(factor)).astype(BF), (gout_ref[...].T * F32(factor)).astype(BF)]
        )


def dense_chunk(pieces, cot_t, w_in, w_out_t, prev, groups, per, chunk, factor):
    pairs, local, packed = pieces[0].shape
    width, hid = w_in.shape
    cells = near((groups * per, pairs, local, width))
    partial = near((width, hid), F32)
    operands = list(pieces) + [w_in, w_out_t, cot_t]
    if prev is not None:
        operands += list(prev)
    scratch = [pltpu.VMEM((groups * per, pairs * local, width), BF)]
    if factor is None:
        outs = [cells, partial, partial]
    else:
        outs = [cells, near((hid, 2 * width))]
        scratch += [pltpu.VMEM((width, hid), F32)] * 2
    return pl.pallas_call(
        functools.partial(dense_kernel, groups, per, chunk, factor),
        in_specs=[IN_VMEM] * len(operands),
        out_specs=[IN_VMEM] * len(outs),
        out_shape=outs,
        scratch_shapes=scratch,
        compiler_params=PARAMS,
        cost_estimate=cost(10**10),
        name=f"dense_{chunk}",
    )(*bring(*operands))


def exchange(pieces, groups):
    return [pieces[0]] + [
        lax.ppermute(pieces[m], "cells", [(s, s ^ m) for s in range(groups)]) for m in range(1, groups)
    ]


def per_device(
    cells_in, train_count, feat_count, feat_qkv, feat_proj, row_qkv, row_proj, w_in, w_out, cotangent
):
    block_t = jnp.swapaxes(cells_in[0], 1, 2)
    local, width, feats = block_t.shape
    groups = lax.axis_size("cells")
    tables = lax.axis_size("tables")
    fg = feats // groups
    per = 2 if fg % 2 == 0 else 1
    half = fg // per
    sub_rows = 16
    row_chunks = local // sub_rows
    feat_chunks = 2 if half % 2 == 0 else 1
    factor = 1.0 / math.sqrt(tables * local * groups * feats)
    pieces = []
    for k in range(row_chunks):
        sent = feature_chunk(block_t, feat_count, feat_qkv, feat_proj, groups, per, k, sub_rows)
        pieces += exchange(sent, groups)
    cot_t = swap_cotangent(jnp.swapaxes(cotangent[0], 1, 2))
    back = []
    for j in range(feat_chunks):
        done = row_chunk(
            pieces, train_count, row_qkv, row_proj, groups, per, row_chunks, j, half // feat_chunks
        )
        back.append(exchange(done, groups))
    outs = []
    grads = None
    for j in range(feat_chunks):
        out_j, *grads = dense_chunk(
            back[j], cot_t, w_in, w_out.T, grads, groups, per, j, factor if j == feat_chunks - 1 else None
        )
        outs.append(out_j)
    output = jnp.swapaxes(swap_output(outs, groups, per, feats), 1, 2)
    pieces = grads[0].reshape(tables * groups, -1, 2 * width)
    total = lax.all_to_all(pieces, ("tables", "cells"), split_axis=0, concat_axis=0, tiled=True)
    total = jnp.sum(total.astype(F32), axis=0)
    grad_in, grad_out = unpack(total, 2, width)
    return (output[None], grad_in.T, grad_out)


def solution(mesh):
    spread = P("tables", "cells", None, None)
    return jax.shard_map(
        per_device,
        mesh=mesh,
        in_specs=(spread, P("tables"), P("tables"), P(), P(), P(), P(), P(), P(), spread),
        out_specs=(spread, P(None, ("tables", "cells")), P(("tables", "cells"), None)),
        check_vma=False,
    )
```

```python
import functools
import math

import jax
import jax.numpy as jnp
from jax import lax
from jax.experimental import pallas as pl
from jax.experimental.pallas import tpu as pltpu
from jax.sharding import PartitionSpec as P

HEADS = 6
HEAD_DIM = 32
BF = jnp.bfloat16
F32 = jnp.float32
ERFC_K = 3.5
ERFC_C = (
    0.4096238545958983,
    1.030471715475736,
    9.637057789606283,
    -24.75291485624482,
    177.3359613786631,
    -181.2859739558248,
)
NT = (((1,), (1,)), ((), ()))
TN = (((0,), (0,)), ((), ()))


def dot(a, b, dims=(((1,), (0,)), ((), ()))):
    return lax.dot_general(a, b, dims, preferred_element_type=F32)


def layer_norm(values):
    mean = jnp.mean(values, axis=0, keepdims=True)
    centred = values - mean
    var = jnp.mean(centred * centred, axis=0, keepdims=True)
    return centred * lax.rsqrt(var + 1e-05)


def one_hot(rows, cols):
    row = lax.broadcasted_iota(jnp.int32, (rows, cols), 0)
    col = lax.broadcasted_iota(jnp.int32, (rows, cols), 1)
    return (row == col).astype(F32).astype(BF)


def finish_items(att_ref, ats, w_proj_t, flip, residual_t):
    lanes = att_ref.shape[2]
    mixed = dot(w_proj_t, jnp.concatenate([att_ref[at] for at in ats], axis=1))
    done = []
    for a, at in enumerate(ats):
        normed = layer_norm(residual_t(at).astype(F32) + mixed[:, a * lanes : (a + 1) * lanes]).astype(BF)
        done.append(dot(flip, normed, NT).astype(BF))
    return done


def swap_matrix(side):
    out = lax.broadcasted_iota(jnp.int32, (side * side, side * side), 0)
    src = lax.broadcasted_iota(jnp.int32, (side * side, side * side), 1)
    return (src == (out % side) * side + out // side).astype(F32).astype(BF)


def pack(parts):
    if len(parts) == 1:
        return parts[0]
    a, b = parts
    cut = a.shape[-1] // 128 * 128
    return jnp.concatenate([a[..., :cut], b[..., :cut], a[..., cut:], b[..., cut:]], axis=-1)


def unpack(block, per, width):
    if per == 1:
        return [block]
    cut = width // 128 * 128
    rest = width - cut
    return [
        jnp.concatenate(
            [block[..., q * cut : (q + 1) * cut], block[..., 2 * cut + q * rest : 2 * cut + (q + 1) * rest]],
            axis=-1,
        )
        for q in range(2)
    ]


def mask_of(keys, count):
    rows = lax.broadcasted_iota(jnp.int32, (keys, 1), 0) < count
    lanes = lax.broadcasted_iota(jnp.int32, (1, keys), 1) < count
    return rows, lanes


def keep_projected(refs, at, q_v, k_rows, n, lanes, masks):
    q_ref, k_ref, v_ref = refs
    width, keys = q_ref.shape[1], k_ref.shape[1]
    key_row, key_lane = masks
    scale = F32(math.log2(math.e) / math.sqrt(HEAD_DIM))
    q_ref[at] = (q_v[:width] * scale).astype(BF)
    v_ref[at] = jnp.where(key_lane, q_v[width:, :keys], F32(0)).astype(BF)
    k_ref[at] = jnp.where(key_row, k_rows[:keys], k_rows[0:1]).astype(BF)


def score_blocks(q_own, lanes):
    hd = HEAD_DIM
    width = q_own.shape[0]
    blank = jnp.zeros((hd, lanes), BF)
    blocks = []
    for i in range(HEADS // 2):
        lo = 2 * i * hd
        tile = lo // 128 * 128
        end = min(tile + 128, width)
        pieces = [
            jnp.concatenate([q_own[lo : lo + hd], blank], axis=1),
            jnp.concatenate([blank, q_own[lo + hd : lo + 2 * hd]], axis=1),
        ]
        if lo > tile:
            pieces = [jnp.zeros((lo - tile, 2 * lanes), BF)] + pieces
        if lo + 2 * hd < end:
            pieces = pieces + [jnp.zeros((end - lo - 2 * hd, 2 * lanes), BF)]
        blocks.append((tile, end, jnp.concatenate(pieces, axis=0)))
    return blocks


def attend(refs, att_ref, ats, ones):
    q_ref, k_ref, v_ref = refs
    lanes = q_ref.shape[2]
    hd = HEAD_DIM
    scores = []
    for at in ats:
        k_own = k_ref[at]
        for tile, end, block in score_blocks(q_ref[at], lanes):
            scores.append(dot(k_own[:, tile:end], block))
    weights = [jnp.exp2(s - jnp.max(s, axis=0, keepdims=True)).astype(BF) for s in scores]
    for n, at in enumerate(ats):
        v_own = v_ref[at]
        for i in range(HEADS // 2):
            lo = 2 * i * hd
            lhs = jnp.concatenate([v_own[lo : lo + 2 * hd], ones], axis=0)
            mixed = dot(lhs, weights[n * (HEADS // 2) + i])
            scale = 1.0 / mixed[2 * hd : 2 * hd + 1]
            att_ref[at, lo : lo + hd] = (mixed[:hd, :lanes] * scale[:, :lanes]).astype(BF)
            att_ref[at, lo + hd : lo + 2 * hd] = (mixed[hd : 2 * hd, lanes:] * scale[:, lanes:]).astype(BF)


def loop(count, most, body):
    group = max(d for d in range(1, most + 1) if count % d == 0)

    def step(i, carry):
        body([i * group + a for a in range(group)])
        return carry

    lax.fori_loop(0, count // group, step, 0)


def pad_lanes(value, lanes):
    rows, n = value.shape
    return value if n == lanes else jnp.concatenate([value, jnp.zeros((rows, lanes - n), value.dtype)], axis=1)


def feature_kernel(groups, per, first, rows, cuts, count_ref, cells_ref, wqkv_ref, wproj_ref, *refs):
    outs = refs[: groups * cuts]
    q_ref, k_ref, v_ref, att_ref, mid_ref, swap_ref = refs[groups * cuts :]
    _, width, feats = cells_ref.shape
    lanes = q_ref.shape[2]
    fg = feats // groups
    half = fg // per
    count = count_ref[0]
    w_t = wqkv_ref[...].T
    w_qv = jnp.concatenate([w_t[:width], w_t[2 * width :]], axis=0)
    w_k = w_t[width : 2 * width]
    w_proj_t = wproj_ref[...].T
    flip = one_hot(feats, lanes)
    masks = mask_of(feats, count)
    ones = jnp.broadcast_to(jnp.where(masks[1], F32(1), F32(0)), (16, feats)).astype(BF)
    kept = (q_ref, k_ref, v_ref)

    def project(ats):
        x_t = [pad_lanes(cells_ref[first + at], lanes) for at in ats]
        q_v = dot(w_qv, jnp.concatenate(x_t, axis=1))
        x = [t.T[:feats] for t in x_t]
        k = dot(jnp.concatenate(x, axis=0), w_k, NT)
        for a, at in enumerate(ats):
            keep_projected(
                kept, at, q_v[:, a * lanes : (a + 1) * lanes], k[a * feats : (a + 1) * feats], feats, lanes, masks
            )

    def finish(ats):
        own = lambda at: pad_lanes(cells_ref[first + at], lanes)
        for at, value in zip(ats, finish_items(att_ref, ats, w_proj_t, flip, own)):
            mid_ref[at] = value

    loop(rows, 8, project)
    loop(rows, 8, lambda ats: attend(kept, att_ref, ats, ones))
    loop(rows, 8, finish)
    swap = swap_matrix(rows)
    for f in range(feats // rows):
        block = mid_ref[:, f * rows : (f + 1) * rows, :].reshape(rows * rows, width)
        swap_ref[f * rows : (f + 1) * rows] = dot(swap, block).astype(BF).reshape(rows, rows, width)
    here = lax.axis_index("cells")
    size = half // cuts
    for c in range(cuts):
        for m in range(groups):
            base = (here ^ m) * fg + c * size
            outs[c * groups + m][...] = pack([swap_ref[pl.ds(base + q * half, size)] for q in range(per)])


IN_VMEM = pl.BlockSpec(memory_space=pltpu.VMEM)
IN_SMEM = pl.BlockSpec(memory_space=pltpu.SMEM)


def attention_scratch(items, width, lanes, keys):
    return [
        pltpu.VMEM((items, width, lanes), BF),
        pltpu.VMEM((items, keys, width), BF),
        pltpu.VMEM((items, width, keys), BF),
        pltpu.VMEM((items, width, lanes), BF),
    ]


def near(shape, dtype=BF):
    return pltpu.VMEM(shape, dtype)


def bring(*arrays):
    return [pltpu.with_memory_space_constraint(x, pltpu.VMEM) for x in arrays]


PARAMS = pltpu.CompilerParams(vmem_limit_bytes=32 * 2**20)


def cost(flops):
    return pl.CostEstimate(flops=flops, transcendentals=0, bytes_accessed=10**6)


def feature_chunk(block_t, count, wqkv, wproj, groups, per, chunk, rows, cuts):
    _, width, feats = block_t.shape
    half = feats // groups // per
    lanes = -(-feats // 128) * 128
    operands = [block_t, wqkv, wproj]
    if chunk == 0:
        base, specs = 0, [pl.BlockSpec((rows, width, feats), lambda i: (0, 0, 0)), IN_VMEM, IN_VMEM]
        operands = [pltpu.with_memory_space_constraint(x, pltpu.HBM) for x in operands]
    else:
        base, specs = chunk * rows, [IN_VMEM] * 3
        operands = bring(*operands)
    return pl.pallas_call(
        functools.partial(feature_kernel, groups, per, base, rows, cuts),
        grid=(1,),
        in_specs=[IN_SMEM] + specs,
        out_specs=[IN_VMEM] * (groups * cuts),
        out_shape=[near((half // cuts, rows, per * width))] * (groups * cuts),
        scratch_shapes=attention_scratch(rows, width, lanes, feats)
        + [pltpu.VMEM((rows, feats, width), BF), pltpu.VMEM((feats, rows, width), BF)],
        compiler_params=PARAMS,
        cost_estimate=cost(4 * 10**9),
        name=f"feature_{chunk}",
    )(count, *operands)


def row_kernel(groups, per, chunks, firsts, count_ref, wqkv_ref, wproj_ref, *refs):
    ins = refs[: groups * chunks]
    outs = refs[groups * chunks : groups * chunks + groups]
    q_ref, k_ref, v_ref, att_ref, x_ref, xt_ref, y_ref = refs[groups * chunks + groups :]
    pairs, local, _ = outs[0].shape
    sub_rows = local // chunks
    items, rows, width = x_ref.shape
    keys = k_ref.shape[1]
    count = count_ref[0]
    w_t = wqkv_ref[...].T
    w_qv = jnp.concatenate([w_t[:width], w_t[2 * width :], one_hot(width, width)], axis=0)
    w_k = w_t[width : 2 * width]
    w_proj_t = wproj_ref[...].T
    flip = one_hot(rows, rows)
    masks = mask_of(keys, count)
    ones = jnp.broadcast_to(jnp.where(masks[1], F32(1), F32(0)), (16, keys)).astype(BF)
    kept = (q_ref, k_ref, v_ref)
    here = lax.axis_index("cells")
    for m in range(groups):
        for k in range(chunks):
            at = pl.multiple_of((here ^ m) * local + k * sub_rows, sub_rows)
            for q, part in enumerate(unpack(ins[k * groups + m][firsts[k] : firsts[k] + pairs], per, width)):
                x_ref[q * pairs : (q + 1) * pairs, pl.ds(at, sub_rows), :] = part

    def project(ats):
        x = jnp.concatenate([x_ref[at] for at in ats], axis=0)
        q_v = dot(w_qv, x, NT)
        for a, at in enumerate(ats):
            k = dot(x[a * rows : a * rows + keys], w_k, NT)
            own = q_v[:, a * rows : (a + 1) * rows]
            xt_ref[at] = own[2 * width :].astype(BF)
            keep_projected(kept, at, own[: 2 * width], k, rows, rows, masks)

    def finish(ps):
        ats = [q * pairs + p for p in ps for q in range(per)]
        done = finish_items(att_ref, ats, w_proj_t, flip, lambda at: xt_ref[at])
        for a, p in enumerate(ps):
            y_ref[p] = pack(done[a * per : (a + 1) * per])

    most = max(1, 1024 // rows)
    loop(items, min(most, 7), project)
    loop(items, min(most, 7), lambda ats: attend(kept, att_ref, ats, ones))
    loop(pairs, min(most, 7), finish)
    for m in range(groups):
        at = pl.multiple_of((here ^ m) * local, local)
        outs[m][...] = y_ref[:, pl.ds(at, local), :]


def row_chunk(pieces, count, wqkv, wproj, groups, per, chunks, chunk, pairs, firsts):
    sub_rows, packed = pieces[0].shape[1:]
    width = wproj.shape[0]
    local = sub_rows * chunks
    rows = local * groups
    keys = rows - rows // 4
    return pl.pallas_call(
        functools.partial(row_kernel, groups, per, chunks, firsts),
        in_specs=[IN_SMEM] + [IN_VMEM] * (2 + len(pieces)),
        out_specs=[IN_VMEM] * groups,
        out_shape=[near((pairs, local, packed))] * groups,
        scratch_shapes=attention_scratch(pairs * per, width, rows, keys)
        + [
            pltpu.VMEM((pairs * per, rows, width), BF),
            pltpu.VMEM((pairs * per, width, rows), BF),
            pltpu.VMEM((pairs, rows, packed), BF),
        ],
        compiler_params=PARAMS,
        cost_estimate=cost(4 * 10**9),
        name=f"row_{chunk}",
    )(count, *bring(wqkv, wproj, *pieces))


def swap_kernel(in_ref, out_ref, x_ref):
    first, width, second = in_ref.shape
    lanes = -(-second // 128) * 128
    side = 16
    swap = swap_matrix(side)
    for a in range(first):
        x_ref[a] = pad_lanes(in_ref[a], lanes).T[:second]
    for a in range(first // side):
        for b in range(second // side):
            block = x_ref[a * side : (a + 1) * side, b * side : (b + 1) * side, :]
            swapped = dot(swap, block.reshape(side * side, width)).astype(BF)
            out_ref[b * side : (b + 1) * side, a * side : (a + 1) * side, :] = swapped.reshape(side, side, width)


def swap_cotangent(array_t):
    first, width, second = array_t.shape
    return pl.pallas_call(
        swap_kernel,
        in_specs=[IN_VMEM],
        out_specs=IN_VMEM,
        out_shape=near((second, first, width)),
        scratch_shapes=[pltpu.VMEM((first, second, width), BF)],
        compiler_params=PARAMS,
        cost_estimate=cost(10**9),
        name="swap_cotangent",
    )(*bring(array_t))


def output_kernel(groups, per, *refs):
    ins, (out_ref, y_ref) = refs[:-2], refs[-2:]
    local, width, feats = out_ref.shape
    pairs = ins[0].shape[1]
    half = feats // groups // per
    lanes = -(-feats // 128) * 128
    side = 16
    swap = swap_matrix(side)

    def rows_of(feature, start):
        at, rest = divmod(feature, half)
        return ins[rest // pairs][at, rest % pairs, start : start + side, :]

    for f in range(0, feats, side):
        for r in range(0, local, side):
            block = jnp.concatenate([rows_of(f + i, r) for i in range(side)], axis=0)
            y_ref[r : r + side, f : f + side, :] = dot(swap, block).astype(BF).reshape(side, side, width)
    for r in range(local):
        y = y_ref[r]
        if lanes > feats:
            y = jnp.concatenate([y, jnp.zeros((lanes - feats, width), BF)], axis=0)
        out_ref[r] = y.T[:, :feats]


def swap_output(chunks, groups, per, feats):
    _, _, local, width = chunks[0].shape
    return pl.pallas_call(
        functools.partial(output_kernel, groups, per),
        in_specs=[IN_VMEM] * len(chunks),
        out_specs=IN_VMEM,
        out_shape=jax.ShapeDtypeStruct((local, width, feats), BF),
        scratch_shapes=[pltpu.VMEM((local, feats, width), BF)],
        compiler_params=PARAMS,
        cost_estimate=cost(10**9),
        name="swap_output",
    )(*bring(*chunks))


def gelu_and_slope(pre):
    size = jnp.abs(pre)
    bell = jnp.exp2(pre * pre * F32(-0.5 * math.log2(math.e)))
    t = 1.0 / (size + F32(ERFC_K))
    poly = F32(ERFC_C[-1])
    for coefficient in ERFC_C[-2::-1]:
        poly = poly * t + F32(coefficient)
    tail = poly * t * bell
    cdf = jnp.where(pre >= 0, 1.0 - tail, tail)
    return pre * cdf, cdf + pre * (bell * F32(1.0 / math.sqrt(2.0 * math.pi)))


def dense_kernel(groups, per, chunk, factor, *refs):
    last = factor is not None
    ins = refs[:groups]
    win_ref, woutt_ref, cot_ref = refs[groups : groups + 3]
    rest = refs[groups + 3 :]
    if chunk > 0:
        prev_in, prev_out = rest[:2]
        rest = rest[2:]
    if last:
        out_ref, grad_ref, n_ref, gin_ref, gout_ref = rest
    else:
        out_ref, gin_ref, gout_ref, n_ref = rest
    pairs, local, _ = ins[0].shape
    width, hid = win_ref.shape
    size = pairs * local
    fg = cot_ref.shape[0] // groups
    half = fg // per
    here = lax.axis_index("cells")
    for m in range(groups):
        for q, part in enumerate(unpack(ins[m][...], per, width)):
            n_ref[m, q * size : (q + 1) * size] = part.reshape(size, width)
    if chunk > 0:
        gin_ref[...] = prev_in[...]
        gout_ref[...] = prev_out[...]
    else:
        gin_ref[...] = jnp.zeros_like(gin_ref)
        gout_ref[...] = jnp.zeros_like(gout_ref)
    w_in = win_ref[...]
    w_out_t = woutt_ref[...]

    def step(b, carry):
        group = here ^ b
        feature = group * fg + chunk * pairs
        normed = n_ref[b]
        cot = [cot_ref[pl.ds(feature + q * half, pairs)].reshape(size, width) for q in range(per)]
        cot = jnp.concatenate(cot, axis=0)
        act, slope = gelu_and_slope(dot(normed, w_in))
        act = act.astype(BF)
        dpre = (dot(cot, w_out_t) * slope).astype(BF)
        result = (normed.astype(F32) + dot(act, w_out_t, NT)).astype(BF)
        for q in range(per):
            out_ref[group * per + q] = result[q * size : (q + 1) * size].reshape(pairs, local, width)
        gin_ref[...] += dot(normed, dpre, TN)
        gout_ref[...] += dot(cot, act, TN)
        return carry

    lax.fori_loop(0, groups, step, 0)
    if last:
        grad_ref[...] = pack(
            [(gin_ref[...].T * F32(factor)).astype(BF), (gout_ref[...].T * F32(factor)).astype(BF)]
        )


def dense_chunk(pieces, cot_t, w_in, w_out_t, prev, groups, per, chunk, factor):
    pairs, local, packed = pieces[0].shape
    width, hid = w_in.shape
    cells = near((groups * per, pairs, local, width))
    partial = near((width, hid), F32)
    operands = list(pieces) + [w_in, w_out_t, cot_t]
    if prev is not None:
        operands += list(prev)
    scratch = [pltpu.VMEM((groups, per * pairs * local, width), BF)]
    if factor is None:
        outs = [cells, partial, partial]
    else:
        outs = [cells, near((hid, 2 * width))]
        scratch += [pltpu.VMEM((width, hid), F32)] * 2
    return pl.pallas_call(
        functools.partial(dense_kernel, groups, per, chunk, factor),
        in_specs=[IN_VMEM] * len(operands),
        out_specs=[IN_VMEM] * len(outs),
        out_shape=outs,
        scratch_shapes=scratch,
        compiler_params=PARAMS,
        cost_estimate=cost(10**10),
        name=f"dense_{chunk}",
    )(*bring(*operands))


def exchange(pieces, groups):
    return [pieces[0]] + [
        lax.ppermute(pieces[m], "cells", [(s, s ^ m) for s in range(groups)]) for m in range(1, groups)
    ]


def per_device(
    cells_in, train_count, feat_count, feat_qkv, feat_proj, row_qkv, row_proj, w_in, w_out, cotangent
):
    block_t = jnp.swapaxes(cells_in[0], 1, 2)
    local, width, feats = block_t.shape
    groups = lax.axis_size("cells")
    tables = lax.axis_size("tables")
    fg = feats // groups
    per = 2 if fg % 2 == 0 else 1
    half = fg // per
    sub_rows = 16
    row_chunks = local // sub_rows
    feat_chunks = 2 if half % 2 == 0 else 1
    factor = 1.0 / math.sqrt(tables * local * groups * feats)
    pairs = half // feat_chunks
    pieces = [[] for _ in range(feat_chunks)]
    firsts = []
    for k in range(row_chunks):
        cuts = feat_chunks if k == row_chunks - 1 else 1
        sent = feature_chunk(block_t, feat_count, feat_qkv, feat_proj, groups, per, k, sub_rows, cuts)
        come = [exchange(sent[c * groups : (c + 1) * groups], groups) for c in range(cuts)]
        for j in range(feat_chunks):
            pieces[j] += come[j % cuts]
        firsts.append(cuts == 1)
    cot_t = swap_cotangent(jnp.swapaxes(cotangent[0], 1, 2))
    back = []
    for j in range(feat_chunks):
        starts = tuple(j * pairs if whole else 0 for whole in firsts)
        done = row_chunk(
            pieces[j], train_count, row_qkv, row_proj, groups, per, row_chunks, j, pairs, starts
        )
        back.append(exchange(done, groups))
    outs = []
    grads = None
    for j in range(feat_chunks):
        out_j, *grads = dense_chunk(
            back[j], cot_t, w_in, w_out.T, grads, groups, per, j, factor if j == feat_chunks - 1 else None
        )
        outs.append(out_j)
    output = jnp.swapaxes(swap_output(outs, groups, per, feats), 1, 2)
    pieces = grads[0].reshape(tables * groups, -1, 2 * width)
    total = lax.all_to_all(pieces, ("tables", "cells"), split_axis=0, concat_axis=0, tiled=True)
    total = jnp.sum(total.astype(F32), axis=0)
    grad_in, grad_out = unpack(total, 2, width)
    return (output[None], grad_in.T, grad_out)


def solution(mesh):
    spread = P("tables", "cells", None, None)
    return jax.shard_map(
        per_device,
        mesh=mesh,
        in_specs=(spread, P("tables"), P("tables"), P(), P(), P(), P(), P(), P(), spread),
        out_specs=(spread, P(None, ("tables", "cells")), P(("tables", "cells"), None)),
        check_vma=False,
    )
```

```python
import functools
import math

import jax
import jax.numpy as jnp
from jax import lax
from jax.experimental import pallas as pl
from jax.experimental.pallas import tpu as pltpu
from jax.sharding import PartitionSpec as P


HEADS = 6
HEAD_DIM = 32
BF = jnp.bfloat16
F32 = jnp.float32
ERFC_K = 3.5
ERFC_C = (
    0.4096238545958983,
    1.030471715475736,
    9.637057789606283,
    -24.75291485624482,
    177.3359613786631,
    -181.2859739558248,
)
NT = (((1,), (1,)), ((), ()))
TN = (((0,), (0,)), ((), ()))


def dot(a, b, dims=(((1,), (0,)), ((), ()))):
    return lax.dot_general(a, b, dims, preferred_element_type=F32)


def layer_norm(values):
    mean = jnp.mean(values, axis=0, keepdims=True)
    centred = values - mean
    var = jnp.mean(centred * centred, axis=0, keepdims=True)
    return centred * lax.rsqrt(var + 1e-05)


def one_hot(rows, cols):
    row = lax.broadcasted_iota(jnp.int32, (rows, cols), 0)
    col = lax.broadcasted_iota(jnp.int32, (rows, cols), 1)
    return (row == col).astype(F32).astype(BF)


def finish_items(att_ref, ats, w_proj_t, flip, residual_t):
    lanes = att_ref.shape[2]
    mixed = dot(w_proj_t, jnp.concatenate([att_ref[at] for at in ats], axis=1))
    done = []
    for a, at in enumerate(ats):
        normed = layer_norm(residual_t(at).astype(F32) + mixed[:, a * lanes : (a + 1) * lanes]).astype(BF)
        done.append(dot(flip, normed, NT).astype(BF))
    return done


def swap_matrix(side):
    out = lax.broadcasted_iota(jnp.int32, (side * side, side * side), 0)
    src = lax.broadcasted_iota(jnp.int32, (side * side, side * side), 1)
    return (src == (out % side) * side + out // side).astype(F32).astype(BF)


def pack(parts):
    if len(parts) == 1:
        return parts[0]
    a, b = parts
    cut = a.shape[-1] // 128 * 128
    return jnp.concatenate([a[..., :cut], b[..., :cut], a[..., cut:], b[..., cut:]], axis=-1)


def unpack(block, per, width):
    if per == 1:
        return [block]
    cut = width // 128 * 128
    rest = width - cut
    return [
        jnp.concatenate(
            [block[..., q * cut : (q + 1) * cut], block[..., 2 * cut + q * rest : 2 * cut + (q + 1) * rest]],
            axis=-1,
        )
        for q in range(2)
    ]


CELLS = ("chips", "core")


def cell_index():
    return lax.axis_index("chips") * 2 + lax.axis_index("core")


def mask_of(keys, count):
    rows = lax.broadcasted_iota(jnp.int32, (keys, 1), 0) < count
    lanes = lax.broadcasted_iota(jnp.int32, (1, keys), 1) < count
    return rows, lanes


def keep_projected(refs, at, q_v, k_rows, masks):
    q_ref, k_ref, v_ref = refs
    width, keys = q_ref.shape[1], k_ref.shape[1]
    key_row, key_lane = masks
    scale = F32(math.log2(math.e) / math.sqrt(HEAD_DIM))
    q_ref[at] = (q_v[:width] * scale).astype(BF)
    v_ref[at] = jnp.where(key_lane, q_v[width:, :keys], F32(0)).astype(BF)
    k_ref[at] = jnp.where(key_row, k_rows[:keys], k_rows[0:1]).astype(BF)


def score_blocks(q_own, lanes):
    hd = HEAD_DIM
    width = q_own.shape[0]
    blank = jnp.zeros((hd, lanes), BF)
    blocks = []
    for i in range(HEADS // 2):
        lo = 2 * i * hd
        tile = lo // 128 * 128
        end = min(tile + 128, width)
        pieces = [
            jnp.concatenate([q_own[lo : lo + hd], blank], axis=1),
            jnp.concatenate([blank, q_own[lo + hd : lo + 2 * hd]], axis=1),
        ]
        if lo > tile:
            pieces = [jnp.zeros((lo - tile, 2 * lanes), BF)] + pieces
        if lo + 2 * hd < end:
            pieces = pieces + [jnp.zeros((end - lo - 2 * hd, 2 * lanes), BF)]
        blocks.append((tile, end, jnp.concatenate(pieces, axis=0)))
    return blocks


def attend(refs, att_ref, ats, ones):
    q_ref, k_ref, v_ref = refs
    lanes = q_ref.shape[2]
    hd = HEAD_DIM
    scores = []
    for at in ats:
        k_own = k_ref[at]
        for tile, end, block in score_blocks(q_ref[at], lanes):
            scores.append(dot(k_own[:, tile:end], block))
    weights = [jnp.exp2(s - jnp.max(s, axis=0, keepdims=True)).astype(BF) for s in scores]
    for n, at in enumerate(ats):
        v_own = v_ref[at]
        for i in range(HEADS // 2):
            lo = 2 * i * hd
            lhs = jnp.concatenate([v_own[lo : lo + 2 * hd], ones], axis=0)
            mixed = dot(lhs, weights[n * (HEADS // 2) + i])
            scale = 1.0 / mixed[2 * hd : 2 * hd + 1]
            att_ref[at, lo : lo + hd] = (mixed[:hd, :lanes] * scale[:, :lanes]).astype(BF)
            att_ref[at, lo + hd : lo + 2 * hd] = (mixed[hd : 2 * hd, lanes:] * scale[:, lanes:]).astype(BF)


def loop(count, most, body):
    group = max(d for d in range(1, most + 1) if count % d == 0)

    def step(i, carry):
        body([i * group + a for a in range(group)])
        return carry

    lax.fori_loop(0, count // group, step, 0)


def pad_lanes(value, lanes):
    rows, n = value.shape
    return value if n == lanes else jnp.concatenate([value, jnp.zeros((rows, lanes - n), value.dtype)], axis=1)


def feature_kernel(groups, per, first, rows, cuts, count_ref, cells_ref, wqkv_ref, wproj_ref, *refs):
    outs = refs[: groups * cuts]
    q_ref, k_ref, v_ref, att_ref, mid_ref, swap_ref = refs[groups * cuts :]
    _, width, feats = cells_ref.shape
    lanes = q_ref.shape[2]
    fg = feats // groups
    half = fg // per
    count = count_ref[0]
    w_t = wqkv_ref[...].T
    w_qv = jnp.concatenate([w_t[:width], w_t[2 * width :]], axis=0)
    w_k = w_t[width : 2 * width]
    w_proj_t = wproj_ref[...].T
    flip = one_hot(feats, lanes)
    masks = mask_of(feats, count)
    ones = jnp.broadcast_to(jnp.where(masks[1], F32(1), F32(0)), (16, feats)).astype(BF)
    kept = (q_ref, k_ref, v_ref)

    def project(ats):
        x_t = [pad_lanes(cells_ref[first + at], lanes) for at in ats]
        q_v = dot(w_qv, jnp.concatenate(x_t, axis=1))
        x = [t.T[:feats] for t in x_t]
        k = dot(jnp.concatenate(x, axis=0), w_k, NT)
        for a, at in enumerate(ats):
            keep_projected(kept, at, q_v[:, a * lanes : (a + 1) * lanes], k[a * feats : (a + 1) * feats], masks)

    def finish(ats):
        own = lambda at: pad_lanes(cells_ref[first + at], lanes)
        for at, value in zip(ats, finish_items(att_ref, ats, w_proj_t, flip, own)):
            mid_ref[at] = value

    loop(rows, 8, project)
    loop(rows, 8, lambda ats: attend(kept, att_ref, ats, ones))
    loop(rows, 8, finish)
    swap = swap_matrix(rows)
    for f in range(feats // rows):
        block = mid_ref[:, f * rows : (f + 1) * rows, :].reshape(rows * rows, width)
        swap_ref[f * rows : (f + 1) * rows] = dot(swap, block).astype(BF).reshape(rows, rows, width)
    here = cell_index()
    size = half // cuts
    for c in range(cuts):
        for m in range(groups):
            base = (here ^ m) * fg + c * size
            outs[c * groups + m][...] = pack([swap_ref[pl.ds(base + q * half, size)] for q in range(per)])


IN_VMEM = pl.BlockSpec(memory_space=pltpu.VMEM)
IN_SMEM = pl.BlockSpec(memory_space=pltpu.SMEM)


def attention_scratch(items, width, lanes, keys):
    return [
        pltpu.VMEM((items, width, lanes), BF),
        pltpu.VMEM((items, keys, width), BF),
        pltpu.VMEM((items, width, keys), BF),
        pltpu.VMEM((items, width, lanes), BF),
    ]


def near(shape, dtype=BF):
    return pltpu.VMEM(shape, dtype)


def bring(*arrays):
    return [pltpu.with_memory_space_constraint(x, pltpu.VMEM) for x in arrays]


PARAMS = pltpu.CompilerParams(vmem_limit_bytes=14 * 2**20)


def cost(flops):
    return pl.CostEstimate(flops=flops, transcendentals=0, bytes_accessed=10**6)


def feature_chunk(block_t, count, wqkv, wproj, groups, per, chunk, rows, cuts):
    _, width, feats = block_t.shape
    half = feats // groups // per
    lanes = -(-feats // 128) * 128
    operands = [block_t, wqkv, wproj]
    if chunk == 0:
        base, specs = 0, [pl.BlockSpec((rows, width, feats), lambda i: (0, 0, 0)), IN_VMEM, IN_VMEM]
        operands = [pltpu.with_memory_space_constraint(x, pltpu.HBM) for x in operands]
    else:
        base, specs = chunk * rows, [IN_VMEM] * 3
        operands = bring(*operands)
    return pl.pallas_call(
        functools.partial(feature_kernel, groups, per, base, rows, cuts),
        grid=(1,),
        in_specs=[IN_SMEM] + specs,
        out_specs=[IN_VMEM] * (groups * cuts),
        out_shape=[near((half // cuts, rows, per * width))] * (groups * cuts),
        scratch_shapes=attention_scratch(rows, width, lanes, feats)
        + [pltpu.VMEM((rows, feats, width), BF), pltpu.VMEM((feats, rows, width), BF)],
        compiler_params=PARAMS,
        cost_estimate=cost(10**8),
    )(count, *operands)


def row_kernel(groups, per, chunks, firsts, count_ref, wqkv_ref, wproj_ref, *refs):
    ins = refs[: groups * chunks]
    outs = refs[groups * chunks : groups * chunks + groups]
    q_ref, k_ref, v_ref, att_ref, x_ref, xt_ref, y_ref = refs[groups * chunks + groups :]
    pairs, local, _ = outs[0].shape
    sub_rows = local // chunks
    items, rows, width = x_ref.shape
    keys = k_ref.shape[1]
    count = count_ref[0]
    w_t = wqkv_ref[...].T
    w_qv = jnp.concatenate([w_t[:width], w_t[2 * width :], one_hot(width, width)], axis=0)
    w_k = w_t[width : 2 * width]
    w_proj_t = wproj_ref[...].T
    flip = one_hot(rows, rows)
    masks = mask_of(keys, count)
    ones = jnp.broadcast_to(jnp.where(masks[1], F32(1), F32(0)), (16, keys)).astype(BF)
    kept = (q_ref, k_ref, v_ref)
    here = cell_index()
    for m in range(groups):
        for k in range(chunks):
            at = pl.multiple_of((here ^ m) * local + k * sub_rows, sub_rows)
            for q, part in enumerate(unpack(ins[k * groups + m][firsts[k] : firsts[k] + pairs], per, width)):
                x_ref[q * pairs : (q + 1) * pairs, pl.ds(at, sub_rows), :] = part

    def project(ats):
        x = jnp.concatenate([x_ref[at] for at in ats], axis=0)
        q_v = dot(w_qv, x, NT)
        for a, at in enumerate(ats):
            k = dot(x[a * rows : a * rows + keys], w_k, NT)
            own = q_v[:, a * rows : (a + 1) * rows]
            xt_ref[at] = own[2 * width :].astype(BF)
            keep_projected(kept, at, own[: 2 * width], k, masks)

    def finish(ps):
        ats = [q * pairs + p for p in ps for q in range(per)]
        done = finish_items(att_ref, ats, w_proj_t, flip, lambda at: xt_ref[at])
        for a, p in enumerate(ps):
            y_ref[p] = pack(done[a * per : (a + 1) * per])

    most = max(1, 1024 // rows)
    loop(items, min(most, 7), project)
    loop(items, min(most, 7), lambda ats: attend(kept, att_ref, ats, ones))
    loop(pairs, min(most, 7), finish)
    for m in range(groups):
        at = pl.multiple_of((here ^ m) * local, local)
        outs[m][...] = y_ref[:, pl.ds(at, local), :]


def row_chunk(pieces, count, wqkv, wproj, groups, per, chunks, pairs, firsts):
    sub_rows, packed = pieces[0].shape[1:]
    width = wproj.shape[0]
    local = sub_rows * chunks
    rows = local * groups
    keys = rows - rows // 4
    return pl.pallas_call(
        functools.partial(row_kernel, groups, per, chunks, firsts),
        in_specs=[IN_SMEM] + [IN_VMEM] * (2 + len(pieces)),
        out_specs=[IN_VMEM] * groups,
        out_shape=[near((pairs, local, packed))] * groups,
        scratch_shapes=attention_scratch(pairs * per, width, rows, keys)
        + [
            pltpu.VMEM((pairs * per, rows, width), BF),
            pltpu.VMEM((pairs * per, width, rows), BF),
            pltpu.VMEM((pairs, rows, packed), BF),
        ],
        compiler_params=PARAMS,
        cost_estimate=cost(10**8),
    )(count, *bring(wqkv, wproj, *pieces))


def swap_kernel(in_ref, out_ref, x_ref):
    first, width, second = in_ref.shape
    lanes = -(-second // 128) * 128
    side = 16
    swap = swap_matrix(side)
    for a in range(first):
        x_ref[a] = pad_lanes(in_ref[a], lanes).T[:second]
    for a in range(first // side):
        for b in range(second // side):
            block = x_ref[a * side : (a + 1) * side, b * side : (b + 1) * side, :]
            swapped = dot(swap, block.reshape(side * side, width)).astype(BF)
            out_ref[b * side : (b + 1) * side, a * side : (a + 1) * side, :] = swapped.reshape(side, side, width)


def swap_cotangent(array_t):
    first, width, second = array_t.shape
    return pl.pallas_call(
        swap_kernel,
        in_specs=[IN_VMEM],
        out_specs=IN_VMEM,
        out_shape=near((second, first, width)),
        scratch_shapes=[pltpu.VMEM((first, second, width), BF)],
        compiler_params=PARAMS,
        cost_estimate=cost(10**8),
        name="swap_cotangent",
    )(*bring(array_t))


def output_kernel(groups, per, chunks, *refs):
    parts, (out_ref, f_ref, y_ref) = refs[:-3], refs[-3:]
    feats, local, width = f_ref.shape
    half = feats // groups // per
    pairs = half // chunks
    size = pairs * local
    lanes = -(-feats // 128) * 128
    here = cell_index()
    count = parts[0].shape[0]
    for n, part in enumerate(parts):
        for b in range(count):
            at = n * count + b
            base = (here ^ (at // chunks)) * (half * per) + (at % chunks) * pairs
            for q in range(per):
                rows = part[b, q * size : (q + 1) * size].reshape(pairs, local, width)
                f_ref[pl.ds(base + q * half, pairs)] = rows
    side = 16
    swap = swap_matrix(side)
    for f in range(0, feats, side):
        for r in range(0, local, side):
            block = f_ref[f : f + side, r : r + side, :].reshape(side * side, width)
            y_ref[r : r + side, f : f + side, :] = dot(swap, block).astype(BF).reshape(side, side, width)
    for r in range(local):
        y = y_ref[r]
        if lanes > feats:
            y = jnp.concatenate([y, jnp.zeros((lanes - feats, width), BF)], axis=0)
        out_ref[r] = y.T[:, :feats]


def make_output(parts, groups, per, chunks, feats, local):
    width = parts[0].shape[-1]
    return pl.pallas_call(
        functools.partial(output_kernel, groups, per, chunks),
        in_specs=[IN_VMEM] * len(parts),
        out_specs=IN_VMEM,
        out_shape=jax.ShapeDtypeStruct((local, width, feats), BF),
        scratch_shapes=[pltpu.VMEM((feats, local, width), BF), pltpu.VMEM((local, feats, width), BF)],
        compiler_params=PARAMS,
        cost_estimate=cost(10**8),
        name="make_output",
    )(*bring(*parts))


def gelu_and_slope(pre):
    size = jnp.abs(pre)
    bell = jnp.exp2(pre * pre * F32(-0.5 * math.log2(math.e)))
    t = 1.0 / (size + F32(ERFC_K))
    poly = F32(ERFC_C[-1])
    for coefficient in ERFC_C[-2::-1]:
        poly = poly * t + F32(coefficient)
    tail = poly * t * bell
    cdf = jnp.where(pre >= 0, 1.0 - tail, tail)
    return pre * cdf, cdf + pre * (bell * F32(1.0 / math.sqrt(2.0 * math.pi)))


def dense_kernel(groups, per, chunks, first, factor, *refs):
    last = factor is not None
    blocks = refs[-1].shape[0]
    ins = refs[:blocks]
    win_ref, woutt_ref, cot_ref = refs[blocks : blocks + 3]
    rest = refs[blocks + 3 :]
    if first > 0:
        prev_in, prev_out = rest[:2]
        rest = rest[2:]
    if last:
        out_ref, keep_ref, send_ref, gin_ref, gout_ref, n_ref = rest
    else:
        out_ref, gin_ref, gout_ref, n_ref = rest
    pairs, local, _ = ins[0].shape
    width, _ = win_ref.shape
    size = pairs * local
    fg = cot_ref.shape[0] // groups
    half = fg // per
    here = cell_index()
    for b in range(blocks):
        for q, part in enumerate(unpack(ins[b][...], per, width)):
            n_ref[b, q * size : (q + 1) * size] = part.reshape(size, width)
    if first > 0:
        gin_ref[...] = prev_in[...]
        gout_ref[...] = prev_out[...]
    else:
        gin_ref[...] = jnp.zeros_like(gin_ref)
        gout_ref[...] = jnp.zeros_like(gout_ref)
    w_in = win_ref[...]
    w_out_t = woutt_ref[...]

    def step(b, carry):
        at = first + b
        feature = (here ^ (at // chunks)) * fg + (at % chunks) * pairs
        normed = n_ref[b]
        cot = [cot_ref[pl.ds(feature + q * half, pairs)].reshape(size, width) for q in range(per)]
        cot = jnp.concatenate(cot, axis=0)
        act, slope = gelu_and_slope(dot(normed, w_in))
        act = act.astype(BF)
        out_ref[b] = (normed.astype(F32) + dot(act, w_out_t, NT)).astype(BF)
        dpre = (dot(cot, w_out_t) * slope).astype(BF)
        gin_ref[...] += dot(normed, dpre, TN)
        gout_ref[...] += dot(cot, act, TN)
        return carry

    lax.fori_loop(0, blocks, step, 0)
    if last:
        both = pack([(gin_ref[...].T * F32(factor)).astype(BF), (gout_ref[...].T * F32(factor)).astype(BF)])
        both = both.reshape(keep_ref.shape[0], 2, *keep_ref.shape[1:])
        even = here % 2 == 0
        keep_ref[...] = jnp.where(even, both[:, 0], both[:, 1])
        send_ref[...] = jnp.where(even, both[:, 1], both[:, 0])


def dense_part(blocks, cot_t, w_in, w_out_t, prev, groups, per, chunks, first, factor, shares):
    pairs, local, _ = blocks[0].shape
    width, hid = w_in.shape
    size = per * pairs * local
    count = len(blocks)
    outs = [near((count, size, width))]
    operands = list(blocks) + [w_in, w_out_t, cot_t]
    if first > 0:
        operands += list(prev)
    scratch = []
    if factor is None:
        outs += [near((width, hid), F32)] * 2
    else:
        outs += [near((shares // 2, hid // shares, 2 * width))] * 2
        scratch = [pltpu.VMEM((width, hid), F32)] * 2
    scratch += [pltpu.VMEM((count, size, width), BF)]
    return pl.pallas_call(
        functools.partial(dense_kernel, groups, per, chunks, first, factor),
        in_specs=[IN_VMEM] * len(operands),
        out_specs=[IN_VMEM] * len(outs),
        out_shape=outs,
        scratch_shapes=scratch,
        compiler_params=PARAMS,
        cost_estimate=cost(10**8),
    )(*bring(*operands))


def add_kernel(a_ref, b_ref, out_ref):
    out_ref[...] = (a_ref[...].astype(F32) + b_ref[...].astype(F32)).astype(BF)


def add_pair(a, b):
    return pl.pallas_call(
        add_kernel,
        in_specs=[IN_VMEM] * 2,
        out_specs=IN_VMEM,
        out_shape=jax.ShapeDtypeStruct(a.shape, BF),
        compiler_params=PARAMS,
        cost_estimate=cost(10**6),
        name="add_pair",
    )(*bring(a, b))


def exchange(pieces, groups):
    come = [pieces[0]]
    for m in range(1, groups):
        come.append(lax.ppermute(pieces[m], CELLS, [(s, s ^ m) for s in range(groups)]))
    return come


def per_device(
    cells_in, train_count, feat_count, feat_qkv, feat_proj, row_qkv, row_proj, w_in, w_out, cotangent
):
    block_t = jnp.swapaxes(cells_in[0], 1, 2)
    local, width, feats = block_t.shape
    groups = lax.axis_size(CELLS)
    tables = lax.axis_size("tables")
    fg = feats // groups
    per = 2 if fg % 2 == 0 else 1
    half = fg // per
    sub_rows = 16
    row_chunks = local // sub_rows
    feat_chunks = 2 if half % 2 == 0 else 1
    factor = 1.0 / math.sqrt(tables * local * groups * feats)
    pairs = half // feat_chunks
    pieces = [[] for _ in range(feat_chunks)]
    firsts = []
    for k in range(row_chunks):
        cuts = feat_chunks if k == row_chunks - 1 else 1
        sent = feature_chunk(block_t, feat_count, feat_qkv, feat_proj, groups, per, k, sub_rows, cuts)
        come = [exchange(sent[c * groups : (c + 1) * groups], groups) for c in range(cuts)]
        for j in range(feat_chunks):
            pieces[j] += come[j % cuts]
        firsts.append(cuts == 1)
    cot_t = swap_cotangent(jnp.swapaxes(cotangent[0], 1, 2))
    back = []
    for j in range(feat_chunks):
        starts = tuple(j * pairs if whole else 0 for whole in firsts)
        done = row_chunk(pieces[j], train_count, row_qkv, row_proj, groups, per, row_chunks, pairs, starts)
        back.append(exchange(done, groups))
    w_out_t = w_out.T
    shares = tables * groups
    blocks = [back[j][m] for m in range(groups) for j in range(feat_chunks)]
    cut = len(blocks) // 2
    args = (cot_t, w_in, w_out_t)
    shape = (groups, per, feat_chunks)
    out_0, *partial = dense_part(blocks[:cut], *args, None, *shape, 0, None, shares)
    out_1, keep, send = dense_part(blocks[cut:], *args, partial, *shape, cut, factor, shares)
    other = lax.ppermute(send, "core", [(0, 1), (1, 0)])
    pieces = add_pair(keep, other)
    total = lax.all_to_all(pieces, ("tables", "chips"), split_axis=0, concat_axis=0, tiled=True)
    total = jnp.sum(total.astype(F32), axis=0)
    output = make_output([out_0, out_1], *shape, feats, local)
    grad_in, grad_out = unpack(total, 2, width)
    return (jnp.swapaxes(output, 1, 2)[None], grad_in.T, grad_out)


def solution(mesh):
    tables, cells = mesh.devices.shape
    split = jax.sharding.Mesh(mesh.devices.reshape(tables, cells // 2, 2), ("tables", "chips", "core"))
    spread = P("tables", CELLS, None, None)
    shares = ("tables",) + CELLS
    return jax.shard_map(
        per_device,
        mesh=split,
        in_specs=(spread, P("tables"), P("tables"), P(), P(), P(), P(), P(), P(), spread),
        out_specs=(spread, P(None, shares), P(shares, None)),
        check_vma=False,
    )
```

```python
import functools
import math

import jax
import jax.numpy as jnp
from jax import lax
from jax.experimental import pallas as pl
from jax.experimental.pallas import tpu as pltpu
from jax.sharding import PartitionSpec as P


HEADS = 6
HEAD_DIM = 32
BF = jnp.bfloat16
F32 = jnp.float32
ERFC_K = 2.9
ERFC_C = (
    0.38553786502648235,
    1.4917549496141058,
    -0.32977430445565825,
    21.663540536082817,
    -21.146073738657215,
)
NT = (((1,), (1,)), ((), ()))
TN = (((0,), (0,)), ((), ()))


def dot(a, b, dims=(((1,), (0,)), ((), ()))):
    return lax.dot_general(a, b, dims, preferred_element_type=F32)


def layer_norm(values):
    mean = jnp.mean(values, axis=0, keepdims=True)
    centred = values - mean
    var = jnp.mean(centred * centred, axis=0, keepdims=True)
    return centred * lax.rsqrt(var + 1e-05)


def one_hot(rows, cols):
    row = lax.broadcasted_iota(jnp.int32, (rows, cols), 0)
    col = lax.broadcasted_iota(jnp.int32, (rows, cols), 1)
    return (row == col).astype(F32).astype(BF)


def finish_items(att_ref, ats, w_proj_t, flip, residual_t):
    lanes = att_ref.shape[2]
    mixed = dot(w_proj_t, jnp.concatenate([att_ref[at] for at in ats], axis=1))
    done = []
    for a, at in enumerate(ats):
        normed = layer_norm(residual_t(at).astype(F32) + mixed[:, a * lanes : (a + 1) * lanes]).astype(BF)
        done.append(dot(flip, normed, NT).astype(BF))
    return done


def swap_matrix(side):
    out = lax.broadcasted_iota(jnp.int32, (side * side, side * side), 0)
    src = lax.broadcasted_iota(jnp.int32, (side * side, side * side), 1)
    return (src == (out % side) * side + out // side).astype(F32).astype(BF)


def pack(parts):
    if len(parts) == 1:
        return parts[0]
    a, b = parts
    cut = a.shape[-1] // 128 * 128
    return jnp.concatenate([a[..., :cut], b[..., :cut], a[..., cut:], b[..., cut:]], axis=-1)


def unpack(block, per, width):
    if per == 1:
        return [block]
    cut = width // 128 * 128
    rest = width - cut
    return [
        jnp.concatenate(
            [block[..., q * cut : (q + 1) * cut], block[..., 2 * cut + q * rest : 2 * cut + (q + 1) * rest]],
            axis=-1,
        )
        for q in range(2)
    ]


CELLS = ("chips", "core")


def cell_index():
    return lax.axis_index("chips") * 2 + lax.axis_index("core")


def mask_of(keys, count):
    rows = lax.broadcasted_iota(jnp.int32, (keys, 1), 0) < count
    lanes = lax.broadcasted_iota(jnp.int32, (1, keys), 1) < count
    return rows, lanes


def keep_projected(refs, at, q_v, k_rows, masks):
    q_ref, k_ref, v_ref = refs
    width, keys = q_ref.shape[1], k_ref.shape[1]
    key_row, key_lane = masks
    scale = F32(math.log2(math.e) / math.sqrt(HEAD_DIM))
    q_ref[at] = (q_v[:width] * scale).astype(BF)
    v_ref[at] = jnp.where(key_lane, q_v[width:, :keys], F32(0)).astype(BF)
    k_ref[at] = jnp.where(key_row, k_rows[:keys], k_rows[0:1]).astype(BF)


def score_blocks(q_own, lanes):
    hd = HEAD_DIM
    width = q_own.shape[0]
    blank = jnp.zeros((hd, lanes), BF)
    blocks = []
    for i in range(HEADS // 2):
        lo = 2 * i * hd
        tile = lo // 128 * 128
        end = min(tile + 128, width)
        pieces = [
            jnp.concatenate([q_own[lo : lo + hd], blank], axis=1),
            jnp.concatenate([blank, q_own[lo + hd : lo + 2 * hd]], axis=1),
        ]
        if lo > tile:
            pieces = [jnp.zeros((lo - tile, 2 * lanes), BF)] + pieces
        if lo + 2 * hd < end:
            pieces = pieces + [jnp.zeros((end - lo - 2 * hd, 2 * lanes), BF)]
        blocks.append((tile, end, jnp.concatenate(pieces, axis=0)))
    return blocks


def attend(refs, att_ref, ats, ones):
    q_ref, k_ref, v_ref = refs
    lanes = q_ref.shape[2]
    hd = HEAD_DIM
    scores = []
    for at in ats:
        k_own = k_ref[at]
        for tile, end, block in score_blocks(q_ref[at], lanes):
            scores.append(dot(k_own[:, tile:end], block))
    weights = [jnp.exp2(s - jnp.max(s, axis=0, keepdims=True)).astype(BF) for s in scores]
    for n, at in enumerate(ats):
        v_own = v_ref[at]
        for i in range(HEADS // 2):
            lo = 2 * i * hd
            lhs = jnp.concatenate([v_own[lo : lo + 2 * hd], ones], axis=0)
            mixed = dot(lhs, weights[n * (HEADS // 2) + i])
            scale = 1.0 / mixed[2 * hd : 2 * hd + 1]
            att_ref[at, lo : lo + hd] = (mixed[:hd, :lanes] * scale[:, :lanes]).astype(BF)
            att_ref[at, lo + hd : lo + 2 * hd] = (mixed[hd : 2 * hd, lanes:] * scale[:, lanes:]).astype(BF)


def loop(count, most, body):
    group = max(d for d in range(1, most + 1) if count % d == 0)

    def step(i, carry):
        body([i * group + a for a in range(group)])
        return carry

    lax.fori_loop(0, count // group, step, 0)


def pad_lanes(value, lanes):
    rows, n = value.shape
    return value if n == lanes else jnp.concatenate([value, jnp.zeros((rows, lanes - n), value.dtype)], axis=1)


def feature_kernel(groups, per, first, rows, cuts, count_ref, cells_ref, wqkv_ref, wproj_ref, *refs):
    outs = refs[: groups * cuts]
    refs = refs[groups * cuts :]
    parts = 2 if first == 0 else 1
    waits = [[] for _ in range(parts)]
    if first == 0:
        sems, wqkv_buf, wproj_buf, cells_buf = refs[6:]
        refs = refs[:6]
        step = rows // parts
        moves = [(wqkv_ref, wqkv_buf), (wproj_ref, wproj_buf)]
        for n in range(parts):
            moves.append((cells_ref.at[pl.ds(n * step, step)], cells_buf.at[pl.ds(n * step, step)]))
        moves = [pltpu.make_async_copy(a, b, sems.at[n]) for n, (a, b) in enumerate(moves)]
        for move in moves:
            move.start()
        for move in moves[:2]:
            move.wait()
        waits = [[move] for move in moves[2:]]
        wqkv_ref, wproj_ref, cells_ref = wqkv_buf, wproj_buf, cells_buf
    count = count_ref[0]
    q_ref, k_ref, v_ref, att_ref, mid_ref, swap_ref = refs
    _, width, feats = cells_ref.shape
    lanes = q_ref.shape[2]
    fg = feats // groups
    half = fg // per
    w_t = wqkv_ref[...].T
    w_qv = jnp.concatenate([w_t[:width], w_t[2 * width :]], axis=0)
    w_k = w_t[width : 2 * width]
    w_proj_t = wproj_ref[...].T
    flip = one_hot(feats, lanes)
    masks = mask_of(feats, count)
    ones = jnp.broadcast_to(jnp.where(masks[1], F32(1), F32(0)), (16, feats)).astype(BF)
    kept = (q_ref, k_ref, v_ref)

    def project(ats):
        x_t = [pad_lanes(cells_ref[first + at], lanes) for at in ats]
        q_v = dot(w_qv, jnp.concatenate(x_t, axis=1))
        x = [t.T[:feats] for t in x_t]
        k = dot(jnp.concatenate(x, axis=0), w_k, NT)
        for a, at in enumerate(ats):
            keep_projected(kept, at, q_v[:, a * lanes : (a + 1) * lanes], k[a * feats : (a + 1) * feats], masks)

    def finish(ats):
        own = lambda at: pad_lanes(cells_ref[first + at], lanes)
        for at, value in zip(ats, finish_items(att_ref, ats, w_proj_t, flip, own)):
            mid_ref[at] = value

    for n, moves in enumerate(waits):
        for move in moves:
            move.wait()
        step = rows // parts
        project(list(range(n * step, (n + 1) * step)))
    loop(rows, 8, lambda ats: attend(kept, att_ref, ats, ones))
    loop(rows, 16, finish)
    swap = swap_matrix(rows)
    for f in range(feats // rows):
        block = mid_ref[:, f * rows : (f + 1) * rows, :].reshape(rows * rows, width)
        swap_ref[f * rows : (f + 1) * rows] = dot(swap, block).astype(BF).reshape(rows, rows, width)
    here = cell_index()
    size = half // cuts
    for c in range(cuts):
        for m in range(groups):
            base = (here ^ m) * fg + c * size
            outs[c * groups + m][...] = pack([swap_ref[pl.ds(base + q * half, size)] for q in range(per)])


BLOCKS = 2
IN_VMEM = pl.BlockSpec(memory_space=pltpu.VMEM)
IN_SMEM = pl.BlockSpec(memory_space=pltpu.SMEM)


def attention_scratch(items, width, lanes, keys):
    return [
        pltpu.VMEM((items, width, lanes), BF),
        pltpu.VMEM((items, keys, width), BF),
        pltpu.VMEM((items, width, keys), BF),
        pltpu.VMEM((items, width, lanes), BF),
    ]


def near(shape, dtype=BF):
    return pltpu.VMEM(shape, dtype)


def bring(*arrays):
    return [pltpu.with_memory_space_constraint(x, pltpu.VMEM) for x in arrays]


PARAMS = pltpu.CompilerParams(vmem_limit_bytes=14 * 2**20)


def cost(flops):
    return pl.CostEstimate(flops=flops, transcendentals=0, bytes_accessed=10**6)


def feature_chunk(block_t, count, wqkv, wproj, groups, per, chunk, rows, cuts):
    _, width, feats = block_t.shape
    half = feats // groups // per
    lanes = -(-feats // 128) * 128
    outs = [near((half // cuts, rows, per * width))] * (groups * cuts)
    scratch = attention_scratch(rows, width, lanes, feats)
    scratch += [pltpu.VMEM((rows, feats, width), BF), pltpu.VMEM((feats, rows, width), BF)]
    operands = [block_t, wqkv, wproj]
    if chunk == 0:
        operands = [pltpu.with_memory_space_constraint(x, pltpu.HBM) for x in operands]
        specs = [pl.BlockSpec(memory_space=pltpu.HBM)] * 3
        scratch += [pltpu.SemaphoreType.DMA((4,))]
        scratch += [pltpu.VMEM(x.shape, BF) for x in (wqkv, wproj)]
        scratch += [pltpu.VMEM((rows, width, feats), BF)]
    else:
        operands = bring(*operands)
        specs = [IN_VMEM] * 3
    return pl.pallas_call(
        functools.partial(feature_kernel, groups, per, chunk * rows, rows, cuts),
        in_specs=[IN_SMEM] + specs,
        out_specs=[IN_VMEM] * len(outs),
        out_shape=outs,
        scratch_shapes=scratch,
        compiler_params=PARAMS,
        cost_estimate=cost(10**8),
    )(count, *operands)


def row_kernel(groups, per, chunks, firsts, count_ref, wqkv_ref, wproj_ref, *refs):
    ins = refs[: groups * chunks]
    outs = refs[groups * chunks : groups * chunks + groups]
    q_ref, k_ref, v_ref, att_ref, x_ref, xt_ref, y_ref = refs[groups * chunks + groups :]
    pairs, local, _ = outs[0].shape
    sub_rows = local // chunks
    items, rows, width = x_ref.shape
    keys = k_ref.shape[1]
    count = count_ref[0]
    w_t = wqkv_ref[...].T
    w_qv = jnp.concatenate([w_t[:width], w_t[2 * width :], one_hot(width, width)], axis=0)
    w_k = w_t[width : 2 * width]
    w_proj_t = wproj_ref[...].T
    flip = one_hot(rows, rows)
    masks = mask_of(keys, count)
    ones = jnp.broadcast_to(jnp.where(masks[1], F32(1), F32(0)), (16, keys)).astype(BF)
    kept = (q_ref, k_ref, v_ref)
    here = cell_index()
    for m in range(groups):
        for k in range(chunks):
            at = pl.multiple_of((here ^ m) * local + k * sub_rows, sub_rows)
            for q, part in enumerate(unpack(ins[k * groups + m][firsts[k] : firsts[k] + pairs], per, width)):
                x_ref[q * pairs : (q + 1) * pairs, pl.ds(at, sub_rows), :] = part

    def project(ats):
        x = jnp.concatenate([x_ref[at] for at in ats], axis=0)
        q_v = dot(w_qv, x, NT)
        for a, at in enumerate(ats):
            k = dot(x[a * rows : a * rows + keys], w_k, NT)
            own = q_v[:, a * rows : (a + 1) * rows]
            xt_ref[at] = own[2 * width :].astype(BF)
            keep_projected(kept, at, own[: 2 * width], k, masks)

    def finish(ps):
        ats = [q * pairs + p for p in ps for q in range(per)]
        done = finish_items(att_ref, ats, w_proj_t, flip, lambda at: xt_ref[at])
        for a, p in enumerate(ps):
            y_ref[p] = pack(done[a * per : (a + 1) * per])

    most = max(1, 1024 // rows)
    loop(items, min(2 * most, 14), project)
    loop(items, min(most, 7), lambda ats: attend(kept, att_ref, ats, ones))
    loop(pairs, min(most, 7), finish)
    for m in range(groups):
        at = pl.multiple_of((here ^ m) * local, local)
        outs[m][...] = y_ref[:, pl.ds(at, local), :]


def row_chunk(pieces, count, wqkv, wproj, groups, per, chunks, pairs, firsts):
    sub_rows, packed = pieces[0].shape[1:]
    width = wproj.shape[0]
    local = sub_rows * chunks
    rows = local * groups
    keys = rows - rows // 4
    return pl.pallas_call(
        functools.partial(row_kernel, groups, per, chunks, firsts),
        in_specs=[IN_SMEM] + [IN_VMEM] * (2 + len(pieces)),
        out_specs=[IN_VMEM] * groups,
        out_shape=[near((pairs, local, packed))] * groups,
        scratch_shapes=attention_scratch(pairs * per, width, rows, keys)
        + [
            pltpu.VMEM((pairs * per, rows, width), BF),
            pltpu.VMEM((pairs * per, width, rows), BF),
            pltpu.VMEM((pairs, rows, packed), BF),
        ],
        compiler_params=PARAMS,
        cost_estimate=cost(10**8),
    )(count, *bring(wqkv, wproj, *pieces))


def swap_kernel(in_ref, out_ref, x_ref):
    first, width, second = in_ref.shape
    lanes = -(-second // 128) * 128
    side = 16
    swap = swap_matrix(side)
    for a in range(first):
        x_ref[a] = pad_lanes(in_ref[a], lanes).T[:second]
    for a in range(first // side):
        for b in range(second // side):
            block = x_ref[a * side : (a + 1) * side, b * side : (b + 1) * side, :]
            swapped = dot(swap, block.reshape(side * side, width)).astype(BF)
            out_ref[b * side : (b + 1) * side, a * side : (a + 1) * side, :] = swapped.reshape(side, side, width)


def swap_cotangent(array_t):
    first, width, second = array_t.shape
    return pl.pallas_call(
        swap_kernel,
        in_specs=[IN_VMEM],
        out_specs=IN_VMEM,
        out_shape=near((second, first, width)),
        scratch_shapes=[pltpu.VMEM((first, second, width), BF)],
        compiler_params=PARAMS,
        cost_estimate=cost(10**8),
        name="swap_cotangent",
    )(*bring(array_t))


def output_kernel(groups, per, chunks, *refs):
    parts, (out_ref, f_ref, y_ref) = refs[:-3], refs[-3:]
    feats, local, width = f_ref.shape
    half = feats // groups // per
    pairs = half // chunks
    size = pairs * local
    lanes = -(-feats // 128) * 128
    here = cell_index()
    count = parts[0].shape[0]
    for n, part in enumerate(parts):
        for b in range(count):
            at = n * count + b
            base = (here ^ (at // chunks)) * (half * per) + (at % chunks) * pairs
            for q in range(per):
                rows = part[b, q * size : (q + 1) * size].reshape(pairs, local, width)
                f_ref[pl.ds(base + q * half, pairs)] = rows
    side = 16
    swap = swap_matrix(side)
    for f in range(0, feats, side):
        for r in range(0, local, side):
            block = f_ref[f : f + side, r : r + side, :].reshape(side * side, width)
            y_ref[r : r + side, f : f + side, :] = dot(swap, block).astype(BF).reshape(side, side, width)
    for r in range(local):
        y = y_ref[r]
        if lanes > feats:
            y = jnp.concatenate([y, jnp.zeros((lanes - feats, width), BF)], axis=0)
        out_ref[r] = y.T[:, :feats]


def make_output(parts, groups, per, chunks, feats, local):
    width = parts[0].shape[-1]
    return pl.pallas_call(
        functools.partial(output_kernel, groups, per, chunks),
        in_specs=[IN_VMEM] * len(parts),
        out_specs=IN_VMEM,
        out_shape=jax.ShapeDtypeStruct((local, width, feats), BF),
        scratch_shapes=[pltpu.VMEM((feats, local, width), BF), pltpu.VMEM((local, feats, width), BF)],
        compiler_params=PARAMS,
        cost_estimate=cost(10**8),
        name="make_output",
    )(*bring(*parts))


def gelu_and_slope(pre):
    size = jnp.abs(pre)
    bell = jnp.exp2(pre * pre * F32(-0.5 * math.log2(math.e)))
    t = 1.0 / (size + F32(ERFC_K))
    poly = F32(ERFC_C[-1])
    for coefficient in ERFC_C[-2::-1]:
        poly = poly * t + F32(coefficient)
    tail = poly * t * bell
    cdf = jnp.where(pre >= 0, 1.0 - tail, tail)
    return pre * cdf, cdf + pre * (bell * F32(1.0 / math.sqrt(2.0 * math.pi)))


def dense_kernel(groups, per, chunks, first, factor, *refs):
    last = factor is not None
    blocks = refs[-1].shape[0]
    ins = refs[:blocks]
    win_ref, woutt_ref, cot_ref = refs[blocks : blocks + 3]
    rest = refs[blocks + 3 :]
    if first > 0:
        prev_in, prev_out = rest[:2]
        rest = rest[2:]
    if last:
        out_ref, keep_ref, send_ref, gin_ref, gout_ref, n_ref = rest
    else:
        out_ref, gin_ref, gout_ref, n_ref = rest
    pairs, local, _ = ins[0].shape
    width, _ = win_ref.shape
    size = pairs * local
    fg = cot_ref.shape[0] // groups
    half = fg // per
    here = cell_index()
    for b in range(blocks):
        for q, part in enumerate(unpack(ins[b][...], per, width)):
            n_ref[b, q * size : (q + 1) * size] = part.reshape(size, width)
    if first > 0:
        gin_ref[...] = prev_in[...]
        gout_ref[...] = prev_out[...]
    else:
        gin_ref[...] = jnp.zeros_like(gin_ref)
        gout_ref[...] = jnp.zeros_like(gout_ref)
    w_in = win_ref[...]
    w_out_t = woutt_ref[...]

    def step(b):
        at = first + b
        feature = (here ^ (at // chunks)) * fg + (at % chunks) * pairs
        normed = n_ref[b]
        cot = [cot_ref[pl.ds(feature + q * half, pairs)].reshape(size, width) for q in range(per)]
        cot = jnp.concatenate(cot, axis=0)
        act, slope = gelu_and_slope(dot(normed, w_in))
        act = act.astype(BF)
        out_ref[b] = (normed.astype(F32) + dot(act, w_out_t, NT)).astype(BF)
        dpre = (dot(cot, w_out_t) * slope).astype(BF)
        gin_ref[...] += dot(normed, dpre, TN)
        gout_ref[...] += dot(cot, act, TN)

    loop(blocks, BLOCKS, lambda bs: [step(b) for b in bs])
    if last:
        both = pack([(gin_ref[...].T * F32(factor)).astype(BF), (gout_ref[...].T * F32(factor)).astype(BF)])
        both = both.reshape(keep_ref.shape[0], 2, *keep_ref.shape[1:])
        even = here % 2 == 0
        keep_ref[...] = jnp.where(even, both[:, 0], both[:, 1])
        send_ref[...] = jnp.where(even, both[:, 1], both[:, 0])


def dense_part(blocks, cot_t, w_in, w_out_t, prev, groups, per, chunks, first, factor, shares):
    pairs, local, _ = blocks[0].shape
    width, hid = w_in.shape
    size = per * pairs * local
    count = len(blocks)
    outs = [near((count, size, width))]
    operands = list(blocks) + [w_in, w_out_t, cot_t]
    if first > 0:
        operands += list(prev)
    scratch = []
    if factor is None:
        outs += [near((width, hid), F32)] * 2
    else:
        outs += [near((shares // 2, hid // shares, 2 * width))] * 2
        scratch = [pltpu.VMEM((width, hid), F32)] * 2
    scratch += [pltpu.VMEM((count, size, width), BF)]
    return pl.pallas_call(
        functools.partial(dense_kernel, groups, per, chunks, first, factor),
        in_specs=[IN_VMEM] * len(operands),
        out_specs=[IN_VMEM] * len(outs),
        out_shape=outs,
        scratch_shapes=scratch,
        compiler_params=PARAMS,
        cost_estimate=cost(10**8),
    )(*bring(*operands))


def add_kernel(a_ref, b_ref, out_ref):
    out_ref[...] = (a_ref[...].astype(F32) + b_ref[...].astype(F32)).astype(BF)


def add_pair(a, b):
    return pl.pallas_call(
        add_kernel,
        in_specs=[IN_VMEM] * 2,
        out_specs=IN_VMEM,
        out_shape=jax.ShapeDtypeStruct(a.shape, BF),
        compiler_params=PARAMS,
        cost_estimate=cost(10**6),
        name="add_pair",
    )(*bring(a, b))


def exchange(pieces, groups):
    come = [pieces[0]]
    for m in range(1, groups):
        come.append(lax.ppermute(pieces[m], CELLS, [(s, s ^ m) for s in range(groups)]))
    return come


def per_device(
    cells_in, train_count, feat_count, feat_qkv, feat_proj, row_qkv, row_proj, w_in, w_out, cotangent
):
    block_t = jnp.swapaxes(cells_in[0], 1, 2)
    local, width, feats = block_t.shape
    groups = lax.axis_size(CELLS)
    tables = lax.axis_size("tables")
    fg = feats // groups
    per = 2 if fg % 2 == 0 else 1
    half = fg // per
    sub_rows = 16
    row_chunks = local // sub_rows
    feat_chunks = 2 if half % 2 == 0 else 1
    factor = 1.0 / math.sqrt(tables * local * groups * feats)
    pairs = half // feat_chunks
    pieces = [[] for _ in range(feat_chunks)]
    firsts = []
    for k in range(row_chunks):
        cuts = feat_chunks if k == row_chunks - 1 else 1
        sent = feature_chunk(block_t, feat_count, feat_qkv, feat_proj, groups, per, k, sub_rows, cuts)
        come = [exchange(sent[c * groups : (c + 1) * groups], groups) for c in range(cuts)]
        for j in range(feat_chunks):
            pieces[j] += come[j % cuts]
        firsts.append(cuts == 1)
    cot_t = swap_cotangent(jnp.swapaxes(cotangent[0], 1, 2))
    back = []
    for j in range(feat_chunks):
        starts = tuple(j * pairs if whole else 0 for whole in firsts)
        done = row_chunk(pieces[j], train_count, row_qkv, row_proj, groups, per, row_chunks, pairs, starts)
        back.append(exchange(done, groups))
    w_out_t = w_out.T
    shares = tables * groups
    blocks = [back[j][m] for m in range(groups) for j in range(feat_chunks)]
    cut = len(blocks) // 2
    args = (cot_t, w_in, w_out_t)
    shape = (groups, per, feat_chunks)
    out_0, *partial = dense_part(blocks[:cut], *args, None, *shape, 0, None, shares)
    out_1, keep, send = dense_part(blocks[cut:], *args, partial, *shape, cut, factor, shares)
    other = lax.ppermute(send, "core", [(0, 1), (1, 0)])
    pieces = add_pair(keep, other)
    total = lax.all_to_all(pieces, ("tables", "chips"), split_axis=0, concat_axis=0, tiled=True)
    total = jnp.sum(total.astype(F32), axis=0)
    output = make_output([out_0, out_1], *shape, feats, local)
    grad_in, grad_out = unpack(total, 2, width)
    return (jnp.swapaxes(output, 1, 2)[None], grad_in.T, grad_out)


def solution(mesh):
    tables, cells = mesh.devices.shape
    split = jax.sharding.Mesh(mesh.devices.reshape(tables, cells // 2, 2), ("tables", "chips", "core"))
    spread = P("tables", CELLS, None, None)
    shares = ("tables",) + CELLS
    return jax.shard_map(
        per_device,
        mesh=split,
        in_specs=(spread, P("tables"), P("tables"), P(), P(), P(), P(), P(), P(), spread),
        out_specs=(spread, P(None, shares), P(shares, None)),
        check_vma=False,
    )
```

```python
import functools
import math

import jax
import jax.numpy as jnp
from jax import lax
from jax.experimental import pallas as pl
from jax.experimental.pallas import tpu as pltpu
from jax.sharding import PartitionSpec as P


HEADS = 6
HEAD_DIM = 32
BF = jnp.bfloat16
F32 = jnp.float32
ERFC_K = 2.9
ERFC_C = (
    0.38553786502648235,
    1.4917549496141058,
    -0.32977430445565825,
    21.663540536082817,
    -21.146073738657215,
)
NT = (((1,), (1,)), ((), ()))
TN = (((0,), (0,)), ((), ()))


def dot(a, b, dims=(((1,), (0,)), ((), ()))):
    return lax.dot_general(a, b, dims, preferred_element_type=F32)


def layer_norm(values):
    mean = jnp.mean(values, axis=0, keepdims=True)
    centred = values - mean
    var = jnp.mean(centred * centred, axis=0, keepdims=True)
    return centred * lax.rsqrt(var + 1e-05)


def one_hot(rows, cols):
    row = lax.broadcasted_iota(jnp.int32, (rows, cols), 0)
    col = lax.broadcasted_iota(jnp.int32, (rows, cols), 1)
    return (row == col).astype(F32).astype(BF)


def finish_items(att_ref, ats, w_proj_t, flip, residual_t):
    lanes = att_ref.shape[2]
    mixed = dot(w_proj_t, jnp.concatenate([att_ref[at] for at in ats], axis=1))
    done = []
    for a, at in enumerate(ats):
        normed = layer_norm(residual_t(at).astype(F32) + mixed[:, a * lanes : (a + 1) * lanes]).astype(BF)
        done.append(dot(flip, normed, NT).astype(BF))
    return done


def swap_matrix(side):
    out = lax.broadcasted_iota(jnp.int32, (side * side, side * side), 0)
    src = lax.broadcasted_iota(jnp.int32, (side * side, side * side), 1)
    return (src == (out % side) * side + out // side).astype(F32).astype(BF)


def pack(parts):
    if len(parts) == 1:
        return parts[0]
    a, b = parts
    cut = a.shape[-1] // 128 * 128
    return jnp.concatenate([a[..., :cut], b[..., :cut], a[..., cut:], b[..., cut:]], axis=-1)


def unpack(block, per, width):
    if per == 1:
        return [block]
    cut = width // 128 * 128
    rest = width - cut
    return [
        jnp.concatenate(
            [block[..., q * cut : (q + 1) * cut], block[..., 2 * cut + q * rest : 2 * cut + (q + 1) * rest]],
            axis=-1,
        )
        for q in range(2)
    ]


CELLS = ("chips", "core")


def cell_index():
    return lax.axis_index("chips") * 2 + lax.axis_index("core")


def mask_of(keys, count):
    rows = lax.broadcasted_iota(jnp.int32, (keys, 1), 0) < count
    lanes = lax.broadcasted_iota(jnp.int32, (1, keys), 1) < count
    return rows, lanes


def keep_projected(refs, at, q_v, k_rows, masks):
    q_ref, k_ref, v_ref = refs
    width, keys = q_ref.shape[1], k_ref.shape[1]
    key_row, key_lane = masks
    scale = F32(math.log2(math.e) / math.sqrt(HEAD_DIM))
    q_ref[at] = (q_v[:width] * scale).astype(BF)
    v_ref[at] = jnp.where(key_lane, q_v[width:, :keys], F32(0)).astype(BF)
    k_ref[at] = jnp.where(key_row, k_rows[:keys], k_rows[0:1]).astype(BF)


def score_blocks(q_own, lanes):
    hd = HEAD_DIM
    width = q_own.shape[0]
    blank = jnp.zeros((hd, lanes), BF)
    blocks = []
    for i in range(HEADS // 2):
        lo = 2 * i * hd
        tile = lo // 128 * 128
        end = min(tile + 128, width)
        pieces = [
            jnp.concatenate([q_own[lo : lo + hd], blank], axis=1),
            jnp.concatenate([blank, q_own[lo + hd : lo + 2 * hd]], axis=1),
        ]
        if lo > tile:
            pieces = [jnp.zeros((lo - tile, 2 * lanes), BF)] + pieces
        if lo + 2 * hd < end:
            pieces = pieces + [jnp.zeros((end - lo - 2 * hd, 2 * lanes), BF)]
        blocks.append((tile, end, jnp.concatenate(pieces, axis=0)))
    return blocks


def attend(refs, att_ref, ats, ones):
    q_ref, k_ref, v_ref = refs
    lanes = q_ref.shape[2]
    hd = HEAD_DIM
    scores = []
    for at in ats:
        k_own = k_ref[at]
        for tile, end, block in score_blocks(q_ref[at], lanes):
            scores.append(dot(k_own[:, tile:end], block))
    weights = [jnp.exp2(s - jnp.max(s, axis=0, keepdims=True)).astype(BF) for s in scores]
    for n, at in enumerate(ats):
        v_own = v_ref[at]
        for i in range(HEADS // 2):
            lo = 2 * i * hd
            lhs = jnp.concatenate([v_own[lo : lo + 2 * hd], ones], axis=0)
            mixed = dot(lhs, weights[n * (HEADS // 2) + i])
            scale = 1.0 / mixed[2 * hd : 2 * hd + 1]
            att_ref[at, lo : lo + hd] = (mixed[:hd, :lanes] * scale[:, :lanes]).astype(BF)
            att_ref[at, lo + hd : lo + 2 * hd] = (mixed[hd : 2 * hd, lanes:] * scale[:, lanes:]).astype(BF)


def loop(count, most, body):
    group = max(d for d in range(1, most + 1) if count % d == 0)

    def step(i, carry):
        body([i * group + a for a in range(group)])
        return carry

    lax.fori_loop(0, count // group, step, 0)


def pad_lanes(value, lanes):
    rows, n = value.shape
    return value if n == lanes else jnp.concatenate([value, jnp.zeros((rows, lanes - n), value.dtype)], axis=1)


def feature_kernel(groups, per, first, rows, cuts, count_ref, cells_ref, wqkv_ref, wproj_ref, *refs):
    outs = refs[: groups * cuts]
    refs = refs[groups * cuts :]
    parts = 1
    waits = [[] for _ in range(parts)]
    if first == 0:
        sems, wqkv_buf, wproj_buf, cells_buf = refs[6:]
        refs = refs[:6]
        step = rows // parts
        moves = [(wqkv_ref, wqkv_buf), (wproj_ref, wproj_buf)]
        for n in range(parts):
            moves.append((cells_ref.at[pl.ds(n * step, step)], cells_buf.at[pl.ds(n * step, step)]))
        moves = [pltpu.make_async_copy(a, b, sems.at[n]) for n, (a, b) in enumerate(moves)]
        for move in moves:
            move.start()
        for move in moves[:2]:
            move.wait()
        waits = [[move] for move in moves[2:]]
        wqkv_ref, wproj_ref, cells_ref = wqkv_buf, wproj_buf, cells_buf
    count = count_ref[0]
    q_ref, k_ref, v_ref, att_ref, mid_ref, swap_ref = refs
    _, width, feats = cells_ref.shape
    lanes = q_ref.shape[2]
    fg = feats // groups
    half = fg // per
    w_t = wqkv_ref[...].T
    w_qv = jnp.concatenate([w_t[:width], w_t[2 * width :]], axis=0)
    w_k = w_t[width : 2 * width]
    w_proj_t = wproj_ref[...].T
    flip = one_hot(feats, lanes)
    masks = mask_of(feats, count)
    ones = jnp.broadcast_to(jnp.where(masks[1], F32(1), F32(0)), (16, feats)).astype(BF)
    kept = (q_ref, k_ref, v_ref)

    def project(ats):
        x_t = [pad_lanes(cells_ref[first + at], lanes) for at in ats]
        q_v = dot(w_qv, jnp.concatenate(x_t, axis=1))
        x = [t.T[:feats] for t in x_t]
        k = dot(jnp.concatenate(x, axis=0), w_k, NT)
        for a, at in enumerate(ats):
            keep_projected(kept, at, q_v[:, a * lanes : (a + 1) * lanes], k[a * feats : (a + 1) * feats], masks)

    def finish(ats):
        own = lambda at: pad_lanes(cells_ref[first + at], lanes)
        for at, value in zip(ats, finish_items(att_ref, ats, w_proj_t, flip, own)):
            mid_ref[at] = value

    for n, moves in enumerate(waits):
        for move in moves:
            move.wait()
        step = rows // parts
        project(list(range(n * step, (n + 1) * step)))
    loop(rows, 8, lambda ats: attend(kept, att_ref, ats, ones))
    loop(rows, 16, finish)
    swap = swap_matrix(rows)
    for f in range(feats // rows):
        block = mid_ref[:, f * rows : (f + 1) * rows, :].reshape(rows * rows, width)
        swap_ref[f * rows : (f + 1) * rows] = dot(swap, block).astype(BF).reshape(rows, rows, width)
    here = cell_index()
    size = half // cuts
    for c in range(cuts):
        for m in range(groups):
            base = (here ^ m) * fg + c * size
            outs[c * groups + m][...] = pack([swap_ref[pl.ds(base + q * half, size)] for q in range(per)])


BLOCKS = 2
IN_VMEM = pl.BlockSpec(memory_space=pltpu.VMEM)
IN_SMEM = pl.BlockSpec(memory_space=pltpu.SMEM)


def attention_scratch(items, width, lanes, keys):
    return [
        pltpu.VMEM((items, width, lanes), BF),
        pltpu.VMEM((items, keys, width), BF),
        pltpu.VMEM((items, width, keys), BF),
        pltpu.VMEM((items, width, lanes), BF),
    ]


def near(shape, dtype=BF):
    return pltpu.VMEM(shape, dtype)


def bring(*arrays):
    return [pltpu.with_memory_space_constraint(x, pltpu.VMEM) for x in arrays]


PARAMS = pltpu.CompilerParams(vmem_limit_bytes=14 * 2**20)


def cost(flops):
    return pl.CostEstimate(flops=flops, transcendentals=0, bytes_accessed=10**6)


def feature_chunk(block_t, count, wqkv, wproj, groups, per, chunk, rows, cuts):
    _, width, feats = block_t.shape
    half = feats // groups // per
    lanes = -(-feats // 128) * 128
    outs = [near((half // cuts, rows, per * width))] * (groups * cuts)
    scratch = attention_scratch(rows, width, lanes, feats)
    scratch += [pltpu.VMEM((rows, feats, width), BF), pltpu.VMEM((feats, rows, width), BF)]
    operands = [block_t, wqkv, wproj]
    if chunk == 0:
        operands = [pltpu.with_memory_space_constraint(x, pltpu.HBM) for x in operands]
        specs = [pl.BlockSpec(memory_space=pltpu.HBM)] * 3
        scratch += [pltpu.SemaphoreType.DMA((4,))]
        scratch += [pltpu.VMEM(x.shape, BF) for x in (wqkv, wproj)]
        scratch += [pltpu.VMEM((rows, width, feats), BF)]
    else:
        operands = bring(*operands)
        specs = [IN_VMEM] * 3
    return pl.pallas_call(
        functools.partial(feature_kernel, groups, per, chunk * rows, rows, cuts),
        in_specs=[IN_SMEM] + specs,
        out_specs=[IN_VMEM] * len(outs),
        out_shape=outs,
        scratch_shapes=scratch,
        compiler_params=PARAMS,
        cost_estimate=cost(10**8),
    )(count, *operands)


def row_kernel(groups, per, chunks, firsts, count_ref, wqkv_ref, wproj_ref, *refs):
    ins = refs[: groups * chunks]
    outs = refs[groups * chunks : groups * chunks + groups]
    q_ref, k_ref, v_ref, att_ref, x_ref, xt_ref, y_ref = refs[groups * chunks + groups :]
    pairs, local, _ = outs[0].shape
    sub_rows = local // chunks
    items, rows, width = x_ref.shape
    keys = k_ref.shape[1]
    count = count_ref[0]
    w_t = wqkv_ref[...].T
    w_qv = jnp.concatenate([w_t[:width], w_t[2 * width :], one_hot(width, width)], axis=0)
    w_k = w_t[width : 2 * width]
    w_proj_t = wproj_ref[...].T
    flip = one_hot(rows, rows)
    masks = mask_of(keys, count)
    ones = jnp.broadcast_to(jnp.where(masks[1], F32(1), F32(0)), (16, keys)).astype(BF)
    kept = (q_ref, k_ref, v_ref)
    here = cell_index()
    for m in range(groups):
        for k in range(chunks):
            at = pl.multiple_of((here ^ m) * local + k * sub_rows, sub_rows)
            for q, part in enumerate(unpack(ins[k * groups + m][firsts[k] : firsts[k] + pairs], per, width)):
                x_ref[q * pairs : (q + 1) * pairs, pl.ds(at, sub_rows), :] = part

    def project(ats):
        x = jnp.concatenate([x_ref[at] for at in ats], axis=0)
        q_v = dot(w_qv, x, NT)
        for a, at in enumerate(ats):
            k = dot(x[a * rows : a * rows + keys], w_k, NT)
            own = q_v[:, a * rows : (a + 1) * rows]
            xt_ref[at] = own[2 * width :].astype(BF)
            keep_projected(kept, at, own[: 2 * width], k, masks)

    def finish(ps):
        ats = [q * pairs + p for p in ps for q in range(per)]
        done = finish_items(att_ref, ats, w_proj_t, flip, lambda at: xt_ref[at])
        for a, p in enumerate(ps):
            y_ref[p] = pack(done[a * per : (a + 1) * per])

    most = max(1, 1024 // rows)
    loop(items, min(2 * most, 14), project)
    loop(items, min(most, 7), lambda ats: attend(kept, att_ref, ats, ones))
    loop(pairs, min(most, 7), finish)
    for m in range(groups):
        at = pl.multiple_of((here ^ m) * local, local)
        outs[m][...] = y_ref[:, pl.ds(at, local), :]


def row_chunk(pieces, count, wqkv, wproj, groups, per, chunks, pairs, firsts):
    sub_rows, packed = pieces[0].shape[1:]
    width = wproj.shape[0]
    local = sub_rows * chunks
    rows = local * groups
    keys = rows - rows // 4
    return pl.pallas_call(
        functools.partial(row_kernel, groups, per, chunks, firsts),
        in_specs=[IN_SMEM] + [IN_VMEM] * (2 + len(pieces)),
        out_specs=[IN_VMEM] * groups,
        out_shape=[near((pairs, local, packed))] * groups,
        scratch_shapes=attention_scratch(pairs * per, width, rows, keys)
        + [
            pltpu.VMEM((pairs * per, rows, width), BF),
            pltpu.VMEM((pairs * per, width, rows), BF),
            pltpu.VMEM((pairs, rows, packed), BF),
        ],
        compiler_params=PARAMS,
        cost_estimate=cost(10**8),
    )(count, *bring(wqkv, wproj, *pieces))


def swap_kernel(in_ref, out_ref, x_ref):
    first, width, second = in_ref.shape
    lanes = -(-second // 128) * 128
    side = 16
    swap = swap_matrix(side)
    for a in range(first):
        x_ref[a] = pad_lanes(in_ref[a], lanes).T[:second]
    for a in range(first // side):
        for b in range(second // side):
            block = x_ref[a * side : (a + 1) * side, b * side : (b + 1) * side, :]
            swapped = dot(swap, block.reshape(side * side, width)).astype(BF)
            out_ref[b * side : (b + 1) * side, a * side : (a + 1) * side, :] = swapped.reshape(side, side, width)


def swap_cotangent(array_t):
    first, width, second = array_t.shape
    return pl.pallas_call(
        swap_kernel,
        in_specs=[IN_VMEM],
        out_specs=IN_VMEM,
        out_shape=near((second, first, width)),
        scratch_shapes=[pltpu.VMEM((first, second, width), BF)],
        compiler_params=PARAMS,
        cost_estimate=cost(10**8),
        name="swap_cotangent",
    )(*bring(array_t))


def output_kernel(groups, per, chunks, spots, *refs):
    parts, (out_ref, f_ref, y_ref) = refs[:-3], refs[-3:]
    feats, local, width = f_ref.shape
    half = feats // groups // per
    pairs = half // chunks
    size = pairs * local
    lanes = -(-feats // 128) * 128
    here = cell_index()
    for (first_m, some, first_j), part in zip(spots, parts):
        for b in range(part.shape[0]):
            base = (here ^ (first_m + b // some)) * (half * per) + (first_j + b % some) * pairs
            for q in range(per):
                rows = part[b, q * size : (q + 1) * size].reshape(pairs, local, width)
                f_ref[pl.ds(base + q * half, pairs)] = rows
    side = 16
    swap = swap_matrix(side)
    for f in range(0, feats, side):
        for r in range(0, local, side):
            block = f_ref[f : f + side, r : r + side, :].reshape(side * side, width)
            y_ref[r : r + side, f : f + side, :] = dot(swap, block).astype(BF).reshape(side, side, width)
    for r in range(local):
        y = y_ref[r]
        if lanes > feats:
            y = jnp.concatenate([y, jnp.zeros((lanes - feats, width), BF)], axis=0)
        out_ref[r] = y.T[:, :feats]


def make_output(parts, spots, groups, per, chunks, feats, local):
    width = parts[0].shape[-1]
    return pl.pallas_call(
        functools.partial(output_kernel, groups, per, chunks, spots),
        in_specs=[IN_VMEM] * len(parts),
        out_specs=IN_VMEM,
        out_shape=jax.ShapeDtypeStruct((local, width, feats), BF),
        scratch_shapes=[pltpu.VMEM((feats, local, width), BF), pltpu.VMEM((local, feats, width), BF)],
        compiler_params=PARAMS,
        cost_estimate=cost(10**8),
        name="make_output",
    )(*bring(*parts))


def gelu_and_slope(pre):
    size = jnp.abs(pre)
    bell = jnp.exp2(pre * pre * F32(-0.5 * math.log2(math.e)))
    t = 1.0 / (size + F32(ERFC_K))
    poly = F32(ERFC_C[-1])
    for coefficient in ERFC_C[-2::-1]:
        poly = poly * t + F32(coefficient)
    tail = poly * t * bell
    cdf = jnp.where(pre >= 0, 1.0 - tail, tail)
    return pre * cdf, cdf + pre * (bell * F32(1.0 / math.sqrt(2.0 * math.pi)))


def dense_kernel(groups, per, spot, fresh, factor, *refs):
    first_m, chunks, first_j = spot
    last = factor is not None
    blocks = refs[-1].shape[0]
    ins = refs[:blocks]
    win_ref, woutt_ref, cot_ref = refs[blocks : blocks + 3]
    rest = refs[blocks + (3 if fresh else 5) :]
    if last:
        out_ref, gin_ref, gout_ref, keep_ref, send_ref, n_ref = rest
    else:
        out_ref, gin_ref, gout_ref, n_ref = rest
    pairs, local, _ = ins[0].shape
    width, _ = win_ref.shape
    size = pairs * local
    fg = cot_ref.shape[0] // groups
    half = fg // per
    here = cell_index()
    for b in range(blocks):
        for q, part in enumerate(unpack(ins[b][...], per, width)):
            n_ref[b, q * size : (q + 1) * size] = part.reshape(size, width)
    if fresh:
        gin_ref[...] = jnp.zeros_like(gin_ref)
        gout_ref[...] = jnp.zeros_like(gout_ref)
    w_in = win_ref[...]
    w_out_t = woutt_ref[...]

    def step(b):
        group = here ^ (first_m + b // chunks)
        feature = group * fg + (first_j + b % chunks) * pairs
        normed = n_ref[b]
        cot = [cot_ref[pl.ds(feature + q * half, pairs)].reshape(size, width) for q in range(per)]
        cot = jnp.concatenate(cot, axis=0)
        act, slope = gelu_and_slope(dot(normed, w_in))
        act = act.astype(BF)
        out_ref[b] = (normed.astype(F32) + dot(act, w_out_t, NT)).astype(BF)
        dpre = (dot(cot, w_out_t) * slope).astype(BF)
        gin_ref[...] += dot(normed, dpre, TN)
        gout_ref[...] += dot(cot, act, TN)

    loop(blocks, BLOCKS, lambda bs: [step(b) for b in bs])
    if last:
        both = pack([(gin_ref[...].T * F32(factor)).astype(BF), (gout_ref[...].T * F32(factor)).astype(BF)])
        both = both.reshape(keep_ref.shape[0], 2, *keep_ref.shape[1:])
        even = here % 2 == 0
        keep_ref[...] = jnp.where(even, both[:, 0], both[:, 1])
        send_ref[...] = jnp.where(even, both[:, 1], both[:, 0])


def dense_part(blocks, cot_t, w_in, w_out_t, prev, groups, per, spot, factor, shares):
    pairs, local, _ = blocks[0].shape
    width, hid = w_in.shape
    size = per * pairs * local
    count = len(blocks)
    outs = [near((count, size, width))] + [near((width, hid), F32)] * 2
    operands = list(blocks) + [w_in, w_out_t, cot_t]
    alias = {}
    if prev is not None:
        alias = {len(operands) + n: 1 + n for n in range(2)}
        operands += list(prev)
    if factor is not None:
        outs += [near((shares // 2, hid // shares, 2 * width))] * 2
    return pl.pallas_call(
        functools.partial(dense_kernel, groups, per, spot, prev is None, factor),
        in_specs=[IN_VMEM] * len(operands),
        out_specs=[IN_VMEM] * len(outs),
        out_shape=outs,
        input_output_aliases=alias,
        scratch_shapes=[pltpu.VMEM((count, size, width), BF)],
        compiler_params=PARAMS,
        cost_estimate=cost(10**8),
    )(*bring(*operands))


def add_kernel(a_ref, b_ref, out_ref):
    out_ref[...] = (a_ref[...].astype(F32) + b_ref[...].astype(F32)).astype(BF)


def add_pair(a, b):
    return pl.pallas_call(
        add_kernel,
        in_specs=[IN_VMEM] * 2,
        out_specs=IN_VMEM,
        out_shape=near(a.shape),
        compiler_params=PARAMS,
        cost_estimate=cost(10**6),
        name="add_pair",
    )(*bring(a, b))


def exchange(pieces, groups):
    come = [pieces[0]]
    for m in range(1, groups):
        come.append(lax.ppermute(pieces[m], CELLS, [(s, s ^ m) for s in range(groups)]))
    return come


def per_device(
    cells_in, train_count, feat_count, feat_qkv, feat_proj, row_qkv, row_proj, w_in, w_out, cotangent
):
    block_t = jnp.swapaxes(cells_in[0], 1, 2)
    local, width, feats = block_t.shape
    groups = lax.axis_size(CELLS)
    tables = lax.axis_size("tables")
    fg = feats // groups
    per = 2 if fg % 2 == 0 else 1
    half = fg // per
    sub_rows = 16
    row_chunks = local // sub_rows
    feat_chunks = 2 if half % 2 == 0 else 1
    factor = 1.0 / math.sqrt(tables * local * groups * feats)
    pairs = half // feat_chunks
    pieces = [[] for _ in range(feat_chunks)]
    firsts = []
    for k in range(row_chunks):
        cuts = feat_chunks if k == row_chunks - 1 else 1
        sent = feature_chunk(block_t, feat_count, feat_qkv, feat_proj, groups, per, k, sub_rows, cuts)
        come = [exchange(sent[c * groups : (c + 1) * groups], groups) for c in range(cuts)]
        for j in range(feat_chunks):
            pieces[j] += come[j % cuts]
        firsts.append(cuts == 1)
    cot_t = swap_cotangent(jnp.swapaxes(cotangent[0], 1, 2))
    back = []
    for j in range(feat_chunks):
        starts = tuple(j * pairs if whole else 0 for whole in firsts)
        done = row_chunk(pieces[j], train_count, row_qkv, row_proj, groups, per, row_chunks, pairs, starts)
        back.append(exchange(done, groups))
    w_out_t = w_out.T
    shares = tables * groups
    near_by = groups // 2
    spots = [(0, feat_chunks, 0)] + [(near_by, 1, j) for j in range(feat_chunks)]
    parts = []
    grads = None
    for spot in spots:
        first_m, some, first_j = spot
        blocks = [back[first_j + j][first_m + m] for m in range(near_by) for j in range(some)]
        scale = factor if spot == spots[-1] else None
        made, *grads = dense_part(blocks, cot_t, w_in, w_out_t, grads, groups, per, spot, scale, shares)
        parts.append(made)
    keep, send = grads[2:]
    other = lax.ppermute(send, "core", [(0, 1), (1, 0)])
    pieces = add_pair(keep, other)
    total = lax.all_to_all(pieces, ("tables", "chips"), split_axis=0, concat_axis=0, tiled=True)
    total = jnp.sum(total.astype(F32), axis=0)
    output = make_output(parts, spots, groups, per, feat_chunks, feats, local)
    grad_in, grad_out = unpack(total, 2, width)
    return (jnp.swapaxes(output, 1, 2)[None], grad_in.T, grad_out)


def solution(mesh):
    tables, cells = mesh.devices.shape
    split = jax.sharding.Mesh(mesh.devices.reshape(tables, cells // 2, 2), ("tables", "chips", "core"))
    spread = P("tables", CELLS, None, None)
    shares = ("tables",) + CELLS
    return jax.shard_map(
        per_device,
        mesh=split,
        in_specs=(spread, P("tables"), P("tables"), P(), P(), P(), P(), P(), P(), spread),
        out_specs=(spread, P(None, shares), P(shares, None)),
        check_vma=False,
    )
```

```python
import functools
import math

import jax
import jax.numpy as jnp
from jax import lax
from jax.experimental import pallas as pl
from jax.experimental.pallas import tpu as pltpu
from jax.sharding import PartitionSpec as P


HEADS = 6
HEAD_DIM = 32
BF = jnp.bfloat16
F32 = jnp.float32
ERFC_K = 2.9
ERFC_C = (
    0.38553786502648235,
    1.4917549496141058,
    -0.32977430445565825,
    21.663540536082817,
    -21.146073738657215,
)
NT = (((1,), (1,)), ((), ()))
TN = (((0,), (0,)), ((), ()))


def dot(a, b, dims=(((1,), (0,)), ((), ()))):
    return lax.dot_general(a, b, dims, preferred_element_type=F32)


def layer_norm(values):
    mean = jnp.mean(values, axis=0, keepdims=True)
    centred = values - mean
    var = jnp.mean(centred * centred, axis=0, keepdims=True)
    return centred * lax.rsqrt(var + 1e-05)


def one_hot(rows, cols):
    row = lax.broadcasted_iota(jnp.int32, (rows, cols), 0)
    col = lax.broadcasted_iota(jnp.int32, (rows, cols), 1)
    return (row == col).astype(F32).astype(BF)


def finish_items(att_ref, ats, w_proj_t, flip, residual_t):
    lanes = att_ref.shape[2]
    mixed = dot(w_proj_t, jnp.concatenate([att_ref[at] for at in ats], axis=1))
    done = []
    for a, at in enumerate(ats):
        normed = layer_norm(residual_t(at).astype(F32) + mixed[:, a * lanes : (a + 1) * lanes]).astype(BF)
        done.append(dot(flip, normed, NT).astype(BF))
    return done


def swap_matrix(side):
    out = lax.broadcasted_iota(jnp.int32, (side * side, side * side), 0)
    src = lax.broadcasted_iota(jnp.int32, (side * side, side * side), 1)
    return (src == (out % side) * side + out // side).astype(F32).astype(BF)


def pack(parts):
    if len(parts) == 1:
        return parts[0]
    a, b = parts
    cut = a.shape[-1] // 128 * 128
    return jnp.concatenate([a[..., :cut], b[..., :cut], a[..., cut:], b[..., cut:]], axis=-1)


def unpack(block, per, width):
    if per == 1:
        return [block]
    cut = width // 128 * 128
    rest = width - cut
    return [
        jnp.concatenate(
            [block[..., q * cut : (q + 1) * cut], block[..., 2 * cut + q * rest : 2 * cut + (q + 1) * rest]],
            axis=-1,
        )
        for q in range(2)
    ]


CELLS = ("chips", "core")


def cell_index():
    return lax.axis_index("chips") * 2 + lax.axis_index("core")


def mask_of(keys, count):
    rows = lax.broadcasted_iota(jnp.int32, (keys, 1), 0) < count
    lanes = lax.broadcasted_iota(jnp.int32, (1, keys), 1) < count
    return rows, lanes


def keep_projected(refs, at, q_v, k_rows, masks):
    q_ref, k_ref, v_ref = refs
    width, keys = q_ref.shape[1], k_ref.shape[1]
    key_row, key_lane = masks
    scale = F32(math.log2(math.e) / math.sqrt(HEAD_DIM))
    q_ref[at] = (q_v[:width] * scale).astype(BF)
    v_ref[at] = jnp.where(key_lane, q_v[width:, :keys], F32(0)).astype(BF)
    k_ref[at] = jnp.where(key_row, k_rows[:keys], k_rows[0:1]).astype(BF)


def score_blocks(q_own, lanes):
    hd = HEAD_DIM
    width = q_own.shape[0]
    blank = jnp.zeros((hd, lanes), BF)
    blocks = []
    for i in range(HEADS // 2):
        lo = 2 * i * hd
        tile = lo // 128 * 128
        end = min(tile + 128, width)
        pieces = [
            jnp.concatenate([q_own[lo : lo + hd], blank], axis=1),
            jnp.concatenate([blank, q_own[lo + hd : lo + 2 * hd]], axis=1),
        ]
        if lo > tile:
            pieces = [jnp.zeros((lo - tile, 2 * lanes), BF)] + pieces
        if lo + 2 * hd < end:
            pieces = pieces + [jnp.zeros((end - lo - 2 * hd, 2 * lanes), BF)]
        blocks.append((tile, end, jnp.concatenate(pieces, axis=0)))
    return blocks


def attend(refs, att_ref, ats, ones):
    q_ref, k_ref, v_ref = refs
    lanes = q_ref.shape[2]
    hd = HEAD_DIM
    scores = []
    for at in ats:
        k_own = k_ref[at]
        for tile, end, block in score_blocks(q_ref[at], lanes):
            scores.append(dot(k_own[:, tile:end], block))
    weights = [jnp.exp2(s - jnp.max(s, axis=0, keepdims=True)).astype(BF) for s in scores]
    for n, at in enumerate(ats):
        v_own = v_ref[at]
        for i in range(HEADS // 2):
            lo = 2 * i * hd
            lhs = jnp.concatenate([v_own[lo : lo + 2 * hd], ones], axis=0)
            mixed = dot(lhs, weights[n * (HEADS // 2) + i])
            scale = 1.0 / mixed[2 * hd : 2 * hd + 1]
            att_ref[at, lo : lo + hd] = (mixed[:hd, :lanes] * scale[:, :lanes]).astype(BF)
            att_ref[at, lo + hd : lo + 2 * hd] = (mixed[hd : 2 * hd, lanes:] * scale[:, lanes:]).astype(BF)


def loop(count, most, body):
    group = max(d for d in range(1, most + 1) if count % d == 0)

    def step(i, carry):
        body([i * group + a for a in range(group)])
        return carry

    lax.fori_loop(0, count // group, step, 0)


def pad_lanes(value, lanes):
    rows, n = value.shape
    return value if n == lanes else jnp.concatenate([value, jnp.zeros((rows, lanes - n), value.dtype)], axis=1)


def feature_kernel(groups, per, base, rows, cuts, lead, *refs):
    count_ref, cells_ref, wqkv_ref, wproj_ref, *refs = refs
    count = count_ref[0]
    first = base
    if lead:
        outs = refs[: groups * cuts]
        wqkv_buf, wproj_buf, rest_buf, *refs = refs[groups * cuts :]
        sems, cells_buf = refs[6:]
        moves = [(wqkv_ref, wqkv_buf), (wproj_ref, wproj_buf), (cells_ref.at[pl.ds(0, rows)], cells_buf)]
        late = (cells_ref.at[pl.ds(rows, rest_buf.shape[0])], rest_buf)
        moves = [pltpu.make_async_copy(a, b, sems.at[n]) for n, (a, b) in enumerate(moves)]
        late = pltpu.make_async_copy(*late, sems.at[3])
        for move in moves:
            move.start()
        for move in moves:
            move.wait()
        wqkv_ref, wproj_ref, cells_ref = wqkv_buf, wproj_buf, cells_buf
    else:
        cot_ref, *refs = refs
        outs = refs[: groups * cuts]
        cot_buf, *refs = refs[groups * cuts :]
        late = pltpu.make_async_copy(cot_ref, cot_buf, refs[6].at[0])
    late.start()
    refs = refs[:6]
    q_ref, k_ref, v_ref, att_ref, mid_ref, swap_ref = refs
    _, width, feats = cells_ref.shape
    lanes = q_ref.shape[2]
    fg = feats // groups
    half = fg // per
    w_t = wqkv_ref[...].T
    w_qv = jnp.concatenate([w_t[:width], w_t[2 * width :]], axis=0)
    w_k = w_t[width : 2 * width]
    w_proj_t = wproj_ref[...].T
    flip = one_hot(feats, lanes)
    masks = mask_of(feats, count)
    ones = jnp.broadcast_to(jnp.where(masks[1], F32(1), F32(0)), (16, feats)).astype(BF)
    kept = (q_ref, k_ref, v_ref)

    def project(ats):
        x_t = [pad_lanes(cells_ref[first + at], lanes) for at in ats]
        q_v = dot(w_qv, jnp.concatenate(x_t, axis=1))
        x = [t.T[:feats] for t in x_t]
        k = dot(jnp.concatenate(x, axis=0), w_k, NT)
        for a, at in enumerate(ats):
            keep_projected(kept, at, q_v[:, a * lanes : (a + 1) * lanes], k[a * feats : (a + 1) * feats], masks)

    def finish(ats):
        own = lambda at: pad_lanes(cells_ref[first + at], lanes)
        for at, value in zip(ats, finish_items(att_ref, ats, w_proj_t, flip, own)):
            mid_ref[at] = value

    loop(rows, 16, project)
    loop(rows, 8, lambda ats: attend(kept, att_ref, ats, ones))
    loop(rows, 16, finish)
    swap = swap_matrix(rows)
    for f in range(feats // rows):
        block = mid_ref[:, f * rows : (f + 1) * rows, :].reshape(rows * rows, width)
        swap_ref[f * rows : (f + 1) * rows] = dot(swap, block).astype(BF).reshape(rows, rows, width)
    here = cell_index()
    size = half // cuts
    for c in range(cuts):
        for m in range(groups):
            base = (here ^ m) * fg + c * size
            outs[c * groups + m][...] = pack([swap_ref[pl.ds(base + q * half, size)] for q in range(per)])
    late.wait()


BLOCKS = 2
IN_VMEM = pl.BlockSpec(memory_space=pltpu.VMEM)
IN_SMEM = pl.BlockSpec(memory_space=pltpu.SMEM)


def attention_scratch(items, width, lanes, keys):
    return [
        pltpu.VMEM((items, width, lanes), BF),
        pltpu.VMEM((items, keys, width), BF),
        pltpu.VMEM((items, width, keys), BF),
        pltpu.VMEM((items, width, lanes), BF),
    ]


def near(shape, dtype=BF):
    return pltpu.VMEM(shape, dtype)


def bring(*arrays):
    return [pltpu.with_memory_space_constraint(x, pltpu.VMEM) for x in arrays]


PARAMS = pltpu.CompilerParams(vmem_limit_bytes=14 * 2**20)


def cost(flops):
    return pl.CostEstimate(flops=flops, transcendentals=0, bytes_accessed=10**6)


def feature_chunk(cells_t, count, wqkv, wproj, cot_t, groups, per, base, rows, cuts):
    whole, width, feats = cells_t.shape
    half = feats // groups // per
    lanes = -(-feats // 128) * 128
    far = pl.BlockSpec(memory_space=pltpu.HBM)
    lead = cot_t is None
    outs = [near((half // cuts, rows, per * width))] * (groups * cuts)
    scratch = attention_scratch(rows, width, lanes, feats)
    scratch += [pltpu.VMEM((rows, feats, width), BF), pltpu.VMEM((feats, rows, width), BF)]
    operands = [cells_t, wqkv, wproj]
    if lead:
        operands = [pltpu.with_memory_space_constraint(x, pltpu.HBM) for x in operands]
        specs = [far] * 3
        outs += [near(wqkv.shape), near(wproj.shape), near((whole - rows, width, feats))]
        scratch += [pltpu.SemaphoreType.DMA((4,)), pltpu.VMEM((rows, width, feats), BF)]
    else:
        operands = bring(*operands) + [pltpu.with_memory_space_constraint(cot_t, pltpu.HBM)]
        specs = [IN_VMEM] * 3 + [far]
        outs += [near(cot_t.shape)]
        scratch += [pltpu.SemaphoreType.DMA((1,))]
    return pl.pallas_call(
        functools.partial(feature_kernel, groups, per, base, rows, cuts, lead),
        in_specs=[IN_SMEM] + specs,
        out_specs=[IN_VMEM] * len(outs),
        out_shape=outs,
        scratch_shapes=scratch,
        compiler_params=PARAMS,
        cost_estimate=cost(10**8),
        name="feature_0" if lead else "feature_1",
    )(count, *operands)


def row_kernel(groups, per, chunks, firsts, count_ref, wqkv_ref, wproj_ref, *refs):
    ins = refs[: groups * chunks]
    outs = refs[groups * chunks : groups * chunks + groups]
    q_ref, k_ref, v_ref, att_ref, x_ref, xt_ref, y_ref = refs[groups * chunks + groups :]
    pairs, local, _ = outs[0].shape
    sub_rows = local // chunks
    items, rows, width = x_ref.shape
    keys = k_ref.shape[1]
    count = count_ref[0]
    w_t = wqkv_ref[...].T
    w_qv = jnp.concatenate([w_t[:width], w_t[2 * width :], one_hot(width, width)], axis=0)
    w_k = w_t[width : 2 * width]
    w_proj_t = wproj_ref[...].T
    flip = one_hot(rows, rows)
    masks = mask_of(keys, count)
    ones = jnp.broadcast_to(jnp.where(masks[1], F32(1), F32(0)), (16, keys)).astype(BF)
    kept = (q_ref, k_ref, v_ref)
    here = cell_index()
    for m in range(groups):
        for k in range(chunks):
            at = pl.multiple_of((here ^ m) * local + k * sub_rows, sub_rows)
            for q, part in enumerate(unpack(ins[k * groups + m][firsts[k] : firsts[k] + pairs], per, width)):
                x_ref[q * pairs : (q + 1) * pairs, pl.ds(at, sub_rows), :] = part

    def project(ats):
        x = jnp.concatenate([x_ref[at] for at in ats], axis=0)
        q_v = dot(w_qv, x, NT)
        for a, at in enumerate(ats):
            k = dot(x[a * rows : a * rows + keys], w_k, NT)
            own = q_v[:, a * rows : (a + 1) * rows]
            xt_ref[at] = own[2 * width :].astype(BF)
            keep_projected(kept, at, own[: 2 * width], k, masks)

    def finish(ps):
        ats = [q * pairs + p for p in ps for q in range(per)]
        done = finish_items(att_ref, ats, w_proj_t, flip, lambda at: xt_ref[at])
        for a, p in enumerate(ps):
            y_ref[p] = pack(done[a * per : (a + 1) * per])

    most = max(1, 1024 // rows)
    loop(items, min(2 * most, 14), project)
    loop(items, min(most, 7), lambda ats: attend(kept, att_ref, ats, ones))
    loop(pairs, min(most, 7), finish)
    for m in range(groups):
        at = pl.multiple_of((here ^ m) * local, local)
        outs[m][...] = y_ref[:, pl.ds(at, local), :]


def row_chunk(pieces, count, wqkv, wproj, groups, per, chunks, pairs, firsts):
    sub_rows, packed = pieces[0].shape[1:]
    width = wproj.shape[0]
    local = sub_rows * chunks
    rows = local * groups
    keys = rows - rows // 4
    return pl.pallas_call(
        functools.partial(row_kernel, groups, per, chunks, firsts),
        in_specs=[IN_SMEM] + [IN_VMEM] * (2 + len(pieces)),
        out_specs=[IN_VMEM] * groups,
        out_shape=[near((pairs, local, packed))] * groups,
        scratch_shapes=attention_scratch(pairs * per, width, rows, keys)
        + [
            pltpu.VMEM((pairs * per, rows, width), BF),
            pltpu.VMEM((pairs * per, width, rows), BF),
            pltpu.VMEM((pairs, rows, packed), BF),
        ],
        compiler_params=PARAMS,
        cost_estimate=cost(10**8),
    )(count, *bring(wqkv, wproj, *pieces))


def swap_kernel(in_ref, out_ref, x_ref):
    first, width, second = in_ref.shape
    lanes = -(-second // 128) * 128
    side = 16
    swap = swap_matrix(side)
    for a in range(first):
        x_ref[a] = pad_lanes(in_ref[a], lanes).T[:second]
    for a in range(first // side):
        for b in range(second // side):
            block = x_ref[a * side : (a + 1) * side, b * side : (b + 1) * side, :]
            swapped = dot(swap, block.reshape(side * side, width)).astype(BF)
            out_ref[b * side : (b + 1) * side, a * side : (a + 1) * side, :] = swapped.reshape(side, side, width)


def swap_cotangent(array_t):
    first, width, second = array_t.shape
    return pl.pallas_call(
        swap_kernel,
        in_specs=[IN_VMEM],
        out_specs=IN_VMEM,
        out_shape=near((second, first, width)),
        scratch_shapes=[pltpu.VMEM((first, second, width), BF)],
        compiler_params=PARAMS,
        cost_estimate=cost(10**8),
        name="swap_cotangent",
    )(*bring(array_t))


def output_kernel(groups, per, chunks, spots, *refs):
    parts, (out_ref, f_ref, y_ref) = refs[:-3], refs[-3:]
    feats, local, width = f_ref.shape
    half = feats // groups // per
    pairs = half // chunks
    size = pairs * local
    lanes = -(-feats // 128) * 128
    here = cell_index()
    for (first_m, some, first_j), part in zip(spots, parts):
        for b in range(part.shape[0]):
            base = (here ^ (first_m + b // some)) * (half * per) + (first_j + b % some) * pairs
            for q in range(per):
                rows = part[b, q * size : (q + 1) * size].reshape(pairs, local, width)
                f_ref[pl.ds(base + q * half, pairs)] = rows
    side = 16
    swap = swap_matrix(side)
    for f in range(0, feats, side):
        for r in range(0, local, side):
            block = f_ref[f : f + side, r : r + side, :].reshape(side * side, width)
            y_ref[r : r + side, f : f + side, :] = dot(swap, block).astype(BF).reshape(side, side, width)
    for r in range(local):
        y = y_ref[r]
        if lanes > feats:
            y = jnp.concatenate([y, jnp.zeros((lanes - feats, width), BF)], axis=0)
        out_ref[r] = y.T[:, :feats]


def make_output(parts, spots, groups, per, chunks, feats, local):
    width = parts[0].shape[-1]
    return pl.pallas_call(
        functools.partial(output_kernel, groups, per, chunks, spots),
        in_specs=[IN_VMEM] * len(parts),
        out_specs=IN_VMEM,
        out_shape=jax.ShapeDtypeStruct((local, width, feats), BF),
        scratch_shapes=[pltpu.VMEM((feats, local, width), BF), pltpu.VMEM((local, feats, width), BF)],
        compiler_params=PARAMS,
        cost_estimate=cost(10**8),
        name="make_output",
    )(*bring(*parts))


def gelu_and_slope(pre):
    size = jnp.abs(pre)
    bell = jnp.exp2(pre * pre * F32(-0.5 * math.log2(math.e)))
    t = 1.0 / (size + F32(ERFC_K))
    poly = F32(ERFC_C[-1])
    for coefficient in ERFC_C[-2::-1]:
        poly = poly * t + F32(coefficient)
    tail = poly * t * bell
    cdf = jnp.where(pre >= 0, 1.0 - tail, tail)
    return pre * cdf, cdf + pre * (bell * F32(1.0 / math.sqrt(2.0 * math.pi)))


def dense_kernel(groups, per, spot, fresh, factor, *refs):
    first_m, chunks, first_j = spot
    last = factor is not None
    blocks = refs[-1].shape[0]
    ins = refs[:blocks]
    win_ref, woutt_ref, cot_ref = refs[blocks : blocks + 3]
    rest = refs[blocks + (3 if fresh else 5) :]
    if last:
        out_ref, gin_ref, gout_ref, keep_ref, send_ref, n_ref = rest
    else:
        out_ref, gin_ref, gout_ref, n_ref = rest
    pairs, local, _ = ins[0].shape
    width, _ = win_ref.shape
    size = pairs * local
    fg = cot_ref.shape[0] // groups
    half = fg // per
    here = cell_index()
    for b in range(blocks):
        for q, part in enumerate(unpack(ins[b][...], per, width)):
            n_ref[b, q * size : (q + 1) * size] = part.reshape(size, width)
    if fresh:
        gin_ref[...] = jnp.zeros_like(gin_ref)
        gout_ref[...] = jnp.zeros_like(gout_ref)
    w_in = win_ref[...]
    w_out_t = woutt_ref[...]

    def step(b):
        group = here ^ (first_m + b // chunks)
        feature = group * fg + (first_j + b % chunks) * pairs
        normed = n_ref[b]
        cot = [cot_ref[pl.ds(feature + q * half, pairs)].reshape(size, width) for q in range(per)]
        cot = jnp.concatenate(cot, axis=0)
        act, slope = gelu_and_slope(dot(normed, w_in))
        act = act.astype(BF)
        out_ref[b] = (normed.astype(F32) + dot(act, w_out_t, NT)).astype(BF)
        dpre = (dot(cot, w_out_t) * slope).astype(BF)
        gin_ref[...] += dot(normed, dpre, TN)
        gout_ref[...] += dot(cot, act, TN)

    loop(blocks, BLOCKS, lambda bs: [step(b) for b in bs])
    if last:
        both = pack([(gin_ref[...].T * F32(factor)).astype(BF), (gout_ref[...].T * F32(factor)).astype(BF)])
        both = both.reshape(keep_ref.shape[0], 2, *keep_ref.shape[1:])
        even = here % 2 == 0
        keep_ref[...] = jnp.where(even, both[:, 0], both[:, 1])
        send_ref[...] = jnp.where(even, both[:, 1], both[:, 0])


def dense_part(blocks, cot_t, w_in, w_out_t, prev, groups, per, spot, factor, shares):
    pairs, local, _ = blocks[0].shape
    width, hid = w_in.shape
    size = per * pairs * local
    count = len(blocks)
    outs = [near((count, size, width))] + [near((width, hid), F32)] * 2
    operands = list(blocks) + [w_in, w_out_t, cot_t]
    alias = {}
    if prev is not None:
        alias = {len(operands) + n: 1 + n for n in range(2)}
        operands += list(prev)
    if factor is not None:
        outs += [near((shares // 2, hid // shares, 2 * width))] * 2
    return pl.pallas_call(
        functools.partial(dense_kernel, groups, per, spot, prev is None, factor),
        in_specs=[IN_VMEM] * len(operands),
        out_specs=[IN_VMEM] * len(outs),
        out_shape=outs,
        input_output_aliases=alias,
        scratch_shapes=[pltpu.VMEM((count, size, width), BF)],
        compiler_params=PARAMS,
        cost_estimate=cost(10**8),
    )(*bring(*operands))


def add_kernel(a_ref, b_ref, out_ref):
    out_ref[...] = (a_ref[...].astype(F32) + b_ref[...].astype(F32)).astype(BF)


def add_pair(a, b):
    return pl.pallas_call(
        add_kernel,
        in_specs=[IN_VMEM] * 2,
        out_specs=IN_VMEM,
        out_shape=near(a.shape),
        compiler_params=PARAMS,
        cost_estimate=cost(10**6),
        name="add_pair",
    )(*bring(a, b))


def exchange(pieces, groups):
    come = [pieces[0]]
    for m in range(1, groups):
        come.append(lax.ppermute(pieces[m], CELLS, [(s, s ^ m) for s in range(groups)]))
    return come


def per_device(
    cells_in, train_count, feat_count, feat_qkv, feat_proj, row_qkv, row_proj, w_in, w_out, cotangent
):
    block_t = jnp.swapaxes(cells_in[0], 1, 2)
    local, width, feats = block_t.shape
    groups = lax.axis_size(CELLS)
    tables = lax.axis_size("tables")
    fg = feats // groups
    per = 2 if fg % 2 == 0 else 1
    half = fg // per
    sub_rows = 16
    row_chunks = local // sub_rows
    feat_chunks = 2 if half % 2 == 0 else 1
    factor = 1.0 / math.sqrt(tables * local * groups * feats)
    pairs = half // feat_chunks
    pieces = [[] for _ in range(feat_chunks)]
    cot_t = jnp.swapaxes(cotangent[0], 1, 2)
    sent = feature_chunk(
        block_t, feat_count, feat_qkv, feat_proj, None, groups, per, 0, sub_rows, 1
    )
    *sent, wqkv_v, wproj_v, rest = sent
    come = exchange(sent, groups)
    for j in range(feat_chunks):
        pieces[j] += come
    *sent, cot_v = feature_chunk(
        rest, feat_count, wqkv_v, wproj_v, cot_t, groups, per, 0, sub_rows, feat_chunks
    )
    for j in range(feat_chunks):
        pieces[j] += exchange(sent[j * groups : (j + 1) * groups], groups)
    cot_t = swap_cotangent(cot_v)
    back = []
    for j in range(feat_chunks):
        starts = (j * pairs, 0)
        done = row_chunk(pieces[j], train_count, row_qkv, row_proj, groups, per, row_chunks, pairs, starts)
        back.append(exchange(done, groups))
    w_out_t = w_out.T
    shares = tables * groups
    near_by = groups // 2
    spots = [(0, feat_chunks, 0)] + [(near_by, 1, j) for j in range(feat_chunks)]
    parts = []
    grads = None
    for spot in spots:
        first_m, some, first_j = spot
        blocks = [back[first_j + j][first_m + m] for m in range(near_by) for j in range(some)]
        scale = factor if spot == spots[-1] else None
        made, *grads = dense_part(blocks, cot_t, w_in, w_out_t, grads, groups, per, spot, scale, shares)
        parts.append(made)
    keep, send = grads[2:]
    other = lax.ppermute(send, "core", [(0, 1), (1, 0)])
    pieces = add_pair(keep, other)
    total = lax.all_to_all(pieces, ("tables", "chips"), split_axis=0, concat_axis=0, tiled=True)
    total = jnp.sum(total.astype(F32), axis=0)
    output = make_output(parts, spots, groups, per, feat_chunks, feats, local)
    grad_in, grad_out = unpack(total, 2, width)
    return (jnp.swapaxes(output, 1, 2)[None], grad_in.T, grad_out)


def solution(mesh):
    tables, cells = mesh.devices.shape
    split = jax.sharding.Mesh(mesh.devices.reshape(tables, cells // 2, 2), ("tables", "chips", "core"))
    spread = P("tables", CELLS, None, None)
    shares = ("tables",) + CELLS
    return jax.shard_map(
        per_device,
        mesh=split,
        in_specs=(spread, P("tables"), P("tables"), P(), P(), P(), P(), P(), P(), spread),
        out_specs=(spread, P(None, shares), P(shares, None)),
        check_vma=False,
    )
```

```python
import functools
import math

import jax
import jax.numpy as jnp
from jax import lax
from jax.experimental import pallas as pl
from jax.experimental.pallas import tpu as pltpu
from jax.sharding import PartitionSpec as P


HEADS = 6
HEAD_DIM = 32
BF = jnp.bfloat16
F32 = jnp.float32
ERFC_K = 2.9
ERFC_C = (
    0.38553786502648235,
    1.4917549496141058,
    -0.32977430445565825,
    21.663540536082817,
    -21.146073738657215,
)
NT = (((1,), (1,)), ((), ()))
TN = (((0,), (0,)), ((), ()))


def dot(a, b, dims=(((1,), (0,)), ((), ()))):
    return lax.dot_general(a, b, dims, preferred_element_type=F32)


def layer_norm(values):
    mean = jnp.mean(values, axis=0, keepdims=True)
    centred = values - mean
    var = jnp.mean(centred * centred, axis=0, keepdims=True)
    return centred * lax.rsqrt(var + 1e-05)


def one_hot(rows, cols):
    row = lax.broadcasted_iota(jnp.int32, (rows, cols), 0)
    col = lax.broadcasted_iota(jnp.int32, (rows, cols), 1)
    return (row == col).astype(F32).astype(BF)


def finish_items(att_ref, ats, w_proj_t, flip, residual_t):
    lanes = att_ref.shape[2]
    mixed = dot(w_proj_t, jnp.concatenate([att_ref[at] for at in ats], axis=1))
    done = []
    for a, at in enumerate(ats):
        normed = layer_norm(residual_t(at).astype(F32) + mixed[:, a * lanes : (a + 1) * lanes]).astype(BF)
        done.append(dot(flip, normed, NT).astype(BF))
    return done


def swap_matrix(side):
    out = lax.broadcasted_iota(jnp.int32, (side * side, side * side), 0)
    src = lax.broadcasted_iota(jnp.int32, (side * side, side * side), 1)
    return (src == (out % side) * side + out // side).astype(F32).astype(BF)


def pack(parts):
    if len(parts) == 1:
        return parts[0]
    a, b = parts
    cut = a.shape[-1] // 128 * 128
    return jnp.concatenate([a[..., :cut], b[..., :cut], a[..., cut:], b[..., cut:]], axis=-1)


def unpack(block, per, width):
    if per == 1:
        return [block]
    cut = width // 128 * 128
    rest = width - cut
    return [
        jnp.concatenate(
            [block[..., q * cut : (q + 1) * cut], block[..., 2 * cut + q * rest : 2 * cut + (q + 1) * rest]],
            axis=-1,
        )
        for q in range(2)
    ]


CELLS = ("chips", "core")


def cell_index():
    return lax.axis_index("chips") * 2 + lax.axis_index("core")


def mask_of(keys, count):
    rows = lax.broadcasted_iota(jnp.int32, (keys, 1), 0) < count
    lanes = lax.broadcasted_iota(jnp.int32, (1, keys), 1) < count
    return rows, lanes


def keep_projected(refs, at, q_v, k_rows, masks):
    q_ref, k_ref, v_ref = refs
    width, keys = q_ref.shape[1], k_ref.shape[1]
    key_row, key_lane = masks
    scale = F32(math.log2(math.e) / math.sqrt(HEAD_DIM))
    q_ref[at] = (q_v[:width] * scale).astype(BF)
    v_ref[at] = jnp.where(key_lane, q_v[width:, :keys], F32(0)).astype(BF)
    k_ref[at] = jnp.where(key_row, k_rows[:keys], k_rows[0:1]).astype(BF)


def score_blocks(q_own, lanes):
    hd = HEAD_DIM
    width = q_own.shape[0]
    blank = jnp.zeros((hd, lanes), BF)
    blocks = []
    for i in range(HEADS // 2):
        lo = 2 * i * hd
        tile = lo // 128 * 128
        end = min(tile + 128, width)
        pieces = [
            jnp.concatenate([q_own[lo : lo + hd], blank], axis=1),
            jnp.concatenate([blank, q_own[lo + hd : lo + 2 * hd]], axis=1),
        ]
        if lo > tile:
            pieces = [jnp.zeros((lo - tile, 2 * lanes), BF)] + pieces
        if lo + 2 * hd < end:
            pieces = pieces + [jnp.zeros((end - lo - 2 * hd, 2 * lanes), BF)]
        blocks.append((tile, end, jnp.concatenate(pieces, axis=0)))
    return blocks


def attend(refs, att_ref, ats, ones):
    q_ref, k_ref, v_ref = refs
    lanes = q_ref.shape[2]
    hd = HEAD_DIM
    scores = []
    for at in ats:
        k_own = k_ref[at]
        for tile, end, block in score_blocks(q_ref[at], lanes):
            scores.append(dot(k_own[:, tile:end], block))
    weights = [jnp.exp2(s - jnp.max(s, axis=0, keepdims=True)).astype(BF) for s in scores]
    for n, at in enumerate(ats):
        v_own = v_ref[at]
        for i in range(HEADS // 2):
            lo = 2 * i * hd
            lhs = jnp.concatenate([v_own[lo : lo + 2 * hd], ones], axis=0)
            mixed = dot(lhs, weights[n * (HEADS // 2) + i])
            scale = 1.0 / mixed[2 * hd : 2 * hd + 1]
            att_ref[at, lo : lo + hd] = (mixed[:hd, :lanes] * scale[:, :lanes]).astype(BF)
            att_ref[at, lo + hd : lo + 2 * hd] = (mixed[hd : 2 * hd, lanes:] * scale[:, lanes:]).astype(BF)


def loop(count, most, body):
    group = max(d for d in range(1, most + 1) if count % d == 0)

    def step(i, carry):
        body([i * group + a for a in range(group)])
        return carry

    lax.fori_loop(0, count // group, step, 0)


def pad_lanes(value, lanes):
    rows, n = value.shape
    return value if n == lanes else jnp.concatenate([value, jnp.zeros((rows, lanes - n), value.dtype)], axis=1)


def feature_kernel(groups, per, base, rows, cuts, lead, *refs):
    count_ref, cells_ref, wqkv_ref, wproj_ref, *refs = refs
    count = count_ref[0]
    first = base
    if lead:
        outs = refs[: groups * len(cuts)]
        wqkv_buf, wproj_buf, rest_buf, *refs = refs[groups * len(cuts) :]
        sems, cells_buf = refs[6:]
        moves = [(wqkv_ref, wqkv_buf), (wproj_ref, wproj_buf), (cells_ref.at[pl.ds(0, rows)], cells_buf)]
        late = (cells_ref.at[pl.ds(rows, rest_buf.shape[0])], rest_buf)
        moves = [pltpu.make_async_copy(a, b, sems.at[n]) for n, (a, b) in enumerate(moves)]
        late = pltpu.make_async_copy(*late, sems.at[3])
        for move in moves:
            move.start()
        for move in moves:
            move.wait()
        wqkv_ref, wproj_ref, cells_ref = wqkv_buf, wproj_buf, cells_buf
    else:
        cot_ref, *refs = refs
        outs = refs[: groups * len(cuts)]
        cot_buf, *refs = refs[groups * len(cuts) :]
        late = pltpu.make_async_copy(cot_ref, cot_buf, refs[6].at[0])
    late.start()
    refs = refs[:6]
    q_ref, k_ref, v_ref, att_ref, mid_ref, swap_ref = refs
    _, width, feats = cells_ref.shape
    lanes = q_ref.shape[2]
    fg = feats // groups
    half = fg // per
    w_t = wqkv_ref[...].T
    w_qv = jnp.concatenate([w_t[:width], w_t[2 * width :]], axis=0)
    w_k = w_t[width : 2 * width]
    w_proj_t = wproj_ref[...].T
    flip = one_hot(feats, lanes)
    masks = mask_of(feats, count)
    ones = jnp.broadcast_to(jnp.where(masks[1], F32(1), F32(0)), (16, feats)).astype(BF)
    kept = (q_ref, k_ref, v_ref)

    def project(ats):
        x_t = [pad_lanes(cells_ref[first + at], lanes) for at in ats]
        q_v = dot(w_qv, jnp.concatenate(x_t, axis=1))
        x = [t.T[:feats] for t in x_t]
        k = dot(jnp.concatenate(x, axis=0), w_k, NT)
        for a, at in enumerate(ats):
            keep_projected(kept, at, q_v[:, a * lanes : (a + 1) * lanes], k[a * feats : (a + 1) * feats], masks)

    def finish(ats):
        own = lambda at: pad_lanes(cells_ref[first + at], lanes)
        for at, value in zip(ats, finish_items(att_ref, ats, w_proj_t, flip, own)):
            mid_ref[at] = value

    loop(rows, 16, project)
    loop(rows, 8, lambda ats: attend(kept, att_ref, ats, ones))
    loop(rows, 16, finish)
    swap = swap_matrix(rows)
    for f in range(feats // rows):
        block = mid_ref[:, f * rows : (f + 1) * rows, :].reshape(rows * rows, width)
        swap_ref[f * rows : (f + 1) * rows] = dot(swap, block).astype(BF).reshape(rows, rows, width)
    here = cell_index()
    for c, size in enumerate(cuts):
        for m in range(groups):
            base = (here ^ m) * fg + sum(cuts[:c])
            outs[c * groups + m][...] = pack([swap_ref[pl.ds(base + q * half, size)] for q in range(per)])
    late.wait()


BLOCKS = 2
IN_VMEM = pl.BlockSpec(memory_space=pltpu.VMEM)
IN_SMEM = pl.BlockSpec(memory_space=pltpu.SMEM)


def attention_scratch(items, width, lanes, keys):
    return [
        pltpu.VMEM((items, width, lanes), BF),
        pltpu.VMEM((items, keys, width), BF),
        pltpu.VMEM((items, width, keys), BF),
        pltpu.VMEM((items, width, lanes), BF),
    ]


def near(shape, dtype=BF):
    return pltpu.VMEM(shape, dtype)


def bring(*arrays):
    return [pltpu.with_memory_space_constraint(x, pltpu.VMEM) for x in arrays]


PARAMS = pltpu.CompilerParams(vmem_limit_bytes=14 * 2**20)


def cost(flops):
    return pl.CostEstimate(flops=flops, transcendentals=0, bytes_accessed=10**6)


def feature_chunk(cells_t, count, wqkv, wproj, cot_t, groups, per, base, rows, cuts):
    whole, width, feats = cells_t.shape
    lanes = -(-feats // 128) * 128
    far = pl.BlockSpec(memory_space=pltpu.HBM)
    lead = cot_t is None
    outs = [near((size, rows, per * width)) for size in cuts for _ in range(groups)]
    scratch = attention_scratch(rows, width, lanes, feats)
    scratch += [pltpu.VMEM((rows, feats, width), BF), pltpu.VMEM((feats, rows, width), BF)]
    operands = [cells_t, wqkv, wproj]
    if lead:
        operands = [pltpu.with_memory_space_constraint(x, pltpu.HBM) for x in operands]
        specs = [far] * 3
        outs += [near(wqkv.shape), near(wproj.shape), near((whole - rows, width, feats))]
        scratch += [pltpu.SemaphoreType.DMA((4,)), pltpu.VMEM((rows, width, feats), BF)]
    else:
        operands = bring(*operands) + [pltpu.with_memory_space_constraint(cot_t, pltpu.HBM)]
        specs = [IN_VMEM] * 3 + [far]
        outs += [near(cot_t.shape)]
        scratch += [pltpu.SemaphoreType.DMA((1,))]
    return pl.pallas_call(
        functools.partial(feature_kernel, groups, per, base, rows, cuts, lead),
        in_specs=[IN_SMEM] + specs,
        out_specs=[IN_VMEM] * len(outs),
        out_shape=outs,
        scratch_shapes=scratch,
        compiler_params=PARAMS,
        cost_estimate=cost(10**8),
        name="feature_0" if lead else "feature_1",
    )(count, *operands)


def row_kernel(groups, per, chunks, firsts, count_ref, wqkv_ref, wproj_ref, *refs):
    ins = refs[: groups * chunks]
    outs = refs[groups * chunks : groups * chunks + groups]
    q_ref, k_ref, v_ref, att_ref, x_ref, xt_ref, y_ref = refs[groups * chunks + groups :]
    pairs, local, _ = outs[0].shape
    sub_rows = local // chunks
    items, rows, width = x_ref.shape
    keys = k_ref.shape[1]
    count = count_ref[0]
    w_t = wqkv_ref[...].T
    w_qv = jnp.concatenate([w_t[:width], w_t[2 * width :], one_hot(width, width)], axis=0)
    w_k = w_t[width : 2 * width]
    w_proj_t = wproj_ref[...].T
    flip = one_hot(rows, rows)
    masks = mask_of(keys, count)
    ones = jnp.broadcast_to(jnp.where(masks[1], F32(1), F32(0)), (16, keys)).astype(BF)
    kept = (q_ref, k_ref, v_ref)
    here = cell_index()
    for m in range(groups):
        for k in range(chunks):
            at = pl.multiple_of((here ^ m) * local + k * sub_rows, sub_rows)
            for q, part in enumerate(unpack(ins[k * groups + m][firsts[k] : firsts[k] + pairs], per, width)):
                x_ref[q * pairs : (q + 1) * pairs, pl.ds(at, sub_rows), :] = part

    def project(ats):
        x = jnp.concatenate([x_ref[at] for at in ats], axis=0)
        q_v = dot(w_qv, x, NT)
        for a, at in enumerate(ats):
            k = dot(x[a * rows : a * rows + keys], w_k, NT)
            own = q_v[:, a * rows : (a + 1) * rows]
            xt_ref[at] = own[2 * width :].astype(BF)
            keep_projected(kept, at, own[: 2 * width], k, masks)

    def finish(ps):
        ats = [q * pairs + p for p in ps for q in range(per)]
        done = finish_items(att_ref, ats, w_proj_t, flip, lambda at: xt_ref[at])
        for a, p in enumerate(ps):
            y_ref[p] = pack(done[a * per : (a + 1) * per])

    most = max(1, 1024 // rows)
    loop(items, min(2 * most, 16), project)
    loop(items, min(most, 8), lambda ats: attend(kept, att_ref, ats, ones))
    loop(pairs, min(most, 8), finish)
    for m in range(groups):
        at = pl.multiple_of((here ^ m) * local, local)
        outs[m][...] = y_ref[:, pl.ds(at, local), :]


def row_chunk(pieces, count, wqkv, wproj, groups, per, chunks, pairs, firsts):
    sub_rows, packed = pieces[0].shape[1:]
    width = wproj.shape[0]
    local = sub_rows * chunks
    rows = local * groups
    keys = rows - rows // 4
    return pl.pallas_call(
        functools.partial(row_kernel, groups, per, chunks, firsts),
        in_specs=[IN_SMEM] + [IN_VMEM] * (2 + len(pieces)),
        out_specs=[IN_VMEM] * groups,
        out_shape=[near((pairs, local, packed))] * groups,
        scratch_shapes=attention_scratch(pairs * per, width, rows, keys)
        + [
            pltpu.VMEM((pairs * per, rows, width), BF),
            pltpu.VMEM((pairs * per, width, rows), BF),
            pltpu.VMEM((pairs, rows, packed), BF),
        ],
        compiler_params=PARAMS,
        cost_estimate=cost(10**8),
    )(count, *bring(wqkv, wproj, *pieces))


def swap_kernel(in_ref, out_ref, x_ref):
    first, width, second = in_ref.shape
    lanes = -(-second // 128) * 128
    side = 16
    swap = swap_matrix(side)
    for a in range(first):
        x_ref[a] = pad_lanes(in_ref[a], lanes).T[:second]
    for a in range(first // side):
        for b in range(second // side):
            block = x_ref[a * side : (a + 1) * side, b * side : (b + 1) * side, :]
            swapped = dot(swap, block.reshape(side * side, width)).astype(BF)
            out_ref[b * side : (b + 1) * side, a * side : (a + 1) * side, :] = swapped.reshape(side, side, width)


def swap_cotangent(array_t):
    first, width, second = array_t.shape
    return pl.pallas_call(
        swap_kernel,
        in_specs=[IN_VMEM],
        out_specs=IN_VMEM,
        out_shape=near((second, first, width)),
        scratch_shapes=[pltpu.VMEM((first, second, width), BF)],
        compiler_params=PARAMS,
        cost_estimate=cost(10**8),
        name="swap_cotangent",
    )(*bring(array_t))


def output_kernel(groups, per, spots, *refs):
    parts, (out_ref, f_ref, y_ref) = refs[:-3], refs[-3:]
    feats, local, width = f_ref.shape
    half = feats // groups // per
    lanes = -(-feats // 128) * 128
    here = cell_index()
    for (first_m, start, pairs), part in zip(spots, parts):
        size = pairs * local
        for b in range(part.shape[0]):
            base = (here ^ (first_m + b)) * (half * per) + start
            for q in range(per):
                rows = part[b, q * size : (q + 1) * size].reshape(pairs, local, width)
                f_ref[pl.ds(base + q * half, pairs)] = rows
    side = 16
    swap = swap_matrix(side)
    for f in range(0, feats, side):
        for r in range(0, local, side):
            block = f_ref[f : f + side, r : r + side, :].reshape(side * side, width)
            y_ref[r : r + side, f : f + side, :] = dot(swap, block).astype(BF).reshape(side, side, width)
    for r in range(local):
        y = y_ref[r]
        if lanes > feats:
            y = jnp.concatenate([y, jnp.zeros((lanes - feats, width), BF)], axis=0)
        out_ref[r] = y.T[:, :feats]


def make_output(parts, spots, groups, per, feats, local):
    width = parts[0].shape[-1]
    return pl.pallas_call(
        functools.partial(output_kernel, groups, per, spots),
        in_specs=[IN_VMEM] * len(parts),
        out_specs=IN_VMEM,
        out_shape=jax.ShapeDtypeStruct((local, width, feats), BF),
        scratch_shapes=[pltpu.VMEM((feats, local, width), BF), pltpu.VMEM((local, feats, width), BF)],
        compiler_params=PARAMS,
        cost_estimate=cost(10**8),
        name="make_output",
    )(*bring(*parts))


def gelu_and_slope(pre):
    size = jnp.abs(pre)
    bell = jnp.exp2(pre * pre * F32(-0.5 * math.log2(math.e)))
    t = 1.0 / (size + F32(ERFC_K))
    poly = F32(ERFC_C[-1])
    for coefficient in ERFC_C[-2::-1]:
        poly = poly * t + F32(coefficient)
    tail = poly * t * bell
    cdf = jnp.where(pre >= 0, 1.0 - tail, tail)
    return pre * cdf, cdf + pre * (bell * F32(1.0 / math.sqrt(2.0 * math.pi)))


def dense_kernel(groups, per, spot, fresh, factor, *refs):
    first_m, start, _ = spot
    last = factor is not None
    blocks = refs[-1].shape[0]
    ins = refs[:blocks]
    win_ref, woutt_ref, cot_ref = refs[blocks : blocks + 3]
    rest = refs[blocks + (3 if fresh else 5) :]
    if last:
        out_ref, gin_ref, gout_ref, keep_ref, send_ref, n_ref = rest
    else:
        out_ref, gin_ref, gout_ref, n_ref = rest
    pairs, local, _ = ins[0].shape
    width, _ = win_ref.shape
    size = pairs * local
    fg = cot_ref.shape[0] // groups
    half = fg // per
    here = cell_index()
    for b in range(blocks):
        for q, part in enumerate(unpack(ins[b][...], per, width)):
            n_ref[b, q * size : (q + 1) * size] = part.reshape(size, width)
    if fresh:
        gin_ref[...] = jnp.zeros_like(gin_ref)
        gout_ref[...] = jnp.zeros_like(gout_ref)
    w_in = win_ref[...]
    w_out_t = woutt_ref[...]

    def step(b):
        feature = (here ^ (first_m + b)) * fg + start
        normed = n_ref[b]
        cot = [cot_ref[pl.ds(feature + q * half, pairs)].reshape(size, width) for q in range(per)]
        cot = jnp.concatenate(cot, axis=0)
        act, slope = gelu_and_slope(dot(normed, w_in))
        act = act.astype(BF)
        out_ref[b] = (normed.astype(F32) + dot(act, w_out_t, NT)).astype(BF)
        dpre = (dot(cot, w_out_t) * slope).astype(BF)
        gin_ref[...] += dot(normed, dpre, TN)
        gout_ref[...] += dot(cot, act, TN)

    loop(blocks, BLOCKS, lambda bs: [step(b) for b in bs])
    if last:
        both = pack([(gin_ref[...].T * F32(factor)).astype(BF), (gout_ref[...].T * F32(factor)).astype(BF)])
        both = both.reshape(keep_ref.shape[0], 2, *keep_ref.shape[1:])
        even = here % 2 == 0
        keep_ref[...] = jnp.where(even, both[:, 0], both[:, 1])
        send_ref[...] = jnp.where(even, both[:, 1], both[:, 0])


def dense_part(blocks, cot_t, w_in, w_out_t, prev, groups, per, spot, factor, shares):
    pairs, local, _ = blocks[0].shape
    width, hid = w_in.shape
    size = per * pairs * local
    count = len(blocks)
    outs = [near((count, size, width))] + [near((width, hid), F32)] * 2
    operands = list(blocks) + [w_in, w_out_t, cot_t]
    alias = {}
    if prev is not None:
        alias = {len(operands) + n: 1 + n for n in range(2)}
        operands += list(prev)
    if factor is not None:
        outs += [near((shares // 2, hid // shares, 2 * width))] * 2
    return pl.pallas_call(
        functools.partial(dense_kernel, groups, per, spot, prev is None, factor),
        in_specs=[IN_VMEM] * len(operands),
        out_specs=[IN_VMEM] * len(outs),
        out_shape=outs,
        input_output_aliases=alias,
        scratch_shapes=[pltpu.VMEM((count, size, width), BF)],
        compiler_params=PARAMS,
        cost_estimate=cost(10**8),
    )(*bring(*operands))


def add_kernel(a_ref, b_ref, out_ref):
    out_ref[...] = (a_ref[...].astype(F32) + b_ref[...].astype(F32)).astype(BF)


def add_pair(a, b):
    return pl.pallas_call(
        add_kernel,
        in_specs=[IN_VMEM] * 2,
        out_specs=IN_VMEM,
        out_shape=near(a.shape),
        compiler_params=PARAMS,
        cost_estimate=cost(10**6),
        name="add_pair",
    )(*bring(a, b))


def exchange(pieces, groups):
    come = [pieces[0]]
    for m in range(1, groups):
        come.append(lax.ppermute(pieces[m], CELLS, [(s, s ^ m) for s in range(groups)]))
    return come


def per_device(
    cells_in, train_count, feat_count, feat_qkv, feat_proj, row_qkv, row_proj, w_in, w_out, cotangent
):
    block_t = jnp.swapaxes(cells_in[0], 1, 2)
    local, width, feats = block_t.shape
    groups = lax.axis_size(CELLS)
    tables = lax.axis_size("tables")
    fg = feats // groups
    per = 2 if fg % 2 == 0 else 1
    half = fg // per
    sub_rows = 16
    row_chunks = local // sub_rows
    sizes = (half * 3 // 7, half - half * 3 // 7) if half % 2 == 0 else (half,)
    offsets = [sum(sizes[:j]) for j in range(len(sizes))]
    feat_chunks = len(sizes)
    factor = 1.0 / math.sqrt(tables * local * groups * feats)
    pieces = [[] for _ in range(feat_chunks)]
    cot_t = jnp.swapaxes(cotangent[0], 1, 2)
    sent = feature_chunk(
        block_t, feat_count, feat_qkv, feat_proj, None, groups, per, 0, sub_rows, (half,)
    )
    *sent, wqkv_v, wproj_v, rest = sent
    come = exchange(sent, groups)
    for j in range(feat_chunks):
        pieces[j] += come
    *sent, cot_v = feature_chunk(
        rest, feat_count, wqkv_v, wproj_v, cot_t, groups, per, 0, sub_rows, sizes
    )
    for j in range(feat_chunks):
        pieces[j] += exchange(sent[j * groups : (j + 1) * groups], groups)
    cot_t = swap_cotangent(cot_v)
    back = []
    for j in range(feat_chunks):
        starts = (offsets[j], 0)
        done = row_chunk(pieces[j], train_count, row_qkv, row_proj, groups, per, row_chunks, sizes[j], starts)
        back.append(exchange(done, groups))
    w_out_t = w_out.T
    shares = tables * groups
    near_by = groups // 2
    spots = [(m, offsets[j], sizes[j]) for m in (0, near_by) for j in range(feat_chunks)]
    parts = []
    grads = None
    for spot in spots:
        first_m, start, _ = spot
        blocks = [back[offsets.index(start)][first_m + m] for m in range(near_by)]
        scale = factor if spot == spots[-1] else None
        made, *grads = dense_part(blocks, cot_t, w_in, w_out_t, grads, groups, per, spot, scale, shares)
        parts.append(made)
    keep, send = grads[2:]
    other = lax.ppermute(send, "core", [(0, 1), (1, 0)])
    pieces = add_pair(keep, other)
    total = lax.all_to_all(pieces, ("tables", "chips"), split_axis=0, concat_axis=0, tiled=True)
    total = jnp.sum(total.astype(F32), axis=0)
    output = make_output(parts, spots, groups, per, feats, local)
    grad_in, grad_out = unpack(total, 2, width)
    return (jnp.swapaxes(output, 1, 2)[None], grad_in.T, grad_out)


def solution(mesh):
    tables, cells = mesh.devices.shape
    split = jax.sharding.Mesh(mesh.devices.reshape(tables, cells // 2, 2), ("tables", "chips", "core"))
    spread = P("tables", CELLS, None, None)
    shares = ("tables",) + CELLS
    return jax.shard_map(
        per_device,
        mesh=split,
        in_specs=(spread, P("tables"), P("tables"), P(), P(), P(), P(), P(), P(), spread),
        out_specs=(spread, P(None, shares), P(shares, None)),
        check_vma=False,
    )
```

```python
import functools
import math

import jax
import jax.numpy as jnp
from jax import lax
from jax.experimental import pallas as pl
from jax.experimental.pallas import tpu as pltpu
from jax.sharding import PartitionSpec as P


HEADS = 6
HEAD_DIM = 32
BF = jnp.bfloat16
F32 = jnp.float32
ERFC_K = 2.9
ERFC_C = (
    0.38553786502648235,
    1.4917549496141058,
    -0.32977430445565825,
    21.663540536082817,
    -21.146073738657215,
)
NT = (((1,), (1,)), ((), ()))
TN = (((0,), (0,)), ((), ()))


def dot(a, b, dims=(((1,), (0,)), ((), ()))):
    return lax.dot_general(a, b, dims, preferred_element_type=F32)


def layer_norm(values):
    mean = jnp.mean(values, axis=0, keepdims=True)
    centred = values - mean
    var = jnp.mean(centred * centred, axis=0, keepdims=True)
    return centred * lax.rsqrt(var + 1e-05)


def one_hot(rows, cols):
    row = lax.broadcasted_iota(jnp.int32, (rows, cols), 0)
    col = lax.broadcasted_iota(jnp.int32, (rows, cols), 1)
    return (row == col).astype(F32).astype(BF)


def finish_items(att_ref, ats, w_proj_t, flip, residual_t):
    lanes = att_ref.shape[2]
    mixed = dot(w_proj_t, jnp.concatenate([att_ref[at] for at in ats], axis=1))
    done = []
    for a, at in enumerate(ats):
        normed = layer_norm(residual_t(at).astype(F32) + mixed[:, a * lanes : (a + 1) * lanes]).astype(BF)
        done.append(dot(flip, normed, NT).astype(BF))
    return done


def swap_matrix(side):
    out = lax.broadcasted_iota(jnp.int32, (side * side, side * side), 0)
    src = lax.broadcasted_iota(jnp.int32, (side * side, side * side), 1)
    return (src == (out % side) * side + out // side).astype(F32).astype(BF)


def pack(parts):
    if len(parts) == 1:
        return parts[0]
    a, b = parts
    cut = a.shape[-1] // 128 * 128
    return jnp.concatenate([a[..., :cut], b[..., :cut], a[..., cut:], b[..., cut:]], axis=-1)


def unpack(block, per, width):
    if per == 1:
        return [block]
    cut = width // 128 * 128
    rest = width - cut
    return [
        jnp.concatenate(
            [block[..., q * cut : (q + 1) * cut], block[..., 2 * cut + q * rest : 2 * cut + (q + 1) * rest]],
            axis=-1,
        )
        for q in range(2)
    ]


CELLS = ("chips", "core")


def cell_index():
    return lax.axis_index("chips") * 2 + lax.axis_index("core")


def mask_of(keys, count):
    rows = lax.broadcasted_iota(jnp.int32, (keys, 1), 0) < count
    lanes = lax.broadcasted_iota(jnp.int32, (1, keys), 1) < count
    return rows, lanes


def keep_projected(refs, at, q_v, k_rows, masks):
    q_ref, k_ref, v_ref = refs
    width, keys = q_ref.shape[1], k_ref.shape[1]
    key_row, key_lane = masks
    scale = F32(math.log2(math.e) / math.sqrt(HEAD_DIM))
    q_ref[at] = (q_v[:width] * scale).astype(BF)
    v_ref[at] = jnp.where(key_lane, q_v[width:, :keys], F32(0)).astype(BF)
    k_ref[at] = jnp.where(key_row, k_rows[:keys], k_rows[0:1]).astype(BF)


def score_blocks(q_own, lanes):
    hd = HEAD_DIM
    width = q_own.shape[0]
    blank = jnp.zeros((hd, lanes), BF)
    blocks = []
    for i in range(HEADS // 2):
        lo = 2 * i * hd
        tile = lo // 128 * 128
        end = min(tile + 128, width)
        pieces = [
            jnp.concatenate([q_own[lo : lo + hd], blank], axis=1),
            jnp.concatenate([blank, q_own[lo + hd : lo + 2 * hd]], axis=1),
        ]
        if lo > tile:
            pieces = [jnp.zeros((lo - tile, 2 * lanes), BF)] + pieces
        if lo + 2 * hd < end:
            pieces = pieces + [jnp.zeros((end - lo - 2 * hd, 2 * lanes), BF)]
        blocks.append((tile, end, jnp.concatenate(pieces, axis=0)))
    return blocks


def attend(refs, att_ref, ats, ones):
    q_ref, k_ref, v_ref = refs
    lanes = q_ref.shape[2]
    hd = HEAD_DIM
    scores = []
    for at in ats:
        k_own = k_ref[at]
        for tile, end, block in score_blocks(q_ref[at], lanes):
            scores.append(dot(k_own[:, tile:end], block))
    weights = [jnp.exp2(s - jnp.max(s, axis=0, keepdims=True)).astype(BF) for s in scores]
    for n, at in enumerate(ats):
        v_own = v_ref[at]
        for i in range(HEADS // 2):
            lo = 2 * i * hd
            lhs = jnp.concatenate([v_own[lo : lo + 2 * hd], ones], axis=0)
            mixed = dot(lhs, weights[n * (HEADS // 2) + i])
            scale = 1.0 / mixed[2 * hd : 2 * hd + 1]
            att_ref[at, lo : lo + hd] = (mixed[:hd, :lanes] * scale[:, :lanes]).astype(BF)
            att_ref[at, lo + hd : lo + 2 * hd] = (mixed[hd : 2 * hd, lanes:] * scale[:, lanes:]).astype(BF)


def loop(count, most, body):
    group = max(d for d in range(1, most + 1) if count % d == 0)

    def step(i, carry):
        body([i * group + a for a in range(group)])
        return carry

    lax.fori_loop(0, count // group, step, 0)


def pad_lanes(value, lanes):
    rows, n = value.shape
    return value if n == lanes else jnp.concatenate([value, jnp.zeros((rows, lanes - n), value.dtype)], axis=1)


def feature_kernel(groups, per, base, rows, cuts, lead, *refs):
    count_ref, cells_ref, wqkv_ref, wproj_ref, *refs = refs
    count = count_ref[0]
    first = base
    if lead:
        outs = refs[: groups * len(cuts)]
        wqkv_buf, wproj_buf, rest_buf, *refs = refs[groups * len(cuts) :]
        sems, cells_buf = refs[6:]
        moves = [(wqkv_ref, wqkv_buf)]
        for n in range(0, rows, 4):
            moves.append((cells_ref.at[pl.ds(n, 4)], cells_buf.at[pl.ds(n, 4)]))
        moves.append((wproj_ref, wproj_buf))
        late = (cells_ref.at[pl.ds(rows, rest_buf.shape[0])], rest_buf)
        moves = [pltpu.make_async_copy(a, b, sems.at[n]) for n, (a, b) in enumerate(moves)]
        late = pltpu.make_async_copy(*late, sems.at[len(moves)])
        for move in moves:
            move.start()
        for move in moves:
            move.wait()
        wqkv_ref, wproj_ref, cells_ref = wqkv_buf, wproj_buf, cells_buf
    else:
        cot_ref, *refs = refs
        outs = refs[: groups * len(cuts)]
        cot_buf, *refs = refs[groups * len(cuts) :]
        late = pltpu.make_async_copy(cot_ref, cot_buf, refs[6].at[0])
    late.start()
    refs = refs[:6]
    q_ref, k_ref, v_ref, att_ref, mid_ref, swap_ref = refs
    _, width, feats = cells_ref.shape
    lanes = q_ref.shape[2]
    fg = feats // groups
    half = fg // per
    w_t = wqkv_ref[...].T
    w_qv = jnp.concatenate([w_t[:width], w_t[2 * width :]], axis=0)
    w_k = w_t[width : 2 * width]
    w_proj_t = wproj_ref[...].T
    flip = one_hot(feats, lanes)
    masks = mask_of(feats, count)
    ones = jnp.broadcast_to(jnp.where(masks[1], F32(1), F32(0)), (16, feats)).astype(BF)
    kept = (q_ref, k_ref, v_ref)

    def project(ats):
        x_t = [pad_lanes(cells_ref[first + at], lanes) for at in ats]
        q_v = dot(w_qv, jnp.concatenate(x_t, axis=1))
        x = [t.T[:feats] for t in x_t]
        k = dot(jnp.concatenate(x, axis=0), w_k, NT)
        for a, at in enumerate(ats):
            keep_projected(kept, at, q_v[:, a * lanes : (a + 1) * lanes], k[a * feats : (a + 1) * feats], masks)

    def finish(ats):
        own = lambda at: pad_lanes(cells_ref[first + at], lanes)
        for at, value in zip(ats, finish_items(att_ref, ats, w_proj_t, flip, own)):
            mid_ref[at] = value

    loop(rows, 16, project)
    loop(rows, 8, lambda ats: attend(kept, att_ref, ats, ones))
    loop(rows, 16, finish)
    swap = swap_matrix(rows)
    for f in range(feats // rows):
        block = mid_ref[:, f * rows : (f + 1) * rows, :].reshape(rows * rows, width)
        swap_ref[f * rows : (f + 1) * rows] = dot(swap, block).astype(BF).reshape(rows, rows, width)
    here = cell_index()
    for c, size in enumerate(cuts):
        for m in range(groups):
            base = (here ^ m) * fg + sum(cuts[:c])
            outs[c * groups + m][...] = pack([swap_ref[pl.ds(base + q * half, size)] for q in range(per)])
    late.wait()


BLOCKS = 2
IN_VMEM = pl.BlockSpec(memory_space=pltpu.VMEM)
IN_SMEM = pl.BlockSpec(memory_space=pltpu.SMEM)


def attention_scratch(items, width, lanes, keys):
    return [
        pltpu.VMEM((items, width, lanes), BF),
        pltpu.VMEM((items, keys, width), BF),
        pltpu.VMEM((items, width, keys), BF),
        pltpu.VMEM((items, width, lanes), BF),
    ]


def near(shape, dtype=BF):
    return pltpu.VMEM(shape, dtype)


def bring(*arrays):
    return [pltpu.with_memory_space_constraint(x, pltpu.VMEM) for x in arrays]


PARAMS = pltpu.CompilerParams(vmem_limit_bytes=14 * 2**20)


def cost(flops):
    return pl.CostEstimate(flops=flops, transcendentals=0, bytes_accessed=10**6)


def feature_chunk(cells_t, count, wqkv, wproj, cot_t, groups, per, base, rows, cuts):
    whole, width, feats = cells_t.shape
    lanes = -(-feats // 128) * 128
    far = pl.BlockSpec(memory_space=pltpu.HBM)
    lead = cot_t is None
    outs = [near((size, rows, per * width)) for size in cuts for _ in range(groups)]
    scratch = attention_scratch(rows, width, lanes, feats)
    scratch += [pltpu.VMEM((rows, feats, width), BF), pltpu.VMEM((feats, rows, width), BF)]
    operands = [cells_t, wqkv, wproj]
    if lead:
        operands = [pltpu.with_memory_space_constraint(x, pltpu.HBM) for x in operands]
        specs = [far] * 3
        outs += [near(wqkv.shape), near(wproj.shape), near((whole - rows, width, feats))]
        scratch += [pltpu.SemaphoreType.DMA((3 + rows // 4,)), pltpu.VMEM((rows, width, feats), BF)]
    else:
        operands = bring(*operands) + [pltpu.with_memory_space_constraint(cot_t, pltpu.HBM)]
        specs = [IN_VMEM] * 3 + [far]
        outs += [near(cot_t.shape)]
        scratch += [pltpu.SemaphoreType.DMA((1,))]
    return pl.pallas_call(
        functools.partial(feature_kernel, groups, per, base, rows, cuts, lead),
        in_specs=[IN_SMEM] + specs,
        out_specs=[IN_VMEM] * len(outs),
        out_shape=outs,
        scratch_shapes=scratch,
        compiler_params=PARAMS,
        cost_estimate=cost(10**8),
        name="feature_0" if lead else "feature_1",
    )(count, *operands)


def row_kernel(groups, per, chunks, firsts, count_ref, wqkv_ref, wproj_ref, *refs):
    ins = refs[: groups * chunks]
    outs = refs[groups * chunks : groups * chunks + groups]
    q_ref, k_ref, v_ref, att_ref, x_ref, xt_ref, y_ref = refs[groups * chunks + groups :]
    pairs, local, _ = outs[0].shape
    sub_rows = local // chunks
    items, rows, width = x_ref.shape
    keys = k_ref.shape[1]
    count = count_ref[0]
    w_t = wqkv_ref[...].T
    w_qv = jnp.concatenate([w_t[:width], w_t[2 * width :], one_hot(width, width)], axis=0)
    w_k = w_t[width : 2 * width]
    w_proj_t = wproj_ref[...].T
    flip = one_hot(rows, rows)
    masks = mask_of(keys, count)
    ones = jnp.broadcast_to(jnp.where(masks[1], F32(1), F32(0)), (16, keys)).astype(BF)
    kept = (q_ref, k_ref, v_ref)
    here = cell_index()
    for m in range(groups):
        for k in range(chunks):
            at = pl.multiple_of((here ^ m) * local + k * sub_rows, sub_rows)
            for q, part in enumerate(unpack(ins[k * groups + m][firsts[k] : firsts[k] + pairs], per, width)):
                x_ref[q * pairs : (q + 1) * pairs, pl.ds(at, sub_rows), :] = part

    def project(ats):
        x = jnp.concatenate([x_ref[at] for at in ats], axis=0)
        q_v = dot(w_qv, x, NT)
        for a, at in enumerate(ats):
            k = dot(x[a * rows : a * rows + keys], w_k, NT)
            own = q_v[:, a * rows : (a + 1) * rows]
            xt_ref[at] = own[2 * width :].astype(BF)
            keep_projected(kept, at, own[: 2 * width], k, masks)

    def finish(ps):
        ats = [q * pairs + p for p in ps for q in range(per)]
        done = finish_items(att_ref, ats, w_proj_t, flip, lambda at: xt_ref[at])
        for a, p in enumerate(ps):
            y_ref[p] = pack(done[a * per : (a + 1) * per])

    most = max(1, 1024 // rows)
    loop(items, min(2 * most, 16), project)
    loop(items, min(most, 8), lambda ats: attend(kept, att_ref, ats, ones))
    loop(pairs, min(most, 8), finish)
    for m in range(groups):
        at = pl.multiple_of((here ^ m) * local, local)
        outs[m][...] = y_ref[:, pl.ds(at, local), :]


def row_chunk(pieces, count, wqkv, wproj, groups, per, chunks, pairs, firsts):
    sub_rows, packed = pieces[0].shape[1:]
    width = wproj.shape[0]
    local = sub_rows * chunks
    rows = local * groups
    keys = rows - rows // 4
    return pl.pallas_call(
        functools.partial(row_kernel, groups, per, chunks, firsts),
        in_specs=[IN_SMEM] + [IN_VMEM] * (2 + len(pieces)),
        out_specs=[IN_VMEM] * groups,
        out_shape=[near((pairs, local, packed))] * groups,
        scratch_shapes=attention_scratch(pairs * per, width, rows, keys)
        + [
            pltpu.VMEM((pairs * per, rows, width), BF),
            pltpu.VMEM((pairs * per, width, rows), BF),
            pltpu.VMEM((pairs, rows, packed), BF),
        ],
        compiler_params=PARAMS,
        cost_estimate=cost(10**8),
    )(count, *bring(wqkv, wproj, *pieces))


def swap_kernel(in_ref, out_ref, x_ref):
    first, width, second = in_ref.shape
    lanes = -(-second // 128) * 128
    side = 16
    swap = swap_matrix(side)
    for a in range(first):
        x_ref[a] = pad_lanes(in_ref[a], lanes).T[:second]
    for a in range(first // side):
        for b in range(second // side):
            block = x_ref[a * side : (a + 1) * side, b * side : (b + 1) * side, :]
            swapped = dot(swap, block.reshape(side * side, width)).astype(BF)
            out_ref[b * side : (b + 1) * side, a * side : (a + 1) * side, :] = swapped.reshape(side, side, width)


def swap_cotangent(array_t):
    first, width, second = array_t.shape
    return pl.pallas_call(
        swap_kernel,
        in_specs=[IN_VMEM],
        out_specs=IN_VMEM,
        out_shape=near((second, first, width)),
        scratch_shapes=[pltpu.VMEM((first, second, width), BF)],
        compiler_params=PARAMS,
        cost_estimate=cost(10**8),
        name="swap_cotangent",
    )(*bring(array_t))


def output_kernel(groups, per, spots, *refs):
    parts, (out_ref, f_ref, y_ref) = refs[:-3], refs[-3:]
    feats, local, width = f_ref.shape
    half = feats // groups // per
    lanes = -(-feats // 128) * 128
    here = cell_index()
    for (first_m, start, pairs), part in zip(spots, parts):
        size = pairs * local
        for b in range(part.shape[0]):
            base = (here ^ (first_m + b)) * (half * per) + start
            for q in range(per):
                rows = part[b, q * size : (q + 1) * size].reshape(pairs, local, width)
                f_ref[pl.ds(base + q * half, pairs)] = rows
    side = 16
    swap = swap_matrix(side)
    for f in range(0, feats, side):
        for r in range(0, local, side):
            block = f_ref[f : f + side, r : r + side, :].reshape(side * side, width)
            y_ref[r : r + side, f : f + side, :] = dot(swap, block).astype(BF).reshape(side, side, width)
    for r in range(local):
        y = y_ref[r]
        if lanes > feats:
            y = jnp.concatenate([y, jnp.zeros((lanes - feats, width), BF)], axis=0)
        out_ref[r] = y.T[:, :feats]


def make_output(parts, spots, groups, per, feats, local):
    width = parts[0].shape[-1]
    return pl.pallas_call(
        functools.partial(output_kernel, groups, per, spots),
        in_specs=[IN_VMEM] * len(parts),
        out_specs=IN_VMEM,
        out_shape=jax.ShapeDtypeStruct((local, width, feats), BF),
        scratch_shapes=[pltpu.VMEM((feats, local, width), BF), pltpu.VMEM((local, feats, width), BF)],
        compiler_params=PARAMS,
        cost_estimate=cost(10**8),
        name="make_output",
    )(*bring(*parts))


def gelu_and_slope(pre):
    size = jnp.abs(pre)
    bell = jnp.exp2(pre * pre * F32(-0.5 * math.log2(math.e)))
    t = 1.0 / (size + F32(ERFC_K))
    poly = F32(ERFC_C[-1])
    for coefficient in ERFC_C[-2::-1]:
        poly = poly * t + F32(coefficient)
    tail = poly * t * bell
    cdf = jnp.where(pre >= 0, 1.0 - tail, tail)
    return pre * cdf, cdf + pre * (bell * F32(1.0 / math.sqrt(2.0 * math.pi)))


def dense_kernel(groups, per, spot, fresh, factor, *refs):
    first_m, start, _ = spot
    last = factor is not None
    blocks = refs[-1].shape[0]
    ins = refs[:blocks]
    win_ref, woutt_ref, cot_ref = refs[blocks : blocks + 3]
    rest = refs[blocks + (3 if fresh else 5) :]
    if last:
        out_ref, gin_ref, gout_ref, keep_ref, send_ref, n_ref = rest
    else:
        out_ref, gin_ref, gout_ref, n_ref = rest
    pairs, local, _ = ins[0].shape
    width, _ = win_ref.shape
    size = pairs * local
    fg = cot_ref.shape[0] // groups
    half = fg // per
    here = cell_index()
    for b in range(blocks):
        for q, part in enumerate(unpack(ins[b][...], per, width)):
            n_ref[b, q * size : (q + 1) * size] = part.reshape(size, width)
    if fresh:
        gin_ref[...] = jnp.zeros_like(gin_ref)
        gout_ref[...] = jnp.zeros_like(gout_ref)
    w_in = win_ref[...]
    w_out_t = woutt_ref[...]

    def step(b):
        feature = (here ^ (first_m + b)) * fg + start
        normed = n_ref[b]
        cot = [cot_ref[pl.ds(feature + q * half, pairs)].reshape(size, width) for q in range(per)]
        cot = jnp.concatenate(cot, axis=0)
        act, slope = gelu_and_slope(dot(normed, w_in))
        act = act.astype(BF)
        out_ref[b] = (normed.astype(F32) + dot(act, w_out_t, NT)).astype(BF)
        dpre = (dot(cot, w_out_t) * slope).astype(BF)
        gin_ref[...] += dot(normed, dpre, TN)
        gout_ref[...] += dot(cot, act, TN)

    loop(blocks, BLOCKS, lambda bs: [step(b) for b in bs])
    if last:
        both = pack([(gin_ref[...].T * F32(factor)).astype(BF), (gout_ref[...].T * F32(factor)).astype(BF)])
        both = both.reshape(keep_ref.shape[0], 2, *keep_ref.shape[1:])
        even = here % 2 == 0
        keep_ref[...] = jnp.where(even, both[:, 0], both[:, 1])
        send_ref[...] = jnp.where(even, both[:, 1], both[:, 0])


def dense_part(blocks, cot_t, w_in, w_out_t, prev, groups, per, spot, factor, shares):
    pairs, local, _ = blocks[0].shape
    width, hid = w_in.shape
    size = per * pairs * local
    count = len(blocks)
    outs = [near((count, size, width))] + [near((width, hid), F32)] * 2
    operands = list(blocks) + [w_in, w_out_t, cot_t]
    alias = {}
    if prev is not None:
        alias = {len(operands) + n: 1 + n for n in range(2)}
        operands += list(prev)
    if factor is not None:
        outs += [near((shares // 2, hid // shares, 2 * width))] * 2
    return pl.pallas_call(
        functools.partial(dense_kernel, groups, per, spot, prev is None, factor),
        in_specs=[IN_VMEM] * len(operands),
        out_specs=[IN_VMEM] * len(outs),
        out_shape=outs,
        input_output_aliases=alias,
        scratch_shapes=[pltpu.VMEM((count, size, width), BF)],
        compiler_params=PARAMS,
        cost_estimate=cost(10**8),
    )(*bring(*operands))


def add_kernel(a_ref, b_ref, out_ref):
    out_ref[...] = (a_ref[...].astype(F32) + b_ref[...].astype(F32)).astype(BF)


def add_pair(a, b):
    return pl.pallas_call(
        add_kernel,
        in_specs=[IN_VMEM] * 2,
        out_specs=IN_VMEM,
        out_shape=near(a.shape),
        compiler_params=PARAMS,
        cost_estimate=cost(10**6),
        name="add_pair",
    )(*bring(a, b))


def exchange(pieces, groups):
    come = [pieces[0]]
    for m in range(1, groups):
        come.append(lax.ppermute(pieces[m], CELLS, [(s, s ^ m) for s in range(groups)]))
    return come


def per_device(
    cells_in, train_count, feat_count, feat_qkv, feat_proj, row_qkv, row_proj, w_in, w_out, cotangent
):
    block_t = jnp.swapaxes(cells_in[0], 1, 2)
    local, width, feats = block_t.shape
    groups = lax.axis_size(CELLS)
    tables = lax.axis_size("tables")
    fg = feats // groups
    per = 2 if fg % 2 == 0 else 1
    half = fg // per
    sub_rows = 16
    row_chunks = local // sub_rows
    sizes = (half * 3 // 7, half - half * 3 // 7) if half % 2 == 0 else (half,)
    offsets = [sum(sizes[:j]) for j in range(len(sizes))]
    feat_chunks = len(sizes)
    factor = 1.0 / math.sqrt(tables * local * groups * feats)
    pieces = [[] for _ in range(feat_chunks)]
    cot_t = jnp.swapaxes(cotangent[0], 1, 2)
    sent = feature_chunk(
        block_t, feat_count, feat_qkv, feat_proj, None, groups, per, 0, sub_rows, (half,)
    )
    *sent, wqkv_v, wproj_v, rest = sent
    come = exchange(sent, groups)
    for j in range(feat_chunks):
        pieces[j] += come
    *sent, cot_v = feature_chunk(
        rest, feat_count, wqkv_v, wproj_v, cot_t, groups, per, 0, sub_rows, sizes
    )
    for j in range(feat_chunks):
        pieces[j] += exchange(sent[j * groups : (j + 1) * groups], groups)
    cot_t = swap_cotangent(cot_v)
    back = []
    for j in range(feat_chunks):
        starts = (offsets[j], 0)
        done = row_chunk(pieces[j], train_count, row_qkv, row_proj, groups, per, row_chunks, sizes[j], starts)
        back.append(exchange(done, groups))
    w_out_t = w_out.T
    shares = tables * groups
    near_by = groups // 2
    spots = [(m, offsets[j], sizes[j]) for m in (0, near_by) for j in range(feat_chunks)]
    parts = []
    grads = None
    for spot in spots:
        first_m, start, _ = spot
        blocks = [back[offsets.index(start)][first_m + m] for m in range(near_by)]
        scale = factor if spot == spots[-1] else None
        made, *grads = dense_part(blocks, cot_t, w_in, w_out_t, grads, groups, per, spot, scale, shares)
        parts.append(made)
    keep, send = grads[2:]
    other = lax.ppermute(send, "core", [(0, 1), (1, 0)])
    pieces = add_pair(keep, other)
    total = lax.all_to_all(pieces, ("tables", "chips"), split_axis=0, concat_axis=0, tiled=True)
    total = jnp.sum(total.astype(F32), axis=0)
    output = make_output(parts, spots, groups, per, feats, local)
    grad_in, grad_out = unpack(total, 2, width)
    return (jnp.swapaxes(output, 1, 2)[None], grad_in.T, grad_out)


def solution(mesh):
    tables, cells = mesh.devices.shape
    split = jax.sharding.Mesh(mesh.devices.reshape(tables, cells // 2, 2), ("tables", "chips", "core"))
    spread = P("tables", CELLS, None, None)
    shares = ("tables",) + CELLS
    return jax.shard_map(
        per_device,
        mesh=split,
        in_specs=(spread, P("tables"), P("tables"), P(), P(), P(), P(), P(), P(), spread),
        out_specs=(spread, P(None, shares), P(shares, None)),
        check_vma=False,
    )
```

```python
import functools
import math

import jax
import jax.numpy as jnp
from jax import lax
from jax.experimental import pallas as pl
from jax.experimental.pallas import tpu as pltpu
from jax.sharding import PartitionSpec as P


HEADS = 6
HEAD_DIM = 32
BF = jnp.bfloat16
F32 = jnp.float32
ERFC_K = 2.9
ERFC_C = (
    0.38553786502648235,
    1.4917549496141058,
    -0.32977430445565825,
    21.663540536082817,
    -21.146073738657215,
)
NT = (((1,), (1,)), ((), ()))
TN = (((0,), (0,)), ((), ()))


def dot(a, b, dims=(((1,), (0,)), ((), ()))):
    return lax.dot_general(a, b, dims, preferred_element_type=F32)


def layer_norm(values):
    mean = jnp.mean(values, axis=0, keepdims=True)
    centred = values - mean
    var = jnp.mean(centred * centred, axis=0, keepdims=True)
    return centred * lax.rsqrt(var + 1e-05)


def one_hot(rows, cols):
    row = lax.broadcasted_iota(jnp.int32, (rows, cols), 0)
    col = lax.broadcasted_iota(jnp.int32, (rows, cols), 1)
    return (row == col).astype(F32).astype(BF)


def finish_items(att_ref, ats, w_proj_t, flip, residual_t):
    lanes = att_ref.shape[2]
    mixed = dot(w_proj_t, jnp.concatenate([att_ref[at] for at in ats], axis=1))
    done = []
    for a, at in enumerate(ats):
        normed = layer_norm(residual_t(at).astype(F32) + mixed[:, a * lanes : (a + 1) * lanes]).astype(BF)
        done.append(dot(flip, normed, NT).astype(BF))
    return done


def swap_matrix(side):
    out = lax.broadcasted_iota(jnp.int32, (side * side, side * side), 0)
    src = lax.broadcasted_iota(jnp.int32, (side * side, side * side), 1)
    return (src == (out % side) * side + out // side).astype(F32).astype(BF)


def pack(parts):
    if len(parts) == 1:
        return parts[0]
    a, b = parts
    cut = a.shape[-1] // 128 * 128
    return jnp.concatenate([a[..., :cut], b[..., :cut], a[..., cut:], b[..., cut:]], axis=-1)


def unpack(block, per, width):
    if per == 1:
        return [block]
    cut = width // 128 * 128
    rest = width - cut
    return [
        jnp.concatenate(
            [block[..., q * cut : (q + 1) * cut], block[..., 2 * cut + q * rest : 2 * cut + (q + 1) * rest]],
            axis=-1,
        )
        for q in range(2)
    ]


CELLS = ("chips", "core")


def cell_index():
    return lax.axis_index("chips") * 2 + lax.axis_index("core")


def mask_of(keys, count):
    rows = lax.broadcasted_iota(jnp.int32, (keys, 1), 0) < count
    lanes = lax.broadcasted_iota(jnp.int32, (1, keys), 1) < count
    return rows, lanes


def keep_projected(refs, at, q_v, k_rows, masks):
    q_ref, k_ref, v_ref = refs
    width, keys = q_ref.shape[1], k_ref.shape[1]
    key_row, key_lane = masks
    scale = F32(math.log2(math.e) / math.sqrt(HEAD_DIM))
    q_ref[at] = (q_v[:width] * scale).astype(BF)
    v_ref[at] = jnp.where(key_lane, q_v[width:, :keys], F32(0)).astype(BF)
    k_ref[at] = jnp.where(key_row, k_rows[:keys], k_rows[0:1]).astype(BF)


def score_blocks(q_own, lanes):
    hd = HEAD_DIM
    width = q_own.shape[0]
    blank = jnp.zeros((hd, lanes), BF)
    blocks = []
    for i in range(HEADS // 2):
        lo = 2 * i * hd
        tile = lo // 128 * 128
        end = min(tile + 128, width)
        pieces = [
            jnp.concatenate([q_own[lo : lo + hd], blank], axis=1),
            jnp.concatenate([blank, q_own[lo + hd : lo + 2 * hd]], axis=1),
        ]
        if lo > tile:
            pieces = [jnp.zeros((lo - tile, 2 * lanes), BF)] + pieces
        if lo + 2 * hd < end:
            pieces = pieces + [jnp.zeros((end - lo - 2 * hd, 2 * lanes), BF)]
        blocks.append((tile, end, jnp.concatenate(pieces, axis=0)))
    return blocks


def attend(refs, att_ref, ats, ones):
    q_ref, k_ref, v_ref = refs
    lanes = q_ref.shape[2]
    hd = HEAD_DIM
    scores = []
    for at in ats:
        k_own = k_ref[at]
        for tile, end, block in score_blocks(q_ref[at], lanes):
            scores.append(dot(k_own[:, tile:end], block))
    weights = [jnp.exp2(s - jnp.max(s, axis=0, keepdims=True)).astype(BF) for s in scores]
    for n, at in enumerate(ats):
        v_own = v_ref[at]
        for i in range(HEADS // 2):
            lo = 2 * i * hd
            lhs = jnp.concatenate([v_own[lo : lo + 2 * hd], ones], axis=0)
            mixed = dot(lhs, weights[n * (HEADS // 2) + i])
            scale = 1.0 / mixed[2 * hd : 2 * hd + 1]
            att_ref[at, lo : lo + hd] = (mixed[:hd, :lanes] * scale[:, :lanes]).astype(BF)
            att_ref[at, lo + hd : lo + 2 * hd] = (mixed[hd : 2 * hd, lanes:] * scale[:, lanes:]).astype(BF)


def loop(count, most, body):
    group = max(d for d in range(1, most + 1) if count % d == 0)

    def step(i, carry):
        body([i * group + a for a in range(group)])
        return carry

    lax.fori_loop(0, count // group, step, 0)


def pad_lanes(value, lanes):
    rows, n = value.shape
    return value if n == lanes else jnp.concatenate([value, jnp.zeros((rows, lanes - n), value.dtype)], axis=1)


def feature_kernel(groups, per, base, rows, cuts, lead, *refs):
    count_ref, cells_ref, wqkv_ref, wproj_ref, *refs = refs
    count = count_ref[0]
    first = base
    if lead:
        outs = refs[: groups * len(cuts)]
        wqkv_buf, wproj_buf, rest_buf, *refs = refs[groups * len(cuts) :]
        sems, cells_buf = refs[6:]
        moves = [(wqkv_ref, wqkv_buf), (wproj_ref, wproj_buf), (cells_ref.at[pl.ds(0, rows)], cells_buf)]
        late = (cells_ref.at[pl.ds(rows, rest_buf.shape[0])], rest_buf)
        moves = [pltpu.make_async_copy(a, b, sems.at[n]) for n, (a, b) in enumerate(moves)]
        late = pltpu.make_async_copy(*late, sems.at[3])
        for move in moves:
            move.start()
        for move in moves:
            move.wait()
        wqkv_ref, wproj_ref, cells_ref = wqkv_buf, wproj_buf, cells_buf
    else:
        cot_ref, *refs = refs
        outs = refs[: groups * len(cuts)]
        cot_buf, *refs = refs[groups * len(cuts) :]
        late = pltpu.make_async_copy(cot_ref, cot_buf, refs[6].at[0])
    late.start()
    refs = refs[:6]
    q_ref, k_ref, v_ref, att_ref, mid_ref, swap_ref = refs
    _, width, feats = cells_ref.shape
    lanes = q_ref.shape[2]
    fg = feats // groups
    half = fg // per
    w_t = wqkv_ref[...].T
    w_qv = jnp.concatenate([w_t[:width], w_t[2 * width :]], axis=0)
    w_k = w_t[width : 2 * width]
    w_proj_t = wproj_ref[...].T
    flip = one_hot(feats, lanes)
    masks = mask_of(feats, count)
    ones = jnp.broadcast_to(jnp.where(masks[1], F32(1), F32(0)), (16, feats)).astype(BF)
    kept = (q_ref, k_ref, v_ref)

    def project(ats):
        x_t = [pad_lanes(cells_ref[first + at], lanes) for at in ats]
        q_v = dot(w_qv, jnp.concatenate(x_t, axis=1))
        x = [t.T[:feats] for t in x_t]
        k = dot(jnp.concatenate(x, axis=0), w_k, NT)
        for a, at in enumerate(ats):
            keep_projected(kept, at, q_v[:, a * lanes : (a + 1) * lanes], k[a * feats : (a + 1) * feats], masks)

    def finish(ats):
        own = lambda at: pad_lanes(cells_ref[first + at], lanes)
        for at, value in zip(ats, finish_items(att_ref, ats, w_proj_t, flip, own)):
            mid_ref[at] = value

    loop(rows, 16, project)
    loop(rows, 8, lambda ats: attend(kept, att_ref, ats, ones))
    loop(rows, 16, finish)
    swap = swap_matrix(rows)
    for f in range(feats // rows):
        block = mid_ref[:, f * rows : (f + 1) * rows, :].reshape(rows * rows, width)
        swap_ref[f * rows : (f + 1) * rows] = dot(swap, block).astype(BF).reshape(rows, rows, width)
    here = cell_index()
    for c, size in enumerate(cuts):
        for m in range(groups):
            base = (here ^ m) * fg + sum(cuts[:c])
            outs[c * groups + m][...] = pack([swap_ref[pl.ds(base + q * half, size)] for q in range(per)])
    late.wait()


BLOCKS = 2
IN_VMEM = pl.BlockSpec(memory_space=pltpu.VMEM)
IN_SMEM = pl.BlockSpec(memory_space=pltpu.SMEM)


def attention_scratch(items, width, lanes, keys):
    return [
        pltpu.VMEM((items, width, lanes), BF),
        pltpu.VMEM((items, keys, width), BF),
        pltpu.VMEM((items, width, keys), BF),
        pltpu.VMEM((items, width, lanes), BF),
    ]


def near(shape, dtype=BF):
    return pltpu.VMEM(shape, dtype)


def bring(*arrays):
    return [pltpu.with_memory_space_constraint(x, pltpu.VMEM) for x in arrays]


PARAMS = pltpu.CompilerParams(vmem_limit_bytes=14 * 2**20)


def cost(flops):
    return pl.CostEstimate(flops=flops, transcendentals=0, bytes_accessed=10**6)


def feature_chunk(cells_t, count, wqkv, wproj, cot_t, groups, per, base, rows, cuts):
    whole, width, feats = cells_t.shape
    lanes = -(-feats // 128) * 128
    far = pl.BlockSpec(memory_space=pltpu.HBM)
    lead = cot_t is None
    outs = [near((size, rows, per * width)) for size in cuts for _ in range(groups)]
    scratch = attention_scratch(rows, width, lanes, feats)
    scratch += [pltpu.VMEM((rows, feats, width), BF), pltpu.VMEM((feats, rows, width), BF)]
    operands = [cells_t, wqkv, wproj]
    if lead:
        operands = [pltpu.with_memory_space_constraint(x, pltpu.HBM) for x in operands]
        specs = [far] * 3
        outs += [near(wqkv.shape), near(wproj.shape), near((whole - rows, width, feats))]
        scratch += [pltpu.SemaphoreType.DMA((4,)), pltpu.VMEM((rows, width, feats), BF)]
    else:
        operands = bring(*operands) + [pltpu.with_memory_space_constraint(cot_t, pltpu.HBM)]
        specs = [IN_VMEM] * 3 + [far]
        outs += [near(cot_t.shape)]
        scratch += [pltpu.SemaphoreType.DMA((1,))]
    return pl.pallas_call(
        functools.partial(feature_kernel, groups, per, base, rows, cuts, lead),
        in_specs=[IN_SMEM] + specs,
        out_specs=[IN_VMEM] * len(outs),
        out_shape=outs,
        scratch_shapes=scratch,
        compiler_params=PARAMS,
        cost_estimate=cost(10**8),
        name="feature_0" if lead else "feature_1",
    )(count, *operands)


def row_kernel(groups, per, chunks, firsts, count_ref, wqkv_ref, wproj_ref, *refs):
    ins = refs[: groups * chunks]
    outs = refs[groups * chunks : groups * chunks + groups]
    q_ref, k_ref, v_ref, att_ref, x_ref, xt_ref, y_ref = refs[groups * chunks + groups :]
    pairs, local, _ = outs[0].shape
    sub_rows = local // chunks
    items, rows, width = x_ref.shape
    keys = k_ref.shape[1]
    count = count_ref[0]
    w_t = wqkv_ref[...].T
    w_qv = jnp.concatenate([w_t[:width], w_t[2 * width :], one_hot(width, width)], axis=0)
    w_k = w_t[width : 2 * width]
    w_proj_t = wproj_ref[...].T
    flip = one_hot(rows, rows)
    masks = mask_of(keys, count)
    ones = jnp.broadcast_to(jnp.where(masks[1], F32(1), F32(0)), (16, keys)).astype(BF)
    kept = (q_ref, k_ref, v_ref)
    here = cell_index()
    for m in range(groups):
        for k in range(chunks):
            at = pl.multiple_of((here ^ m) * local + k * sub_rows, sub_rows)
            for q, part in enumerate(unpack(ins[k * groups + m][firsts[k] : firsts[k] + pairs], per, width)):
                x_ref[q * pairs : (q + 1) * pairs, pl.ds(at, sub_rows), :] = part

    def project(ats):
        x = jnp.concatenate([x_ref[at] for at in ats], axis=0)
        q_v = dot(w_qv, x, NT)
        for a, at in enumerate(ats):
            k = dot(x[a * rows : a * rows + keys], w_k, NT)
            own = q_v[:, a * rows : (a + 1) * rows]
            xt_ref[at] = own[2 * width :].astype(BF)
            keep_projected(kept, at, own[: 2 * width], k, masks)

    def finish(ps):
        ats = [q * pairs + p for p in ps for q in range(per)]
        done = finish_items(att_ref, ats, w_proj_t, flip, lambda at: xt_ref[at])
        for a, p in enumerate(ps):
            y_ref[p] = pack(done[a * per : (a + 1) * per])

    most = max(1, 1024 // rows)
    loop(items, min(2 * most, 16), project)
    loop(items, min(most, 8), lambda ats: attend(kept, att_ref, ats, ones))
    loop(pairs, min(most, 8), finish)
    for m in range(groups):
        at = pl.multiple_of((here ^ m) * local, local)
        outs[m][...] = y_ref[:, pl.ds(at, local), :]


def row_chunk(pieces, count, wqkv, wproj, groups, per, chunks, pairs, firsts):
    sub_rows, packed = pieces[0].shape[1:]
    width = wproj.shape[0]
    local = sub_rows * chunks
    rows = local * groups
    keys = rows - rows // 4
    return pl.pallas_call(
        functools.partial(row_kernel, groups, per, chunks, firsts),
        in_specs=[IN_SMEM] + [IN_VMEM] * (2 + len(pieces)),
        out_specs=[IN_VMEM] * groups,
        out_shape=[near((pairs, local, packed))] * groups,
        scratch_shapes=attention_scratch(pairs * per, width, rows, keys)
        + [
            pltpu.VMEM((pairs * per, rows, width), BF),
            pltpu.VMEM((pairs * per, width, rows), BF),
            pltpu.VMEM((pairs, rows, packed), BF),
        ],
        compiler_params=PARAMS,
        cost_estimate=cost(10**8),
    )(count, *bring(wqkv, wproj, *pieces))


def swap_kernel(in_ref, out_ref, x_ref):
    first, width, second = in_ref.shape
    lanes = -(-second // 128) * 128
    side = 16
    swap = swap_matrix(side)
    for a in range(first):
        x_ref[a] = pad_lanes(in_ref[a], lanes).T[:second]
    for a in range(first // side):
        for b in range(second // side):
            block = x_ref[a * side : (a + 1) * side, b * side : (b + 1) * side, :]
            swapped = dot(swap, block.reshape(side * side, width)).astype(BF)
            out_ref[b * side : (b + 1) * side, a * side : (a + 1) * side, :] = swapped.reshape(side, side, width)


def swap_cotangent(array_t):
    first, width, second = array_t.shape
    return pl.pallas_call(
        swap_kernel,
        in_specs=[IN_VMEM],
        out_specs=IN_VMEM,
        out_shape=near((second, first, width)),
        scratch_shapes=[pltpu.VMEM((first, second, width), BF)],
        compiler_params=PARAMS,
        cost_estimate=cost(10**8),
        name="swap_cotangent",
    )(*bring(array_t))


def output_kernel(groups, per, spots, *refs):
    parts, (out_ref, f_ref, y_ref) = refs[:-3], refs[-3:]
    feats, local, width = f_ref.shape
    half = feats // groups // per
    lanes = -(-feats // 128) * 128
    here = cell_index()
    for (first_m, start, pairs), part in zip(spots, parts):
        size = pairs * local
        for b in range(part.shape[0]):
            base = (here ^ (first_m + b)) * (half * per) + start
            for q in range(per):
                rows = part[b, q * size : (q + 1) * size].reshape(pairs, local, width)
                f_ref[pl.ds(base + q * half, pairs)] = rows
    side = 16
    swap = swap_matrix(side)
    for f in range(0, feats, side):
        for r in range(0, local, side):
            block = f_ref[f : f + side, r : r + side, :].reshape(side * side, width)
            y_ref[r : r + side, f : f + side, :] = dot(swap, block).astype(BF).reshape(side, side, width)
    for r in range(local):
        y = y_ref[r]
        if lanes > feats:
            y = jnp.concatenate([y, jnp.zeros((lanes - feats, width), BF)], axis=0)
        out_ref[r] = y.T[:, :feats]


def make_output(parts, spots, groups, per, feats, local):
    width = parts[0].shape[-1]
    return pl.pallas_call(
        functools.partial(output_kernel, groups, per, spots),
        in_specs=[IN_VMEM] * len(parts),
        out_specs=IN_VMEM,
        out_shape=jax.ShapeDtypeStruct((local, width, feats), BF),
        scratch_shapes=[pltpu.VMEM((feats, local, width), BF), pltpu.VMEM((local, feats, width), BF)],
        compiler_params=PARAMS,
        cost_estimate=cost(10**8),
        name="make_output",
    )(*bring(*parts))


def gelu_and_slope(pre):
    size = jnp.abs(pre)
    bell = jnp.exp2(pre * pre * F32(-0.5 * math.log2(math.e)))
    t = 1.0 / (size + F32(ERFC_K))
    poly = F32(ERFC_C[-1])
    for coefficient in ERFC_C[-2::-1]:
        poly = poly * t + F32(coefficient)
    tail = poly * t * bell
    cdf = jnp.where(pre >= 0, 1.0 - tail, tail)
    return pre * cdf, cdf + pre * (bell * F32(1.0 / math.sqrt(2.0 * math.pi)))


def dense_kernel(groups, per, spot, fresh, factor, *refs):
    first_m, start, _ = spot
    last = factor is not None
    blocks = refs[-1].shape[0]
    ins = refs[:blocks]
    win_ref, woutt_ref, cot_ref = refs[blocks : blocks + 3]
    rest = refs[blocks + (3 if fresh else 5) :]
    if last:
        out_ref, gin_ref, gout_ref, keep_ref, send_ref, n_ref = rest
    else:
        out_ref, gin_ref, gout_ref, n_ref = rest
    pairs, local, _ = ins[0].shape
    width, _ = win_ref.shape
    size = pairs * local
    fg = cot_ref.shape[0] // groups
    half = fg // per
    here = cell_index()
    for b in range(blocks):
        for q, part in enumerate(unpack(ins[b][...], per, width)):
            n_ref[b, q * size : (q + 1) * size] = part.reshape(size, width)
    if fresh:
        gin_ref[...] = jnp.zeros_like(gin_ref)
        gout_ref[...] = jnp.zeros_like(gout_ref)
    w_in = win_ref[...]
    w_out_t = woutt_ref[...]

    def step(b):
        feature = (here ^ (first_m + b)) * fg + start
        normed = n_ref[b]
        cot = [cot_ref[pl.ds(feature + q * half, pairs)].reshape(size, width) for q in range(per)]
        cot = jnp.concatenate(cot, axis=0)
        act, slope = gelu_and_slope(dot(normed, w_in))
        act = act.astype(BF)
        out_ref[b] = (normed.astype(F32) + dot(act, w_out_t, NT)).astype(BF)
        dpre = (dot(cot, w_out_t) * slope).astype(BF)
        gin_ref[...] += dot(normed, dpre, TN)
        gout_ref[...] += dot(cot, act, TN)

    loop(blocks, BLOCKS, lambda bs: [step(b) for b in bs])
    if last:
        both = [(ref[...].T * F32(factor)).astype(BF) for ref in (gin_ref, gout_ref)]
        both = jnp.concatenate(both, axis=1)
        both = both.reshape(keep_ref.shape[0], 2, *keep_ref.shape[1:])
        even = here % 2 == 0
        keep_ref[...] = jnp.where(even, both[:, 0], both[:, 1])
        send_ref[...] = jnp.where(even, both[:, 1], both[:, 0])


def dense_part(blocks, cot_t, w_in, w_out_t, prev, groups, per, spot, factor, shares):
    pairs, local, _ = blocks[0].shape
    width, hid = w_in.shape
    size = per * pairs * local
    count = len(blocks)
    outs = [near((count, size, width))] + [near((width, hid), F32)] * 2
    operands = list(blocks) + [w_in, w_out_t, cot_t]
    alias = {}
    if prev is not None:
        alias = {len(operands) + n: 1 + n for n in range(2)}
        operands += list(prev)
    if factor is not None:
        outs += [near((shares // 2, hid // shares, 2 * width))] * 2
    return pl.pallas_call(
        functools.partial(dense_kernel, groups, per, spot, prev is None, factor),
        in_specs=[IN_VMEM] * len(operands),
        out_specs=[IN_VMEM] * len(outs),
        out_shape=outs,
        input_output_aliases=alias,
        scratch_shapes=[pltpu.VMEM((count, size, width), BF)],
        compiler_params=PARAMS,
        cost_estimate=cost(10**8),
    )(*bring(*operands))


def add_kernel(a_ref, b_ref, out_ref):
    out_ref[...] = (a_ref[...].astype(F32) + b_ref[...].astype(F32)).astype(BF)


def add_pair(a, b):
    return pl.pallas_call(
        add_kernel,
        in_specs=[IN_VMEM] * 2,
        out_specs=IN_VMEM,
        out_shape=near(a.shape),
        compiler_params=PARAMS,
        cost_estimate=cost(10**6),
        name="add_pair",
    )(*bring(a, b))


def exchange(pieces, groups):
    come = [pieces[0]]
    for m in range(1, groups):
        come.append(lax.ppermute(pieces[m], CELLS, [(s, s ^ m) for s in range(groups)]))
    return come


def per_device(
    cells_in, train_count, feat_count, feat_qkv, feat_proj, row_qkv, row_proj, w_in, w_out, cotangent
):
    block_t = jnp.swapaxes(cells_in[0], 1, 2)
    local, width, feats = block_t.shape
    groups = lax.axis_size(CELLS)
    tables = lax.axis_size("tables")
    fg = feats // groups
    per = 2 if fg % 2 == 0 else 1
    half = fg // per
    sub_rows = 16
    row_chunks = local // sub_rows
    sizes = (half * 3 // 7, half - half * 3 // 7) if half % 2 == 0 else (half,)
    offsets = [sum(sizes[:j]) for j in range(len(sizes))]
    feat_chunks = len(sizes)
    factor = 1.0 / math.sqrt(tables * local * groups * feats)
    pieces = [[] for _ in range(feat_chunks)]
    cot_t = jnp.swapaxes(cotangent[0], 1, 2)
    sent = feature_chunk(
        block_t, feat_count, feat_qkv, feat_proj, None, groups, per, 0, sub_rows, (half,)
    )
    *sent, wqkv_v, wproj_v, rest = sent
    come = exchange(sent, groups)
    for j in range(feat_chunks):
        pieces[j] += come
    *sent, cot_v = feature_chunk(
        rest, feat_count, wqkv_v, wproj_v, cot_t, groups, per, 0, sub_rows, sizes
    )
    for j in range(feat_chunks):
        pieces[j] += exchange(sent[j * groups : (j + 1) * groups], groups)
    cot_t = swap_cotangent(cot_v)
    back = []
    for j in range(feat_chunks):
        starts = (offsets[j], 0)
        done = row_chunk(pieces[j], train_count, row_qkv, row_proj, groups, per, row_chunks, sizes[j], starts)
        back.append(exchange(done, groups))
    w_out_t = w_out.T
    shares = tables * groups
    near_by = groups // 2
    spots = [(m, offsets[j], sizes[j]) for m in (0, near_by) for j in range(feat_chunks)]
    parts = []
    grads = None
    for spot in spots:
        first_m, start, _ = spot
        blocks = [back[offsets.index(start)][first_m + m] for m in range(near_by)]
        scale = factor if spot == spots[-1] else None
        made, *grads = dense_part(blocks, cot_t, w_in, w_out_t, grads, groups, per, spot, scale, shares)
        parts.append(made)
    keep, send = grads[2:]
    other = lax.ppermute(send, "core", [(0, 1), (1, 0)])
    pieces = add_pair(keep, other)
    total = lax.all_to_all(pieces, ("tables", "chips"), split_axis=0, concat_axis=0, tiled=True)
    total = jnp.sum(total.astype(F32), axis=0)
    output = make_output(parts, spots, groups, per, feats, local)
    grad_in, grad_out = total[:, :width], total[:, width:]
    return (jnp.swapaxes(output, 1, 2)[None], grad_in.T, grad_out)


def solution(mesh):
    tables, cells = mesh.devices.shape
    split = jax.sharding.Mesh(mesh.devices.reshape(tables, cells // 2, 2), ("tables", "chips", "core"))
    spread = P("tables", CELLS, None, None)
    shares = ("tables",) + CELLS
    return jax.shard_map(
        per_device,
        mesh=split,
        in_specs=(spread, P("tables"), P("tables"), P(), P(), P(), P(), P(), P(), spread),
        out_specs=(spread, P(None, shares), P(shares, None)),
        check_vma=False,
    )
```
